32 devices in a mesh: data: 1 (over z), model: 4 (over y), beam: 8 (over x, core).
Axes of the slice: x: 4, y: 4, z: 1, core: 2. Of those that a mesh axis runs over, the one named last changes fastest.
The devices are a block of a 4x4x8 slice.
Arguments:
- x_embed: bfloat16 [32, 4096], P(('data', 'beam'))
- parent: int32 [1, 32], P('data')
- position: int32 [], replicated
- score: float32 [32], P(('data', 'beam'))
- k_cache: bfloat16 [1, 32, 512, 32, 128], P(None, ('data', 'beam'), None, 'model')
- v_cache: bfloat16 [1, 32, 512, 32, 128], P(None, ('data', 'beam'), None, 'model')
- gain_attn: bfloat16 [1, 4096], replicated
- w_query: bfloat16 [1, 4096, 4096], P(None, None, 'model')
- w_key: bfloat16 [1, 4096, 4096], P(None, None, 'model')
- w_value: bfloat16 [1, 4096, 4096], P(None, None, 'model')
- w_out: bfloat16 [1, 4096, 4096], P(None, 'model')
- gain_mlp: bfloat16 [1, 4096], replicated
- w_gate: bfloat16 [1, 4096, 11008], P(None, None, 'model')
- w_up: bfloat16 [1, 4096, 11008], P(None, None, 'model')
- w_down: bfloat16 [1, 11008, 4096], P(None, 'model')
- gain_final: bfloat16 [4096], replicated
- w_vocab: bfloat16 [4096, 32000], P(None, 'model')
Outputs:
- output 1: bfloat16 [1, 32, 512, 32, 128], P(None, ('data', 'beam'), None, 'model')
- output 2: bfloat16 [1, 32, 512, 32, 128], P(None, ('data', 'beam'), None, 'model')
- output 3: float32 [32, 32000], P(('data', 'beam'), 'model')
All inputs are finite; a program needn't handle non-finite values.
Results may differ from the reference program's by a relative error of at most 0.001.
Values are sent between devices in bfloat16 or wider.
A program may use at most 768 MiB of HBM per device.

```python
import jax
import jax.numpy as jnp
from jax import lax

D_MODEL = 4096
N_HEADS = 32
KV_HEADS = 32
HEAD_DIM = 128
FF_DIM = 11008
VOCAB_SIZE = 32000
BATCH = 32
BEAM_WIDTH = 32
CACHE_LEN = 512
LAYERS = 1

SENTENCES = BATCH // BEAM_WIDTH
GROUP_SIZE = N_HEADS // KV_HEADS
NORM_EPS = 1e-6
ROPE_BASE = 10000.0


def rms_norm(residual, gain):
    inv_rms = lax.rsqrt(jnp.mean(residual * residual, axis=-1, keepdims=True) + NORM_EPS)
    return (residual * inv_rms * gain.astype(jnp.float32)).astype(jnp.bfloat16)


def rope_rotate(vectors, position):
    half_dim = HEAD_DIM // 2
    inv_freq = ROPE_BASE ** (-jnp.arange(half_dim, dtype=jnp.float32) / half_dim)
    angles = position.astype(jnp.float32) * inv_freq
    cos_part = jnp.cos(angles)
    sin_part = jnp.sin(angles)
    lower_half = vectors[..., :half_dim]
    upper_half = vectors[..., half_dim:]
    return jnp.concatenate([lower_half * cos_part - upper_half * sin_part, upper_half * cos_part + lower_half * sin_part], axis=-1)


def draw_parent(key):
    key_lead, key_coin, key_any = jax.random.split(key, 3)
    lead_beam = jax.random.randint(key_lead, (SENTENCES, 1), 0, BEAM_WIDTH)
    coin_flip = jax.random.randint(key_coin, (SENTENCES, BEAM_WIDTH), 0, 2)
    any_beam = jax.random.randint(key_any, (SENTENCES, BEAM_WIDTH), 0, BEAM_WIDTH)
    beam_offset = jnp.where(coin_flip == 0, lead_beam, any_beam)
    sent_start = jnp.arange(SENTENCES, dtype=jnp.int32)[:, None] * BEAM_WIDTH
    return (sent_start + beam_offset).astype(jnp.int32)


def make_weight(key, shape, scale):
    return (jax.random.normal(key, shape, jnp.float32) * scale).astype(jnp.bfloat16)


def make_gain(key, shape):
    return (1.0 + 0.4 * jax.random.normal(key, shape, jnp.float32)).astype(jnp.bfloat16)


def setup_inputs(seed: int = 0, part: int = 0) -> dict:
    own_keys = jax.random.split(jax.random.fold_in(jax.random.key(seed), part), 6)
    shared_keys = jax.random.split(jax.random.key(seed + 1), 12)
    cache_shape = (LAYERS, BATCH, CACHE_LEN, KV_HEADS, HEAD_DIM)
    q_cols = N_HEADS * HEAD_DIM
    kv_cols = KV_HEADS * HEAD_DIM
    v_mean = jax.random.normal(own_keys[4], (LAYERS, BATCH, 1, KV_HEADS, HEAD_DIM), jnp.float32)
    return {
        'x_embed': jax.random.normal(own_keys[0], (BATCH, D_MODEL), jnp.float32).astype(jnp.bfloat16),
        'parent': draw_parent(own_keys[1]),
        'position': jax.random.randint(shared_keys[0], (), CACHE_LEN // 2, CACHE_LEN).astype(jnp.int32),
        'score': -jax.random.uniform(own_keys[2], (BATCH,), jnp.float32, 0.0, 8.0),
        'k_cache': (2.5 * jax.random.normal(own_keys[3], cache_shape, jnp.float32)).astype(jnp.bfloat16),
        'v_cache': (v_mean + jax.random.normal(own_keys[5], cache_shape, jnp.float32)).astype(jnp.bfloat16),
        'gain_attn': make_gain(shared_keys[1], (LAYERS, D_MODEL)),
        'w_query': make_weight(shared_keys[2], (LAYERS, D_MODEL, q_cols), D_MODEL ** -0.5),
        'w_key': make_weight(shared_keys[3], (LAYERS, D_MODEL, kv_cols), 2.5 * D_MODEL ** -0.5),
        'w_value': make_weight(shared_keys[4], (LAYERS, D_MODEL, kv_cols), D_MODEL ** -0.5),
        'w_out': make_weight(shared_keys[5], (LAYERS, q_cols, D_MODEL), q_cols ** -0.5),
        'gain_mlp': make_gain(shared_keys[6], (LAYERS, D_MODEL)),
        'w_gate': make_weight(shared_keys[7], (LAYERS, D_MODEL, FF_DIM), D_MODEL ** -0.5),
        'w_up': make_weight(shared_keys[8], (LAYERS, D_MODEL, FF_DIM), D_MODEL ** -0.5),
        'w_down': make_weight(shared_keys[9], (LAYERS, FF_DIM, D_MODEL), FF_DIM ** -0.5),
        'gain_final': make_gain(shared_keys[10], (D_MODEL,)),
        'w_vocab': make_weight(shared_keys[11], (D_MODEL, VOCAB_SIZE), 2.0 * D_MODEL ** -0.5),
    }


def reference(x_embed, parent, position, score, k_cache, v_cache, gain_attn, w_query, w_key, w_value, w_out, gain_mlp, w_gate, w_up, w_down, gain_final, w_vocab):
    flat_parent = parent.reshape(BATCH)
    slot_mask = (jnp.arange(CACHE_LEN, dtype=position.dtype) <= position)[None, None, None, :]

    def layer_step(residual, params):
        k_layer, v_layer, g_attn, wq_layer, wk_layer, wv_layer, wo_layer, g_mlp, wg_layer, wu_layer, wd_layer = params
        k_sel = k_layer[flat_parent]
        v_sel = v_layer[flat_parent]
        normed = rms_norm(residual, g_attn)
        q_rot = rope_rotate(jnp.dot(normed, wq_layer, preferred_element_type=jnp.float32).reshape(BATCH, N_HEADS, HEAD_DIM), position).astype(jnp.bfloat16)
        k_new = rope_rotate(jnp.dot(normed, wk_layer, preferred_element_type=jnp.float32).reshape(BATCH, KV_HEADS, HEAD_DIM), position).astype(jnp.bfloat16)
        v_new = jnp.dot(normed, wv_layer, preferred_element_type=jnp.float32).astype(jnp.bfloat16).reshape(BATCH, KV_HEADS, HEAD_DIM)
        k_sel = lax.dynamic_update_slice_in_dim(k_sel, k_new[:, None].astype(k_sel.dtype), position, axis=1)
        v_sel = lax.dynamic_update_slice_in_dim(v_sel, v_new[:, None].astype(v_sel.dtype), position, axis=1)
        q_grouped = q_rot.reshape(BATCH, KV_HEADS, GROUP_SIZE, HEAD_DIM)
        logits = jnp.einsum('bkgd,bskd->bkgs', q_grouped.astype(jnp.float32), k_sel.astype(jnp.float32)) * HEAD_DIM ** -0.5
        logits = jnp.where(slot_mask, logits, -jnp.inf)
        attn_prob = jax.nn.softmax(logits, axis=-1).astype(jnp.bfloat16)
        attn_out = jnp.einsum('bkgs,bskd->bkgd', attn_prob.astype(jnp.float32), v_sel.astype(jnp.float32)).astype(jnp.bfloat16)
        residual = residual + jnp.dot(attn_out.reshape(BATCH, N_HEADS * HEAD_DIM), wo_layer, preferred_element_type=jnp.float32)
        normed = rms_norm(residual, g_mlp)
        gate_proj = jnp.dot(normed, wg_layer, preferred_element_type=jnp.float32)
        up_proj = jnp.dot(normed, wu_layer, preferred_element_type=jnp.float32)
        hidden = (jax.nn.silu(gate_proj) * up_proj).astype(jnp.bfloat16)
        residual = residual + jnp.dot(hidden, wd_layer, preferred_element_type=jnp.float32)
        return residual, (k_sel, v_sel)

    residual, (k_out, v_out) = lax.scan(layer_step, x_embed.astype(jnp.float32), (k_cache, v_cache, gain_attn, w_query, w_key, w_value, w_out, gain_mlp, w_gate, w_up, w_down))
    logits = jnp.dot(rms_norm(residual, gain_final), w_vocab, preferred_element_type=jnp.float32)
    candidates = score[flat_parent][:, None] + jax.nn.log_softmax(logits, axis=-1)
    return k_out, v_out, candidates
```

```python
import functools

import jax
import jax.numpy as jnp
from jax import lax
from jax.experimental import pallas as pl
from jax.experimental.pallas import tpu as pltpu
from jax.sharding import PartitionSpec as P

NORM_EPS = 1e-6
ROPE_BASE = 10000.0
MESH = pl.DeviceIdType.MESH
CHUNKS = 4
TABLE = 24
ROUND_CHOICES = (3, 4)


def rms_norm(residual, gain):
    inv_rms = lax.rsqrt(jnp.mean(residual * residual, axis=-1, keepdims=True) + NORM_EPS)
    return (residual * inv_rms * gain.astype(jnp.float32)).astype(jnp.bfloat16)


def rope_rotate(vectors, position):
    half_dim = vectors.shape[-1] // 2
    inv_freq = ROPE_BASE ** (-jnp.arange(half_dim, dtype=jnp.float32) / half_dim)
    angles = position.astype(jnp.float32) * inv_freq
    cos_part = jnp.cos(angles)
    sin_part = jnp.sin(angles)
    lower_half = vectors[..., :half_dim]
    upper_half = vectors[..., half_dim:]
    return jnp.concatenate([lower_half * cos_part - upper_half * sin_part, upper_half * cos_part + lower_half * sin_part], axis=-1)


def plan_kernel(chips, chip_rows, parent_ref, table_ref, info_ref, need, via, hop1, hop2, load, own, two):
    total = chips * chip_rows
    my_chip = lax.axis_index("beam") // 2

    def each(n, body):
        lax.fori_loop(0, n, lambda i, _: (body(i), 0)[1], 0)

    def clear_rows(q):
        need[q] = 0
        via[q] = 0
        hop1[q] = 0
        hop1[total + q] = 0
        hop2[q] = 0

    def clear_links(i):
        load[i] = 0
        own[i] = 0
        two[i] = 0

    def clear_table(i):
        table_ref[i] = 0

    each(total, clear_rows)
    each(2 * chips, clear_links)
    each(2 * TABLE + chip_rows, clear_table)

    def mark(b):
        q = parent_ref[0, b]
        dist = lax.rem(b // chip_rows - q // chip_rows + chips, chips)
        need[q] = need[q] | (1 << dist)

    each(total, mark)

    def bits(q):
        n = need[q]
        return (n >> 1) & 1, (n >> 2) & 1, (n >> 3) & 1

    def up(c):
        return lax.rem(c + 1, chips)

    def down(c):
        return chips + lax.rem(c + chips - 1, chips)

    def fixed(q):
        c = q // chip_rows
        a, b, d = bits(q)
        plus = b * a * (1 - d)
        minus = b * d * (1 - a)
        own[c] = own[c] + a
        own[chips + c] = own[chips + c] + d
        load[c] = load[c] + a
        load[chips + c] = load[chips + c] + d
        load[up(c)] = load[up(c)] + plus
        load[down(c)] = load[down(c)] + minus
        via[q] = plus + 2 * minus

    each(total, fixed)

    def free(q):
        c = q // chip_rows
        a, b, d = bits(q)
        flex = b * (1 - (a ^ d))
        cost_plus = jnp.maximum(load[c] + 1 - a, load[up(c)] + 1)
        cost_minus = jnp.maximum(load[chips + c] + 1 - d, load[down(c)] + 1)
        side = (cost_plus <= cost_minus).astype(jnp.int32)
        plus = flex * side
        minus = flex * (1 - side)
        load[c] = load[c] + plus * (1 - a)
        own[c] = own[c] + plus * (1 - a)
        load[chips + c] = load[chips + c] + minus * (1 - d)
        own[chips + c] = own[chips + c] + minus * (1 - d)
        load[up(c)] = load[up(c)] + plus
        load[down(c)] = load[down(c)] + minus
        via[q] = via[q] + plus + 2 * minus

    each(total, free)

    def first_two(q):
        c = q // chip_rows
        v = via[q]
        plus = v & 1
        minus = v >> 1
        hop1[q] = two[c] * plus
        hop1[total + q] = two[chips + c] * minus
        two[c] = two[c] + plus
        two[chips + c] = two[chips + c] + minus

    each(total, first_two)

    def restart(i):
        load[i] = two[i]

    each(2 * chips, restart)

    def rest(q, rounds):
        c = q // chip_rows
        a, b, d = bits(q)
        v = via[q]
        plus = v & 1
        minus = v >> 1
        a1 = a * (1 - plus)
        d1 = d * (1 - minus)
        hop1[q] = hop1[q] + a1 * load[c]
        hop1[total + q] = hop1[total + q] + d1 * load[chips + c]
        load[c] = load[c] + a1
        load[chips + c] = load[chips + c] + d1
        onward = plus * (jnp.maximum(own[up(c)], 1) + hop1[q]) + minus * (jnp.maximum(own[down(c)], 1) + hop1[total + q])
        hop2[q] = onward
        used = jnp.maximum(onward + 1, jnp.maximum((hop1[q] + 1) * (a | plus), (hop1[total + q] + 1) * (d | minus)))
        return jnp.maximum(rounds, used * jnp.minimum(need[q] >> 1, 1))

    info_ref[0] = lax.fori_loop(0, total, rest, 0)

    def fill(q):
        c = q // chip_rows
        a, b, d = bits(q)
        v = via[q]

        @pl.when((c == my_chip) & ((a | (v & 1)) == 1))
        def _():
            table_ref[hop1[q]] = lax.rem(q, chip_rows)

        @pl.when((c == my_chip) & ((d | (v >> 1)) == 1))
        def _():
            table_ref[TABLE + hop1[total + q]] = lax.rem(q, chip_rows)

        @pl.when((up(c) == my_chip) & ((v & 1) == 1))
        def _():
            table_ref[hop2[q]] = chip_rows + hop1[q]

        @pl.when((down(c) == chips + my_chip) & ((v >> 1) == 1))
        def _():
            table_ref[TABLE + hop2[q]] = chip_rows + hop1[total + q]

    each(total, fill)

    def place(j):
        q = parent_ref[0, my_chip * chip_rows + j]
        dist = lax.rem(my_chip - q // chip_rows + chips, chips)
        v = via[q]
        at_plus = chip_rows + 2 * jnp.where(dist == 1, hop1[q], hop2[q])
        at_minus = chip_rows + 2 * jnp.where(dist == 3, hop1[total + q], hop2[q]) + 1
        from_plus = (dist == 1) | ((dist == 2) & ((v & 1) == 1))
        where = jnp.where(from_plus, at_plus, at_minus)
        table_ref[2 * TABLE + j] = jnp.where(dist == 0, lax.rem(q, chip_rows), where)

    each(chip_rows, place)


def make_plan(parent, chips, chip_rows):
    total = chips * chip_rows
    smem = pl.BlockSpec(memory_space=pltpu.SMEM)
    return pl.pallas_call(
        functools.partial(plan_kernel, chips, chip_rows),
        out_shape=(jax.ShapeDtypeStruct((2 * TABLE + chip_rows,), jnp.int32), jax.ShapeDtypeStruct((1,), jnp.int32)),
        in_specs=[smem],
        out_specs=(smem, smem),
        scratch_shapes=[
            pltpu.SMEM((total,), jnp.int32),
            pltpu.SMEM((total,), jnp.int32),
            pltpu.SMEM((2 * total,), jnp.int32),
            pltpu.SMEM((total,), jnp.int32),
            pltpu.SMEM((2 * chips,), jnp.int32),
            pltpu.SMEM((2 * chips,), jnp.int32),
            pltpu.SMEM((2 * chips,), jnp.int32),
        ],
        name="plan",
    )(parent)


def move_kernel(rounds, beams, rows, block, table, k_ref, v_ref, k_out, v_out, *scratch):
    nchunk = CHUNKS
    pool = scratch[:nchunk]
    recv = scratch[nchunk : 2 * nchunk]
    send = scratch[2 * nchunk : 3 * nchunk]
    stage = scratch[3 * nchunk : 4 * nchunk]
    pool_sem, swap_send, swap_recv, send_sem, recv_sem, out_sem, give_send, give_recv = scratch[4 * nchunk :]
    me = lax.axis_index("beam")
    core = lax.rem(me, 2)
    sibling = me + 1 - 2 * core
    right = lax.rem(me + 2, beams)
    left = lax.rem(me + beams - 2, beams)
    mine = pl.ds(core * rows, rows)
    theirs = pl.ds((1 - core) * rows, rows)
    chip_rows = 2 * rows

    def part(ref, c):
        return ref.at[:, pl.ds(c * block, block), :]

    def load_own(ref, c):
        return pltpu.make_async_copy(part(ref, c), pool[c].at[mine], pool_sem.at[c])

    def swap(ref, c):
        return pltpu.make_async_remote_copy(part(ref, c), pool[c].at[mine], swap_send.at[c], swap_recv.at[c], device_id={"beam": sibling}, device_id_type=MESH)

    def hop(r, d, c):
        return pltpu.make_async_remote_copy(
            send[c].at[2 * r + d], recv[c].at[2 * r + d], send_sem.at[r, d, c], recv_sem.at[r, d, c],
            device_id={"beam": right if d == 0 else left}, device_id_type=MESH)

    def store_own(ref, c):
        return pltpu.make_async_copy(stage[c].at[mine], part(ref, c), out_sem.at[c])

    def give(ref, c):
        return pltpu.make_async_remote_copy(stage[c].at[theirs], part(ref, c), give_send.at[c], give_recv.at[c], device_id={"beam": sibling}, device_id_type=MESH)

    barrier = pltpu.get_barrier_semaphore()
    for peer in (sibling, left, right):
        pl.semaphore_signal(barrier, inc=1, device_id={"beam": peer}, device_id_type=MESH)

    @pl.when(core == 0)
    def _():
        for c in range(nchunk):
            load_own(k_ref, c).start()

    @pl.when(core == 1)
    def _():
        for c in range(nchunk):
            load_own(v_ref, c).start()

    pl.semaphore_wait(barrier, 3)

    @pl.when(core == 0)
    def _():
        for c in range(nchunk):
            swap(v_ref, c).start()

    @pl.when(core == 1)
    def _():
        for c in range(nchunk):
            swap(k_ref, c).start()

    strip = min(block, 128)

    def build(r, c):
        for d in (0, 1):
            code = table[d * TABLE + r]
            row = jnp.minimum(code, chip_rows - 1)

            def body(i, _):
                at = pl.ds(pl.multiple_of(i * strip, strip), strip)
                x = pool[c][row, at, :]
                for e in range(r):
                    x = jnp.where(code == chip_rows + e, recv[c][2 * e + d, at, :], x)
                send[c][2 * r + d, at, :] = x
                return 0

            lax.fori_loop(0, block // strip, body, 0)
        for d in (0, 1):
            hop(r, d, c).start()

    for c in range(nchunk):
        load_own(k_ref, c).wait()
        swap(k_ref, c).wait_recv()
        build(0, c)
    for r in range(1, rounds):
        for c in range(nchunk):
            for d in (0, 1):
                hop(r - 1, d, c).wait_recv()
            build(r, c)
    for c in range(nchunk):
        for d in (0, 1):
            hop(rounds - 1, d, c).wait_recv()
        for j in range(chip_rows):
            where = table[2 * TABLE + j]
            row = jnp.minimum(where, chip_rows - 1)
            slot = jnp.maximum(where - chip_rows, 0)

            def body(i, _):
                at = pl.ds(pl.multiple_of(i * strip, strip), strip)
                stage[c][j, at, :] = jnp.where(where < chip_rows, pool[c][row, at, :], recv[c][slot, at, :])
                return 0

            lax.fori_loop(0, block // strip, body, 0)

        @pl.when(core == 0)
        def _():
            give(k_out, c).start()
            store_own(k_out, c).start()

        @pl.when(core == 1)
        def _():
            give(v_out, c).start()
            store_own(v_out, c).start()

    for c in range(nchunk):
        swap(k_ref, c).wait_send()
        for r in range(rounds):
            for d in (0, 1):
                hop(r, d, c).wait_send()
        store_own(k_out, c).wait()
        give(k_out, c).wait()


def move_rows(rounds, beams, table, k_rows, v_rows):
    rows, length, lanes = k_rows.shape
    block = length // CHUNKS
    vmem = pltpu.VMEM
    hbm = pl.BlockSpec(memory_space=pl.ANY)
    dtype = k_rows.dtype
    scratch = [vmem((2 * rows, block, lanes), dtype)] * CHUNKS
    scratch += [vmem((2 * rounds, block, lanes), dtype)] * CHUNKS
    scratch += [vmem((2 * rounds, block, lanes), dtype)] * CHUNKS
    scratch += [vmem((2 * rows, block, lanes), dtype)] * CHUNKS
    sem = pltpu.SemaphoreType.DMA
    scratch += [sem((CHUNKS,)), sem((CHUNKS,)), sem((CHUNKS,)), sem((rounds, 2, CHUNKS)), sem((rounds, 2, CHUNKS)), sem((CHUNKS,)), sem((CHUNKS,)), sem((CHUNKS,))]
    out = jax.ShapeDtypeStruct(k_rows.shape, dtype)
    return pl.pallas_call(
        functools.partial(move_kernel, rounds, beams, rows, block),
        out_shape=(out, out),
        in_specs=[pl.BlockSpec(memory_space=pltpu.SMEM), hbm, hbm],
        out_specs=(hbm, hbm),
        scratch_shapes=scratch,
        compiler_params=pltpu.CompilerParams(collective_id=rounds, has_side_effects=True, vmem_limit_bytes=60 * 2**20),
        name=f"move{rounds}",
    )(table, k_rows, v_rows)


def move_any(beams, parent, k_rows, v_rows):
    rows = k_rows.shape[0]
    me = lax.axis_index("beam")
    mine = lax.dynamic_slice(parent.reshape(-1), (me * rows,), (rows,))
    ring = [(i, (i + 1) % beams) for i in range(beams)]

    def step(s, carry):
        k_here, v_here, k_sel, v_sel = carry
        source = lax.rem(me - s + beams, beams)
        hit = (mine // rows == source)[:, None, None]
        local = lax.rem(mine, rows)
        k_sel = jnp.where(hit, jnp.take(k_here, local, axis=0), k_sel)
        v_sel = jnp.where(hit, jnp.take(v_here, local, axis=0), v_sel)
        return lax.ppermute(k_here, "beam", ring), lax.ppermute(v_here, "beam", ring), k_sel, v_sel

    carry = lax.fori_loop(0, beams, step, (k_rows, v_rows, k_rows, v_rows))
    return carry[2], carry[3]


def share_kernel(axis, n, combine, x_ref, out_ref, got, send_sem, recv_sem):
    me = lax.axis_index(axis)
    barrier = pltpu.get_barrier_semaphore()
    peers = [lax.rem(me + s, n) for s in range(1, n)]
    for peer in peers:
        pl.semaphore_signal(barrier, inc=1, device_id={axis: peer}, device_id_type=MESH)
    pl.semaphore_wait(barrier, n - 1)
    copies = []
    for s, peer in enumerate(peers):
        copies.append(pltpu.make_async_remote_copy(x_ref, got.at[s], send_sem.at[s], recv_sem.at[s], device_id={axis: peer}, device_id_type=MESH))
        copies[-1].start()
    for copy in copies:
        copy.wait()
    combine(n, me, x_ref, got, out_ref)


def add_all(n, me, x_ref, got, out_ref):
    total = x_ref[...]
    for s in range(n - 1):
        total = total + got[s]
    out_ref[...] = total


def keep_all(n, me, x_ref, got, out_ref):
    out_ref[0] = x_ref[...]
    for s in range(n - 1):
        out_ref[s + 1] = got[s]


def share(x, axis, n, combine, out_shape, collective_id):
    spec = pl.BlockSpec(memory_space=pltpu.VMEM)
    return pl.pallas_call(
        functools.partial(share_kernel, axis, n, combine),
        out_shape=jax.ShapeDtypeStruct(out_shape, x.dtype),
        in_specs=[spec],
        out_specs=spec,
        scratch_shapes=[pltpu.VMEM((n - 1,) + x.shape, x.dtype), pltpu.SemaphoreType.DMA((n - 1,)), pltpu.SemaphoreType.DMA((n - 1,))],
        compiler_params=pltpu.CompilerParams(collective_id=collective_id, has_side_effects=True),
        name=f"share{collective_id}",
    )(x)


def solution(mesh):
    beams = mesh.shape["beam"]
    models = mesh.shape["model"]
    cache_spec = P(None, ('data', 'beam'), None, 'model', None)
    col_spec = P(None, None, 'model')
    row_spec = P(None, 'model', None)
    in_specs = (P(('data', 'beam'), None), P('data', None), P(), P(('data', 'beam')), cache_spec, cache_spec,
                P(), col_spec, col_spec, col_spec, row_spec, P(), col_spec, col_spec, row_spec, P(), P(None, 'model'))
    out_specs = (cache_spec, cache_spec, P(('data', 'beam'), 'model'))

    def model_sum(x, collective_id):
        if models == 1:
            return x
        return share(x, "model", models, add_all, x.shape, collective_id)

    def local_step(x_embed, parent, position, score, k_cache, v_cache, gain_attn, w_query, w_key, w_value, w_out, gain_mlp, w_gate, w_up, w_down, gain_final, w_vocab):
        rows = x_embed.shape[0]
        _, _, cache_len, heads, head_dim = k_cache.shape
        me = lax.axis_index('beam')
        table, info = make_plan(parent, beams // 2, 2 * rows)
        k_rows = k_cache.reshape(rows, cache_len * heads, head_dim)
        v_rows = v_cache.reshape(rows, cache_len * heads, head_dim)
        branch = jnp.minimum(jnp.maximum(info[0] - ROUND_CHOICES[0], 0), len(ROUND_CHOICES))
        moves = [functools.partial(move_rows, n, beams) for n in ROUND_CHOICES]
        branches = [lambda t, p, k, v, f=f: f(t, k, v) for f in moves] + [lambda t, p, k, v: move_any(beams, p, k, v)]
        k_sel, v_sel = lax.switch(branch, branches, table, parent, k_rows, v_rows)
        k_sel = k_sel.reshape(rows, cache_len, heads, head_dim)
        v_sel = v_sel.reshape(rows, cache_len, heads, head_dim)

        scores = share(jnp.broadcast_to(score[:, None], (rows, 128)), "beam", beams, keep_all, (beams, rows, 128), 10)
        mine = lax.dynamic_slice(parent.reshape(-1), (me * rows,), (rows,))
        slot = lax.rem(me - mine // rows + beams, beams)
        parent_score = scores[slot, lax.rem(mine, rows), 0]

        residual = x_embed.astype(jnp.float32)
        normed = rms_norm(residual, gain_attn[0])
        q_rot = rope_rotate(jnp.dot(normed, w_query[0], preferred_element_type=jnp.float32).reshape(rows, heads, head_dim), position).astype(jnp.bfloat16)
        k_new = rope_rotate(jnp.dot(normed, w_key[0], preferred_element_type=jnp.float32).reshape(rows, heads, head_dim), position).astype(jnp.bfloat16)
        v_new = jnp.dot(normed, w_value[0], preferred_element_type=jnp.float32).astype(jnp.bfloat16).reshape(rows, heads, head_dim)
        here = (jnp.arange(cache_len) == position)[None, :, None, None]
        k_sel = jnp.where(here, k_new[:, None], k_sel)
        v_sel = jnp.where(here, v_new[:, None], v_sel)
        slot_mask = (jnp.arange(cache_len) <= position)[None, None, :]
        logits = jnp.einsum('bkd,bskd->bks', q_rot, k_sel, preferred_element_type=jnp.float32) * head_dim ** -0.5
        logits = jnp.where(slot_mask, logits, -jnp.inf)
        attn_prob = jax.nn.softmax(logits, axis=-1).astype(jnp.bfloat16)
        attn_out = jnp.einsum('bks,bskd->bkd', attn_prob, v_sel, preferred_element_type=jnp.float32).astype(jnp.bfloat16)
        attn_part = jnp.dot(attn_out.reshape(rows, heads * head_dim), w_out[0], preferred_element_type=jnp.float32)
        residual = residual + model_sum(attn_part, 11)
        normed = rms_norm(residual, gain_mlp[0])
        gate_proj = jnp.dot(normed, w_gate[0], preferred_element_type=jnp.float32)
        up_proj = jnp.dot(normed, w_up[0], preferred_element_type=jnp.float32)
        hidden = (jax.nn.silu(gate_proj) * up_proj).astype(jnp.bfloat16)
        residual = residual + model_sum(jnp.dot(hidden, w_down[0], preferred_element_type=jnp.float32), 12)
        logits = jnp.dot(rms_norm(residual, gain_final), w_vocab, preferred_element_type=jnp.float32)
        top = jnp.max(logits, axis=-1, keepdims=True)
        mass = jnp.sum(jnp.exp(logits - top), axis=-1, keepdims=True)
        if models > 1:
            stats = jnp.concatenate([jnp.broadcast_to(top, (rows, 128)), jnp.broadcast_to(mass, (rows, 128))], axis=0)
            stats = share(stats, "model", models, keep_all, (models,) + stats.shape, 13)
            tops = stats[:, :rows, :1]
            masses = stats[:, rows:, :1]
            top = jnp.max(tops, axis=0)
            mass = jnp.sum(masses * jnp.exp(tops - top), axis=0)
        candidates = parent_score[:, None] + (logits - top - jnp.log(mass))
        return k_sel[None], v_sel[None], candidates

    return jax.shard_map(local_step, mesh=mesh, in_specs=in_specs, out_specs=out_specs, check_vma=False)
```

```python
import functools
import types

import jax
import jax.numpy as jnp
from jax import lax
from jax.experimental import pallas as pl
from jax.experimental.pallas import tpu as pltpu
from jax.sharding import PartitionSpec as P

NORM_EPS = 1e-6
ROPE_BASE = 10000.0
MESH = pl.DeviceIdType.MESH
CHUNKS = 4
TABLE = 24
ROUND_CHOICES = (3, 4)
W_BUFFERS = 4
SIDES = (0, 1)
LANES = 128
VMEM_LIMIT = 66 * 10**6


def plan_kernel(chips, chip_rows, parent_ref, table_ref, info_ref, need, via, hop1, hop2, load, own, two):
    total = chips * chip_rows
    my_chip = lax.axis_index("beam") // 2
    row_bits, chip_mask = chip_rows.bit_length() - 1, chips - 1

    def each(n, body):
        lax.fori_loop(0, n, lambda i, _: (body(i), 0)[1], 0, unroll=4)

    def clear_rows(q):
        need[q] = 0
        via[q] = 0
        hop1[q] = 0
        hop1[total + q] = 0
        hop2[q] = 0

    def clear_links(i):
        load[i] = 0
        own[i] = 0
        two[i] = 0

    def clear_table(i):
        table_ref[i] = 0

    each(total, clear_rows)
    each(2 * chips, clear_links)
    each(2 * TABLE + chip_rows, clear_table)

    def mark(b):
        q = parent_ref[0, b]
        dist = ((b >> row_bits) - (q >> row_bits)) & chip_mask
        need[q] = need[q] | (1 << dist)

    each(total, mark)

    def bits(q):
        n = need[q]
        return (n >> 1) & 1, (n >> 2) & 1, (n >> 3) & 1

    def up(c):
        return (c + 1) & chip_mask

    def down(c):
        return chips + ((c - 1) & chip_mask)

    def fixed(q):
        c = q >> row_bits
        a, b, d = bits(q)
        plus = b * a * (1 - d)
        minus = b * d * (1 - a)
        own[c] = own[c] + a
        own[chips + c] = own[chips + c] + d
        load[c] = load[c] + a
        load[chips + c] = load[chips + c] + d
        load[up(c)] = load[up(c)] + plus
        load[down(c)] = load[down(c)] + minus
        via[q] = plus + 2 * minus

    each(total, fixed)

    def free(q):
        c = q >> row_bits
        a, b, d = bits(q)
        flex = b * (1 - (a ^ d))
        cost_plus = jnp.maximum(load[c] + 1 - a, load[up(c)] + 1)
        cost_minus = jnp.maximum(load[chips + c] + 1 - d, load[down(c)] + 1)
        side = (cost_plus <= cost_minus).astype(jnp.int32)
        plus = flex * side
        minus = flex * (1 - side)
        load[c] = load[c] + plus * (1 - a)
        own[c] = own[c] + plus * (1 - a)
        load[chips + c] = load[chips + c] + minus * (1 - d)
        own[chips + c] = own[chips + c] + minus * (1 - d)
        load[up(c)] = load[up(c)] + plus
        load[down(c)] = load[down(c)] + minus
        via[q] = via[q] + plus + 2 * minus

    each(total, free)

    def first_two(q):
        c = q >> row_bits
        v = via[q]
        plus = v & 1
        minus = v >> 1
        hop1[q] = two[c] * plus
        hop1[total + q] = two[chips + c] * minus
        two[c] = two[c] + plus
        two[chips + c] = two[chips + c] + minus

    each(total, first_two)

    def restart(i):
        load[i] = two[i]

    each(2 * chips, restart)

    def rest(q, rounds):
        c = q >> row_bits
        a, b, d = bits(q)
        v = via[q]
        plus = v & 1
        minus = v >> 1
        a1 = a * (1 - plus)
        d1 = d * (1 - minus)
        hop1[q] = hop1[q] + a1 * load[c]
        hop1[total + q] = hop1[total + q] + d1 * load[chips + c]
        load[c] = load[c] + a1
        load[chips + c] = load[chips + c] + d1
        onward = plus * (jnp.maximum(own[up(c)], 1) + hop1[q]) + minus * (jnp.maximum(own[down(c)], 1) + hop1[total + q])
        hop2[q] = onward
        used = jnp.maximum(onward + 1, jnp.maximum((hop1[q] + 1) * (a | plus), (hop1[total + q] + 1) * (d | minus)))
        return jnp.maximum(rounds, used * jnp.minimum(need[q] >> 1, 1))

    info_ref[0] = lax.fori_loop(0, total, rest, 0, unroll=4)

    def fill(q):
        c = q >> row_bits
        a, b, d = bits(q)
        v = via[q]

        @pl.when((c == my_chip) & ((a | (v & 1)) == 1))
        def _():
            table_ref[hop1[q]] = q & (chip_rows - 1)

        @pl.when((c == my_chip) & ((d | (v >> 1)) == 1))
        def _():
            table_ref[TABLE + hop1[total + q]] = q & (chip_rows - 1)

        @pl.when((up(c) == my_chip) & ((v & 1) == 1))
        def _():
            table_ref[hop2[q]] = chip_rows + hop1[q]

        @pl.when((down(c) == chips + my_chip) & ((v >> 1) == 1))
        def _():
            table_ref[TABLE + hop2[q]] = chip_rows + hop1[total + q]

    each(total, fill)

    def place(j):
        q = parent_ref[0, my_chip * chip_rows + j]
        dist = (my_chip - (q >> row_bits)) & chip_mask
        v = via[q]
        at_plus = chip_rows + 2 * jnp.where(dist == 1, hop1[q], hop2[q])
        at_minus = chip_rows + 2 * jnp.where(dist == 3, hop1[total + q], hop2[q]) + 1
        from_plus = (dist == 1) | ((dist == 2) & ((v & 1) == 1))
        where = jnp.where(from_plus, at_plus, at_minus)
        table_ref[2 * TABLE + j] = jnp.where(dist == 0, q & (chip_rows - 1), where)

    each(chip_rows, place)


def make_plan(parent, chips, chip_rows):
    total = chips * chip_rows
    smem = pl.BlockSpec(memory_space=pltpu.SMEM)
    return pl.pallas_call(
        functools.partial(plan_kernel, chips, chip_rows),
        out_shape=(jax.ShapeDtypeStruct((2 * TABLE + chip_rows,), jnp.int32), jax.ShapeDtypeStruct((1,), jnp.int32)),
        in_specs=[smem],
        out_specs=(smem, smem),
        scratch_shapes=[
            pltpu.SMEM((total,), jnp.int32),
            pltpu.SMEM((total,), jnp.int32),
            pltpu.SMEM((2 * total,), jnp.int32),
            pltpu.SMEM((total,), jnp.int32),
            pltpu.SMEM((2 * chips,), jnp.int32),
            pltpu.SMEM((2 * chips,), jnp.int32),
            pltpu.SMEM((2 * chips,), jnp.int32),
        ],
        name="plan",
    )(parent)


def loop(n, body):
    def step(i, carry):
        body(i)
        return carry

    lax.fori_loop(0, n, step, 0)


class Copies:
    def __init__(self, copies):
        self.copies = copies

    def start(self):
        for copy in self.copies:
            copy.start()

    def wait(self):
        for copy in self.copies:
            copy.wait()


def step_kernel(rounds, beams, models, rows, heads, slots, d_model, ff, vocab, names, *refs):
    r = types.SimpleNamespace(**dict(zip(names, refs)))
    table, pos_ref, parent_ref = r.table, r.pos, r.parent
    k_ref, v_ref, k_out, v_out = r.k, r.v, r.k_out, r.v_out
    f32, bf16 = jnp.float32, jnp.bfloat16
    nchunk = CHUNKS
    block = slots * heads // nchunk
    span = slots // nchunk
    chips = beams // 2
    pair = 2 * rows
    lanes = LANES
    me = lax.axis_index("beam")
    core = lax.rem(me, 2)
    chip = me // 2
    is_k, is_v = core == 0, core == 1
    all_half, all_heads = pl.ds(0, d_model // 2), pl.ds(0, heads * LANES)
    sibling = me + 1 - 2 * core
    right = lax.rem(me + 2, beams)
    left = lax.rem(me + beams - 2, beams)
    model = lax.axis_index("model")
    mine = pl.ds(core * rows, rows)
    theirs = pl.ds((1 - core) * rows, rows)
    lane_iota = lax.broadcasted_iota(jnp.int32, (1, lanes), 1)
    pool, recv, send, stage, other = r.pool, r.recv, r.send, r.stage, r.other
    half = d_model // 2

    def to(peer):
        return dict(device_id={"beam": peer}, device_id_type=MESH)

    def across(m, peer):
        return dict(device_id={"model": m, "beam": peer}, device_id_type=MESH)

    def part(ref, c):
        return ref.at[:, pl.ds(c * block, block), :]

    def load_own(ref, c):
        return pltpu.make_async_copy(part(ref, c), pool[c].at[mine], r.pool_sem.at[c])

    def load_other(ref, c):
        return pltpu.make_async_copy(part(ref, c), other[c], r.other_sem.at[c])

    def swap(ref, c):
        return pltpu.make_async_remote_copy(part(ref, c), pool[c].at[mine], r.swap_send.at[c], r.swap_recv.at[c], **to(sibling))

    def hop(n, d, c):
        return pltpu.make_async_remote_copy(
            send[c].at[2 * n + d], recv[c].at[2 * n + d], r.hop_send.at[n, d, c], r.hop_recv.at[n, d, c], **to(right if d == 0 else left))

    def store_own(ref, c):
        return pltpu.make_async_copy(stage[c].at[mine], part(ref, c), r.out_sem.at[c])

    def give(ref, c):
        return pltpu.make_async_remote_copy(stage[c].at[theirs], part(ref, c), r.give_send.at[c], r.give_recv.at[c], **to(sibling))

    w_count = len(r.wbuf)
    groups = []

    def group(blocks):
        groups.append(blocks)

    for ref in (r.w_query, r.w_key, r.w_value):
        width = heads * lanes // 2
        group([(ref, pl.ds(1024 * i, 1024), pl.ds(core * width, width), pl.ds(0, 1024), pl.ds(i * width, width)) for i in range(d_model // 1024)])
    group([(r.w_out, all_heads, pl.ds(core * half, half), all_heads, all_half)])
    ff_core = (ff + 127) // 256 * 128
    ff_full = ff_core // 256
    ff_last = ff_core - 256 * ff_full
    ff_skip = 2 * ff_core - ff
    for i in range(ff_full + 1):
        n = 256 if i < ff_full else ff_last
        first = core * (ff_core - (ff_skip if i == ff_full else 0)) + 256 * i
        first = pl.multiple_of(first, 8)
        group([(ref, pl.ds(first, n), pl.ds(j * half, half), pl.ds(512 * j + n * u, n), all_half) for u, ref in enumerate((r.w_gate, r.w_up)) for j in range(2)])
    down_rows = []
    for i in range(0, 2 * ff_core, 1024):
        n = min(1024, 2 * ff_core - i)
        down_rows.append((i, n))
        blocks = [(i, n, 0)]
        if i + n > 2 * ff_core - ff_last:
            blocks = [(i, n - ff_last, 0), (ff - ff_last, ff_last, n - ff_last)]
        group([(r.w_down, pl.ds(a, b), pl.ds(core * half, half), pl.ds(c, b), all_half) for a, b, c in blocks])
    voc_core = (vocab + 1023) // 1024 * 512
    voc_groups = voc_core // 512
    voc_skip = 2 * voc_core - vocab
    for i in range(voc_groups):
        first = core * (voc_core - (voc_skip if i == voc_groups - 1 else 0)) + 512 * i
        first = pl.multiple_of(first, 8)
        group([(r.w_vocab, pl.ds(first, 512), pl.ds(j * half, half), pl.ds(512 * j, 512), all_half) for j in range(2)])

    def group_copies(g):
        return [pltpu.make_async_copy(ref.at[a, b], r.wbuf[g % w_count].at[c, e], r.w_sem.at[g, i]) for i, (ref, a, b, c, e) in enumerate(groups[g])]

    def load(g):
        if g < len(groups):
            for copy in group_copies(g):
                copy.start()

    taken = [0]

    def with_group(use):
        g = taken[0]
        taken[0] += 1
        for copy in group_copies(g):
            copy.wait()
        use(r.wbuf[g % w_count])
        load(g + w_count)

    barrier = pltpu.get_barrier_semaphore()
    peers = [lax.rem(me + s, beams) for s in range(1, beams)]
    model_peers = [lax.rem(model + s, models) for s in range(1, models)]
    for peer in peers:
        pl.semaphore_signal(barrier, **to(peer))
    for m in model_peers:
        for peer in (me, sibling):
            pl.semaphore_signal(barrier, **across(m, peer))

    load(0)

    @pl.when(is_k)
    def _():
        for c in range(nchunk):
            load_own(k_ref, c).start()

    @pl.when(is_v)
    def _():
        for c in range(nchunk):
            load_own(v_ref, c).start()

    for g in range(1, w_count):
        load(g)

    @pl.when(is_k)
    def _():
        for c in range(nchunk):
            load_other(v_ref, c).start()

    @pl.when(is_v)
    def _():
        for c in range(nchunk):
            load_other(k_ref, c).start()

    pl.semaphore_wait(barrier, beams - 1 + 2 * (models - 1))

    x_swap = pltpu.make_async_remote_copy(r.x, r.x_got, r.pair_send.at[0], r.pair_recv.at[0], **to(sibling))
    x_swap.start()

    @pl.when(is_k)
    def _():
        for c in range(nchunk):
            swap(v_ref, c).start()

    @pl.when(is_v)
    def _():
        for c in range(nchunk):
            swap(k_ref, c).start()

    strip = min(block, 128)

    def build(n, c):
        for d in SIDES:
            code = table[d * TABLE + n]
            row = jnp.minimum(code, pair - 1)

            def body(i):
                at = pl.ds(pl.multiple_of(i * strip, strip), strip)
                x = pool[c][row, at, :]
                for e in range(n):
                    x = jnp.where(code == pair + e, recv[c][2 * e + d, at, :], x)
                send[c][2 * n + d, at, :] = x

            loop(block // strip, body)
        for d in SIDES:
            hop(n, d, c).start()

    waited = set()

    def have_own(c):
        if c not in waited:
            waited.add(c)
            load_own(k_ref, c).wait()

    def first_round(c):
        have_own(c)
        swap(k_ref, c).wait_recv()
        build(0, c)

    def later_round(n, c):
        for d in SIDES:
            hop(n - 1, d, c).wait_recv()
        build(n, c)

    def finish(c):
        for d in SIDES:
            hop(rounds - 1, d, c).wait_recv()
        position = pos_ref[0]
        for j in range(pair):
            where = table[2 * TABLE + j]
            row = jnp.minimum(where, pair - 1)
            slot = jnp.clip(where - pair, 0, 2 * rounds - 1)
            fresh = r.fresh[j]

            def body(i):
                at = pl.ds(pl.multiple_of(i * strip, strip), strip)
                x = jnp.where(where < pair, pool[c][row, at, :], recv[c][slot, at, :])
                here = (lax.broadcasted_iota(jnp.int32, (strip, lanes), 0) + i * strip) // heads + c * span
                new = jnp.concatenate([fresh] * (strip // heads))
                stage[c][j, at, :] = jnp.where(here == position, new, x.astype(f32)).astype(bf16)

            loop(block // strip, body)

        @pl.when(is_k)
        def _():
            give(k_out, c).start()
            store_own(k_out, c).start()

        @pl.when(is_v)
        def _():
            give(v_out, c).start()
            store_own(v_out, c).start()

    todo = [functools.partial(first_round, c) for c in range(nchunk)]
    todo += [functools.partial(later_round, n, c) for n in range(1, rounds) for c in range(nchunk)]
    todo += [functools.partial(finish, c) for c in range(nchunk)]

    def serve(n=1):
        for _ in range(n):
            if todo:
                todo.pop(0)()

    res = r.res

    def normed(gain_ref):
        x = res[...]
        inv = lax.rsqrt(jnp.mean(x * x, axis=-1, keepdims=True) + NORM_EPS)
        r.h[...] = (x * inv * gain_ref[...].astype(f32)).astype(bf16)

    def dot(a, b):
        return jnp.dot(a, b, preferred_element_type=f32)

    def dot_halves(w, n):
        def body(j, x):
            a = h[:, pl.ds(pl.multiple_of(j * half, lanes), half)]
            b = w[pl.ds(pl.multiple_of(j * 512, 512), n), :]
            return x + lax.dot_general(a, b, (((1,), (1,)), ((), ())), preferred_element_type=f32)

        return lax.fori_loop(0, 2, body, jnp.zeros((pair, n), f32))

    def exchange_model(part_ref, got_ref, phase):
        if models == 1:
            return part_ref[...]
        copies = [
            pltpu.make_async_remote_copy(part_ref, got_ref.at[model], r.model_send.at[phase, s], r.model_recv.at[phase, s], **across(m, me))
            for s, m in enumerate(model_peers)]
        for copy in copies:
            copy.start()
        got_ref[model] = part_ref[...]
        for copy in copies:
            copy.wait()
        total = got_ref[0]
        for m in range(1, models):
            total = total + got_ref[m]
        return total

    serve()
    x_swap.wait()

    @pl.when(is_k)
    def _():
        res[0:rows, :] = r.x[...].astype(f32)
        res[rows:pair, :] = r.x_got[...].astype(f32)

    @pl.when(is_v)
    def _():
        res[0:rows, :] = r.x_got[...].astype(f32)
        res[rows:pair, :] = r.x[...].astype(f32)

    normed(r.gain_attn)
    h = r.h
    head_half = heads // 2
    width = head_half * lanes
    qkv = r.qkv
    for kind in range(3):
        def use(w, kind=kind):
            z = dot(h[:, 0:1024], w[:, 0:width])
            for i in range(1, d_model // 1024):
                z = z + dot(h[:, 1024 * i : 1024 * (i + 1)], w[:, i * width : (i + 1) * width])
            for n in range(head_half):
                y = z[:, n * lanes : (n + 1) * lanes]
                if kind < 2:
                    y = y * r.rope[0:1, :] + pltpu.roll(y, lanes // 2, 1) * r.rope[1:2, :]
                qkv[kind, n] = y.astype(bf16)
        with_group(use)

    qkv_all = r.qkv_all
    to_parents = Copies(
        [pltpu.make_async_remote_copy(qkv, qkv_all.at[me], r.beam_send.at[0, s], r.beam_recv.at[0, s], **to(p)) for s, p in enumerate(peers)]
        + [pltpu.make_async_remote_copy(r.score, r.scores.at[me], r.beam_send.at[1, s], r.beam_recv.at[1, s], **to(p)) for s, p in enumerate(peers)])
    to_parents.start()
    qkv_all[me] = qkv[...]
    r.scores[me] = r.score[...]
    serve(2)
    to_parents.wait()

    cat = r.cat
    for kind in range(3):
        for n in range(heads):
            for x in range(chips):
                at = n * beams * rows + x * pair
                cat[kind, at : at + pair, :] = qkv_all[2 * x + n // head_half, kind, n % head_half].astype(f32)
    for j in range(pair):
        at = pl.ds(chip * pair + j, heads, stride=beams * rows)
        r.fresh[j] = jnp.where(is_k, cat[1, at, :], cat[2, at, :])

    query_t = cat[0].T.astype(bf16)
    new_k = cat[1].astype(bf16)
    total_cols = heads * beams * rows
    tiles = total_cols // lanes
    heads_tile = heads // tiles
    lane_head = lane_iota // (beams * rows)
    prow = r.prow
    spread = r.spread
    logit = r.logit
    position = pos_ref[0]

    def own_rows(c, p, kind):
        a = pool[c][core * rows + p]
        b = other[c][p]
        return jnp.where(core == kind, a, b)

    def score_chunk(c):
        have_own(c)
        load_other(k_ref, c).wait()

        def body(p):
            full = dot(own_rows(c, p, 0), query_t)
            for t in range(tiles):
                spread[t][...] = full[:, t * lanes : (t + 1) * lanes]
            for t in range(tiles):
                here = prow[:, t * lanes : (t + 1) * lanes] == me * rows + p
                at = pl.ds(c * span, span)
                x = logit[t][at, :]
                for n in range(heads_tile):
                    got = spread[t][pl.ds(t * heads_tile + n, span, stride=heads), :]
                    x = jnp.where(here & (lane_head == n), got, x)
                logit[t][at, :] = x

        loop(rows, body)

    for t in range(tiles):
        logit[t][...] = jnp.zeros_like(logit[t])
    self_full = dot(new_k, query_t)
    scale = lanes ** -0.5
    for c in range(nchunk):
        score_chunk(c)
        serve(c == nchunk - 1)
    slot_index = lax.broadcasted_iota(jnp.int32, (slots, lanes), 0)
    self_prob = []
    for t in range(tiles):
        diag = lax.broadcasted_iota(jnp.int32, (total_cols, lanes), 0) == lax.broadcasted_iota(jnp.int32, (total_cols, lanes), 1) + t * lanes
        self_row = jnp.sum(jnp.where(diag, self_full[:, t * lanes : (t + 1) * lanes], 0.0), axis=0, keepdims=True)
        x = jnp.where(slot_index == position, self_row, logit[t][...]) * scale
        x = jnp.where(slot_index <= position, x, -jnp.inf)
        e = jnp.exp(x - jnp.max(x, axis=0, keepdims=True))
        prob = e / jnp.sum(e, axis=0, keepdims=True)
        logit[t][...] = jnp.where(slot_index == position, 0.0, prob)
        self_prob.append(jnp.sum(jnp.where(slot_index == position, prob, 0.0), axis=0, keepdims=True))
    for t in range(tiles):
        spread[t][...] = jnp.zeros_like(spread[t])
    out_t = r.out_t
    out_t[...] = cat[2].T * jnp.concatenate(self_prob, axis=1).astype(bf16).astype(f32)

    def value_chunk(c):
        def body(p):
            for t in range(tiles):
                here = prow[:, t * lanes : (t + 1) * lanes] == me * rows + p
                x = logit[t][pl.ds(c * span, span), :]
                for n in range(heads_tile):
                    spread[t][pl.ds(t * heads_tile + n, span, stride=heads), :] = jnp.where(here & (lane_head == n), x, 0.0)
            prob = jnp.concatenate([spread[t][...].astype(bf16) for t in range(tiles)], axis=1)
            out_t[...] += lax.dot_general(own_rows(c, p, 1), prob, (((0,), (0,)), ((), ())), preferred_element_type=f32)

        loop(rows, body)

    for c in range(nchunk):
        value_chunk(c)
    local = prow[...] // rows == me
    o_rows = jnp.where(local, out_t[...], 0.0).T
    o_send, o_got = r.o_send, r.o_got
    for x in range(chips):
        for n in range(heads):
            at = n * beams * rows + x * pair
            o_send[x, n] = o_rows[at : at + pair, :].astype(bf16)
    back = Copies([
        pltpu.make_async_remote_copy(o_send.at[lax.rem(me + s, beams) // 2], o_got.at[me], r.beam_send.at[2, s - 1], r.beam_recv.at[2, s - 1], **to(lax.rem(me + s, beams)))
        for s in range(1, beams)])
    back.start()
    o_got[me] = o_send[chip]
    serve(3)
    back.wait()
    for n in range(heads):
        x = o_got[0, n].astype(f32)
        for s in range(1, beams):
            x = x + o_got[s, n].astype(f32)
        r.o[:, n * lanes : (n + 1) * lanes] = x.astype(bf16)

    part_sum, model_got, res_half, res_got = r.part, r.model_got, r.res_half, r.res_got

    def add_to_residual(phase):
        total = exchange_model(part_sum, model_got.at[phase] if models > 1 else None, phase)
        col = pl.ds(pl.multiple_of(core * half, lanes), half)
        other_col = pl.ds(pl.multiple_of((1 - core) * half, lanes), half)
        fresh = res[:, col] + total
        res_half[phase] = fresh
        trade = pltpu.make_async_remote_copy(res_half.at[phase], res_got.at[phase], r.pair_send.at[1 + phase], r.pair_recv.at[1 + phase], **to(sibling))
        trade.start()
        res[:, col] = fresh
        trade.wait()
        res[:, other_col] = res_got[phase]

    def use_out(w):
        part_sum[0] = dot(r.o[...], w[0 : heads * lanes, :])
    with_group(use_out)
    serve()
    part_sum_ref = part_sum
    part_sum = part_sum_ref.at[0]
    add_to_residual(0)
    normed(r.gain_mlp)

    g_own, g_got, g_all = r.g_own, r.g_got, r.g_all
    for i in range(ff_full + 1):
        n = 256 if i < ff_full else ff_last

        def use(w, i=i, n=n):
            z = dot_halves(w, 2 * n)
            gate, up = z[:, :n], z[:, n:]
            y = jax.nn.silu(gate) * up
            if i == ff_full and ff_skip:
                y = jnp.where(is_v & (lax.broadcasted_iota(jnp.int32, (1, n), 1) < ff_skip), 0.0, y)
            g_own[:, 256 * i : 256 * i + n] = y.astype(bf16)
        with_group(use)
        serve(i == 2)
    g_trade = pltpu.make_async_remote_copy(g_own, g_got, r.pair_send.at[3], r.pair_recv.at[3], **to(sibling))
    g_trade.start()
    g_all[:, pl.ds(pl.multiple_of(core * ff_core, lanes), ff_core)] = g_own[...]
    serve()
    g_trade.wait()
    g_all[:, pl.ds(pl.multiple_of((1 - core) * ff_core, lanes), ff_core)] = g_got[...]
    part_sum = part_sum_ref.at[1]
    for at, n in down_rows:
        def use(w, at=at, n=n):
            x = dot(g_all[:, at : at + n], w[0:n, :])
            part_sum[...] = x if at == 0 else part_sum[...] + x
        with_group(use)
    serve()
    add_to_residual(1)
    normed(r.gain_final)

    word = r.word
    for i in range(voc_groups):
        def use(w, i=i):
            word[:, 512 * i : 512 * (i + 1)] = dot_halves(w, 512)
        with_group(use)
        serve(i % 4 == 1)
    word_send, word_got = r.word_send, r.word_got
    x = word[...]
    word_send[0] = x[0:rows]
    word_send[1] = x[rows:pair]
    word_trade = pltpu.make_async_remote_copy(word_send.at[1 - core], word_got, r.pair_send.at[4], r.pair_recv.at[4], **to(sibling))
    word_trade.start()
    col = lax.broadcasted_iota(jnp.int32, (1, voc_core), 1)
    twice = is_v & (col >= voc_core - 512) & (col < voc_core - 512 + voc_skip)
    x = jnp.where(twice, -jnp.inf, x)
    top = jnp.max(x, axis=-1, keepdims=True)
    mass = jnp.sum(jnp.exp(x - top), axis=-1, keepdims=True)
    stat, stats = r.stat, r.stats
    stat[0] = jnp.broadcast_to(top, (pair, lanes))
    stat[1] = jnp.broadcast_to(mass, (pair, lanes))
    mates = [(m, p) for m in [model] + model_peers for p in (me, sibling)][1:]
    told = Copies([
        pltpu.make_async_remote_copy(stat, stats.at[2 * model + core], r.stat_send.at[i], r.stat_recv.at[i], **across(m, p))
        for i, (m, p) in enumerate(mates)])
    told.start()
    stats[2 * model + core] = stat[...]
    told.wait()
    top = stats[0, 0]
    for i in range(1, 2 * models):
        top = jnp.maximum(top, stats[i, 0])
    mass = stats[0, 1] * jnp.exp(stats[0, 0] - top)
    for i in range(1, 2 * models):
        mass = mass + stats[i, 1] * jnp.exp(stats[i, 0] - top)
    r.stat[0] = top
    r.stat[1] = jnp.log(mass)
    word_trade.wait()
    both = r.word_out
    for j in range(rows):
        q = parent_ref[0, me * rows + j]
        base = r.scores[q // rows, pl.ds(lax.rem(q, rows), 1), :][:, 0:1]
        at = pl.ds(core * rows + j, 1)
        shift = stat[0, at, 0:1]
        log_mass = stat[1, at, 0:1]
        own = word_send[core, j : j + 1, :]
        theirs_ = word_got[j : j + 1, :]
        both[core, j : j + 1, :] = base + (own - shift - log_mass)
        both[1 - core, j : j + 1, :] = base + (theirs_ - shift - log_mass)

    serve(len(todo))
    for c in range(nchunk):
        swap(k_ref, c).wait_send()
        for n in range(rounds):
            for d in SIDES:
                hop(n, d, c).wait_send()
        store_own(k_out, c).wait()
        give(k_out, c).wait()


def run_step(rounds, beams, models, table, pos, parent, score, rope, prow, x, k_rows, v_rows, gains, weights):
    rows, length, lanes = k_rows.shape
    weights_ = types.SimpleNamespace(**weights)
    d_model = x.shape[1]
    heads = weights_.w_query.shape[1] // lanes
    slots = length // heads
    ff = weights_.w_down.shape[0]
    vocab = weights_.w_vocab.shape[0]
    block = length // CHUNKS
    pair = 2 * rows
    half = d_model // 2
    chips = beams // 2
    cols = heads * beams * rows
    bf16, f32 = jnp.bfloat16, jnp.float32
    vmem, dma = pltpu.VMEM, pltpu.SemaphoreType.DMA
    smem, hbm, ram = (pl.BlockSpec(memory_space=s) for s in (pltpu.SMEM, pl.ANY, pltpu.VMEM))
    voc_core = (vocab + 1023) // 1024 * 512
    ff_core = (ff + 127) // 256 * 128
    n_groups = 4 + ff_core // 256 + 1 + -(-2 * ff_core // 1024) + voc_core // 512
    ins = dict(table=(table, smem), pos=(pos, smem), parent=(parent, smem), score=(score, ram), rope=(rope, ram), prow=(prow, ram),
               x=(x, ram), k=(k_rows, hbm), v=(v_rows, hbm))
    ins.update({name: (a, ram) for name, a in gains.items()})
    ins.update({name: (a, hbm) for name, a in weights.items()})
    outs = dict(k_out=(jax.ShapeDtypeStruct(k_rows.shape, bf16), hbm), v_out=(jax.ShapeDtypeStruct(k_rows.shape, bf16), hbm),
                word_out=(jax.ShapeDtypeStruct((2, rows, voc_core), f32), ram))
    scratch = dict(
        pool=[vmem((pair, block, lanes), bf16)] * CHUNKS,
        recv=[vmem((2 * rounds, block, lanes), bf16)] * CHUNKS,
        send=[vmem((2 * rounds, block, lanes), bf16)] * CHUNKS,
        stage=[vmem((pair, block, lanes), bf16)] * CHUNKS,
        other=[vmem((rows, block, lanes), bf16)] * CHUNKS,
        wbuf=[vmem((1024, half), bf16)] * W_BUFFERS,
        spread=[vmem((block, lanes), f32)] * (cols // lanes),
        logit=[vmem((slots, lanes), f32)] * (cols // lanes),
        x_got=vmem(x.shape, bf16),
        res=vmem((pair, d_model), f32),
        h=vmem((pair, d_model), bf16),
        qkv=vmem((3, heads // 2, pair, lanes), bf16),
        qkv_all=vmem((beams, 3, heads // 2, pair, lanes), bf16),
        scores=vmem((beams, rows, lanes), f32),
        cat=vmem((3, cols, lanes), f32),
        fresh=vmem((pair, heads, lanes), f32),
        out_t=vmem((lanes, cols), f32),
        o_send=vmem((chips, heads, pair, lanes), bf16),
        o_got=vmem((beams, heads, pair, lanes), bf16),
        o=vmem((pair, heads * lanes), bf16),
        part=vmem((2, pair, half), f32),
        model_got=vmem((2, models, pair, half), f32),
        res_half=vmem((2, pair, half), f32),
        res_got=vmem((2, pair, half), f32),
        g_own=vmem((pair, ff_core), bf16),
        g_got=vmem((pair, ff_core), bf16),
        g_all=vmem((pair, 2 * ff_core), bf16),
        word=vmem((pair, voc_core), f32),
        word_send=vmem((2, rows, voc_core), f32),
        word_got=vmem((rows, voc_core), f32),
        stat=vmem((2, pair, lanes), f32),
        stats=vmem((2 * models, 2, pair, lanes), f32),
        w_sem=dma((n_groups, 4)),
        pool_sem=dma((CHUNKS,)), other_sem=dma((CHUNKS,)), swap_send=dma((CHUNKS,)), swap_recv=dma((CHUNKS,)),
        hop_send=dma((rounds, 2, CHUNKS)), hop_recv=dma((rounds, 2, CHUNKS)),
        out_sem=dma((CHUNKS,)), give_send=dma((CHUNKS,)), give_recv=dma((CHUNKS,)),
        pair_send=dma((5,)), pair_recv=dma((5,)),
        beam_send=dma((3, beams)), beam_recv=dma((3, beams)),
        model_send=dma((2, models)), model_recv=dma((2, models)),
        stat_send=dma((2 * models,)), stat_recv=dma((2 * models,)),
    )
    flat, places = [], {}
    for name, s in scratch.items():
        many = isinstance(s, list)
        places[name] = (len(flat), len(s) if many else None)
        flat += s if many else [s]
    first = list(ins) + list(outs)

    def kernel(*refs):
        named = list(refs[: len(first)])
        rest = refs[len(first) :]
        for start, count in places.values():
            named.append(rest[start] if count is None else list(rest[start : start + count]))
        step_kernel(rounds, beams, models, rows, heads, slots, d_model, ff, vocab, first + list(places), *named)

    return pl.pallas_call(
        kernel,
        out_shape=tuple(s for s, _ in outs.values()),
        in_specs=[s for _, s in ins.values()],
        out_specs=tuple(s for _, s in outs.values()),
        scratch_shapes=flat,
        compiler_params=pltpu.CompilerParams(collective_id=rounds, has_side_effects=True, vmem_limit_bytes=VMEM_LIMIT),
        name=f"step{rounds}",
    )(*[a for a, _ in ins.values()])


def copy_kernel(pieces, a_ref, b_ref, a_out, b_out, buf, in_sem, out_sem):
    rows, length, _ = a_ref.shape
    per = rows // pieces
    jobs = [(src, dst, i) for i in range(pieces) for src, dst in ((a_ref, a_out), (b_ref, b_out))]

    def get(n):
        src, _, i = jobs[n]
        return pltpu.make_async_copy(src.at[pl.ds(i * per, per)], buf.at[n], in_sem.at[n])

    def put(n):
        _, dst, i = jobs[n]
        return pltpu.make_async_copy(buf.at[n], dst.at[pl.ds(i * per, per)], out_sem.at[n])

    for n in range(len(jobs)):
        get(n).start()
    for n in range(len(jobs)):
        get(n).wait()
        put(n).start()
    for n in range(len(jobs)):
        put(n).wait()


def settle(a, b):
    rows, length, lanes = a.shape
    hbm = pl.BlockSpec(memory_space=pl.ANY)
    out = jax.ShapeDtypeStruct(a.shape, a.dtype)
    return pl.pallas_call(
        functools.partial(copy_kernel, rows),
        out_shape=(out, out),
        in_specs=[hbm, hbm],
        out_specs=(hbm, hbm),
        scratch_shapes=[pltpu.VMEM((2 * rows, 1, length, lanes), a.dtype), pltpu.SemaphoreType.DMA((2 * rows,)), pltpu.SemaphoreType.DMA((2 * rows,))],
        name="settle",
    )(a, b)


def move_any(beams, heads, parent, position, k_rows, v_rows, k_new, v_new):
    rows, length, _ = k_rows.shape
    me = lax.axis_index("beam")
    mine = lax.dynamic_slice(parent.reshape(-1), (me * rows,), (rows,))
    local = lax.rem(mine, rows)
    ring = [(i, (i + 1) % beams) for i in range(beams)]

    def choose(source, here, chosen):
        hit = (mine // rows == source)[:, None, None]
        return jnp.where(hit, jnp.take(here, local, axis=0), chosen)

    def step(s, carry):
        k_here, v_here, k_sel, v_sel = carry
        source = lax.rem(me - s + beams, beams)
        k_sel, v_sel = choose(source, k_here, k_sel), choose(source, v_here, v_sel)
        return lax.ppermute(k_here, "beam", ring), lax.ppermute(v_here, "beam", ring), k_sel, v_sel

    carry = (lax.ppermute(k_rows, "beam", ring), lax.ppermute(v_rows, "beam", ring), choose(me, k_rows, k_new), choose(me, v_rows, v_new))
    carry = lax.fori_loop(1, beams, step, carry)
    written = (jnp.arange(length) // heads == position)[None, :, None]
    return jnp.where(written, k_new, carry[2]), jnp.where(written, v_new, carry[3])


def solution(mesh):
    beams = mesh.shape["beam"]
    models = mesh.shape["model"]
    cache_spec = P(None, ('data', 'beam'), None, 'model', None)
    col_spec = P(None, None, 'model')
    row_spec = P(None, 'model', None)
    in_specs = (P(('data', 'beam'), None), P('data', None), P(), P(('data', 'beam')), cache_spec, cache_spec,
                P(), col_spec, col_spec, col_spec, row_spec, P(), col_spec, col_spec, row_spec, P(), P(None, 'model'))
    out_specs = (cache_spec, cache_spec, P(('data', 'beam'), 'model'))

    def local_step(x_embed, parent, position, score, k_cache, v_cache, gain_attn, w_query, w_key, w_value, w_out, gain_mlp, w_gate, w_up, w_down, gain_final, w_vocab):
        rows = x_embed.shape[0]
        _, _, slots, heads, lanes = k_cache.shape
        table, info = make_plan(parent, beams // 2, 2 * rows)
        k_rows = k_cache.reshape(rows, slots * heads, lanes)
        v_rows = v_cache.reshape(rows, slots * heads, lanes)
        half_dim = lanes // 2
        angles = position.astype(jnp.float32) * ROPE_BASE ** (-jnp.arange(half_dim, dtype=jnp.float32) / half_dim)
        cos_part, sin_part = jnp.cos(angles), jnp.sin(angles)
        rope = jnp.stack([jnp.concatenate([cos_part, cos_part]), jnp.concatenate([-sin_part, sin_part])])
        prow = jnp.tile(parent.reshape(1, -1), (1, heads))
        pos = position.reshape(1)
        gains = dict(gain_attn=gain_attn, gain_mlp=gain_mlp, gain_final=gain_final.reshape(1, -1))
        weights = dict(w_query=w_query[0], w_key=w_key[0], w_value=w_value[0], w_out=w_out[0],
                       w_gate=w_gate[0].T, w_up=w_up[0].T, w_down=w_down[0], w_vocab=w_vocab.T)
        score_rows = jnp.broadcast_to(score[:, None], (rows, lanes))

        def step(rounds):
            return run_step(rounds, beams, models, table, pos, parent, score_rows, rope, prow, x_embed, k_rows, v_rows, gains, weights)

        def whole(word):
            vocab = w_vocab.shape[1]
            voc_core = word.shape[2]
            skip = 2 * voc_core - vocab
            last = voc_core - 512
            return jnp.concatenate([word[0], word[1, :, :last], word[1, :, last + skip :]], axis=1)

        def few(_):
            k_new, v_new, word = step(ROUND_CHOICES[0])
            return *settle(k_new, v_new), whole(word)

        def more(_):
            k_new, v_new, word = step(ROUND_CHOICES[1])
            enough = info[0] <= ROUND_CHOICES[1]
            k_new, v_new = lax.cond(enough, settle, lambda a, b: move_any(beams, heads, parent, position, k_rows, v_rows, a, b), k_new, v_new)
            return k_new, v_new, whole(word)

        k_new, v_new, candidates = lax.cond(info[0] <= ROUND_CHOICES[0], few, more, 0)
        shape = (1, rows, slots, heads, lanes)
        return k_new.reshape(shape), v_new.reshape(shape), candidates

    return jax.shard_map(local_step, mesh=mesh, in_specs=in_specs, out_specs=out_specs, check_vma=False)
```

```python
import functools
import types

import jax
import jax.numpy as jnp
from jax import lax
from jax.experimental import pallas as pl
from jax.experimental.pallas import tpu as pltpu
import numpy as np
from jax.sharding import PartitionSpec as P

NORM_EPS = 1e-6
ROPE_BASE = 10000.0
MESH = pl.DeviceIdType.MESH
CHUNKS = 8
TABLE = 24
ROUND_CHOICES = (3, 4)
W_BUFFERS = 4
SIDES = (0, 1)
LANES = 128
VMEM_LIMIT = 66 * 10**6


def plan_kernel(chips, chip_rows, parent_ref, table_ref, info_ref, hop_plus, hop_minus, onward, side):
    total = chips * chip_rows
    my_chip = lax.axis_index("beam") // 2
    row_bits, chip_mask, row_mask = chip_rows.bit_length() - 1, chips - 1, chip_rows - 1
    spare = 2 * TABLE + chip_rows

    near, far, back = [jnp.int32(0)] * 3
    parents = [parent_ref[0, b] for b in range(total)]
    for b, q in enumerate(parents):
        dist = ((b >> row_bits) - (q >> row_bits)) & chip_mask
        bit = jnp.left_shift(1, q)
        near |= jnp.where(dist == 1, bit, 0)
        far |= jnp.where(dist == 2, bit, 0)
        back |= jnp.where(dist == 3, bit, 0)

    def bit_of(mask, q):
        return jnp.right_shift(mask, q) & 1

    every = [(q, q >> row_bits, bit_of(near, q), bit_of(far, q), bit_of(back, q)) for q in range(total)]
    right = [(c + 1) & chip_mask for c in range(chips)]
    left = [(c - 1) & chip_mask for c in range(chips)]
    load_plus, load_minus, own_plus, own_minus, two_plus, two_minus = [[jnp.int32(0)] * chips for _ in range(6)]
    plus, minus = [], []
    for q, c, a, b, d in every:
        plus.append(b & a & (1 - d))
        minus.append(b & d & (1 - a))
        own_plus[c] += a
        own_minus[c] += d
        load_plus[right[c]] += plus[q]
        load_minus[left[c]] += minus[q]
    load_plus = [x + y for x, y in zip(load_plus, own_plus)]
    load_minus = [x + y for x, y in zip(load_minus, own_minus)]
    for q, c, a, b, d in every:
        flex = b & (1 - (a ^ d))
        cost_plus = jnp.maximum(load_plus[c] - a, load_plus[right[c]])
        cost_minus = jnp.maximum(load_minus[c] - d, load_minus[left[c]])
        go = jnp.where(cost_plus <= cost_minus, flex, 0)
        stay = flex - go
        for load, own, x, y in ((load_plus, own_plus, go, a), (load_minus, own_minus, stay, d)):
            load[c] += x & (1 - y)
            own[c] += x & (1 - y)
        load_plus[right[c]] += go
        load_minus[left[c]] += stay
        plus[q] += go
        minus[q] += stay
    first_plus, first_minus = [], []
    for q, c, *_ in every:
        first_plus.append(two_plus[c])
        first_minus.append(two_minus[c])
        two_plus[c] += plus[q]
        two_minus[c] += minus[q]
    rounds = jnp.int32(0)

    for at in range(spare):
        table_ref[at] = 0

    def write(cond, place, value):
        table_ref[jnp.where(cond, place, spare)] = value

    for q, c, a, b, d in every:
        a, d = a & (1 - plus[q]), d & (1 - minus[q])
        h_plus = jnp.where(a == 1, two_plus[c], first_plus[q])
        h_minus = jnp.where(d == 1, two_minus[c], first_minus[q])
        two_plus[c] += a
        two_minus[c] += d
        second = jnp.where(plus[q] == 1, jnp.maximum(own_plus[right[c]], 1) + h_plus, jnp.maximum(own_minus[left[c]], 1) + h_minus)
        uses_plus, uses_minus, uses_two = (a + plus[q]) == 1, (d + minus[q]) == 1, (plus[q] + minus[q]) == 1
        for use, h in ((uses_plus, h_plus), (uses_minus, h_minus), (uses_two, second)):
            rounds = jnp.maximum(rounds, jnp.where(use, h + 1, 0))
        hop_plus[q] = h_plus
        hop_minus[q] = h_minus
        onward[q] = second
        side[q] = plus[q]
        here = my_chip == c
        write(here & uses_plus, h_plus, q & row_mask)
        write(here & uses_minus, TABLE + h_minus, q & row_mask)
        write((my_chip == right[c]) & (plus[q] == 1), second, chip_rows + h_plus)
        write((my_chip == left[c]) & (minus[q] == 1), TABLE + second, chip_rows + h_minus)
    info_ref[0] = rounds
    for j in range(chip_rows):
        q = parent_ref[0, my_chip * chip_rows + j]
        dist = (my_chip - (q >> row_bits)) & chip_mask
        at_plus = chip_rows + 2 * jnp.where(dist == 1, hop_plus[q], onward[q])
        at_minus = chip_rows + 2 * jnp.where(dist == 3, hop_minus[q], onward[q]) + 1
        from_plus = (dist == 1) | ((dist == 2) & (side[q] == 1))
        table_ref[2 * TABLE + j] = jnp.where(dist == 0, q & row_mask, jnp.where(from_plus, at_plus, at_minus))


def make_plan(parent, chips, chip_rows):
    total = chips * chip_rows
    smem = pl.BlockSpec(memory_space=pltpu.SMEM)
    return pl.pallas_call(
        functools.partial(plan_kernel, chips, chip_rows),
        out_shape=(jax.ShapeDtypeStruct((2 * TABLE + chip_rows + 1,), jnp.int32), jax.ShapeDtypeStruct((1,), jnp.int32)),
        in_specs=[smem],
        out_specs=(smem, smem),
        scratch_shapes=[pltpu.SMEM((total,), jnp.int32)] * 4,
        name="plan",
    )(parent)


def loop(n, body):
    def step(i, carry):
        body(i)
        return carry

    lax.fori_loop(0, n, step, 0)


class Copies:
    def __init__(self, copies):
        self.copies = copies

    def start(self):
        for copy in self.copies:
            copy.start()

    def wait(self):
        for copy in self.copies:
            copy.wait()


def step_kernel(rounds, beams, models, rows, heads, slots, d_model, ff, vocab, names, *refs):
    r = types.SimpleNamespace(**dict(zip(names, refs)))
    table, pos_ref, parent_ref = r.table, r.pos, r.parent
    k_ref, v_ref, k_out, v_out = r.k, r.v, r.k_out, r.v_out
    f32, bf16 = jnp.float32, jnp.bfloat16
    nchunk = CHUNKS
    block = slots * heads // nchunk
    span = slots // nchunk
    chips = beams // 2
    pair = 2 * rows
    lanes = LANES
    me = lax.axis_index("beam")
    core = lax.rem(me, 2)
    chip = me // 2
    is_k, is_v = core == 0, core == 1
    all_half, all_heads = pl.ds(0, d_model // 2), pl.ds(0, heads * LANES)
    sibling = me + 1 - 2 * core
    right = lax.rem(me + 2, beams)
    left = lax.rem(me + beams - 2, beams)
    model = lax.axis_index("model")
    mine = pl.ds(core * rows, rows)
    theirs = pl.ds((1 - core) * rows, rows)
    lane_iota = lax.broadcasted_iota(jnp.int32, (1, lanes), 1)
    pool, recv, send, stage, other = r.pool, r.recv, r.send, r.stage, r.other
    half = d_model // 2

    def to(peer):
        return dict(device_id={"beam": peer}, device_id_type=MESH)

    def across(m, peer):
        return dict(device_id={"model": m, "beam": peer}, device_id_type=MESH)

    def part(ref, c):
        return ref.at[:, pl.ds(c * block, block), :]

    def load_own(ref, c):
        return pltpu.make_async_copy(part(ref, c), pool[c].at[mine], r.pool_sem.at[c])

    def load_other(ref, c):
        return pltpu.make_async_copy(part(ref, c), other[c], r.other_sem.at[c])

    def swap(ref, c):
        return pltpu.make_async_remote_copy(part(ref, c), pool[c].at[mine], r.swap_send.at[c], r.swap_recv.at[c], **to(sibling))

    def hop(n, d, c):
        return pltpu.make_async_remote_copy(
            send[c].at[2 * n + d], recv[c].at[2 * n + d], r.hop_send.at[n, d, c], r.hop_recv.at[n, d, c], **to(right if d == 0 else left))

    def store_own(ref, c):
        return pltpu.make_async_copy(stage[c].at[mine], part(ref, c), r.out_sem.at[c])

    def give(ref, c):
        return pltpu.make_async_remote_copy(stage[c].at[theirs], part(ref, c), r.give_send.at[c], r.give_recv.at[c], **to(sibling))

    w_count = len(r.wbuf)
    groups = []

    def group(blocks):
        groups.append(blocks)

    for ref in (r.w_query, r.w_key, r.w_value):
        width = heads * lanes // 2
        group([(ref, pl.ds(1024 * i, 1024), pl.ds(core * width, width), pl.ds(0, 1024), pl.ds(i * width, width)) for i in range(d_model // 1024)])
    group([(r.w_out, all_heads, pl.ds(core * half, half), all_heads, all_half)])
    ff_core = (ff + 127) // 256 * 128
    ff_full = ff_core // 256
    ff_last = ff_core - 256 * ff_full
    ff_skip = 2 * ff_core - ff
    for i in range(ff_full + 1):
        n = 256 if i < ff_full else ff_last
        first = core * (ff_core - (ff_skip if i == ff_full else 0)) + 256 * i
        first = pl.multiple_of(first, 8)
        group([(ref, pl.ds(first, n), pl.ds(j * half, half), pl.ds(512 * j + n * u, n), all_half) for u, ref in enumerate((r.w_gate, r.w_up)) for j in range(2)])
    down_rows = []
    for i in range(0, 2 * ff_core, 1024):
        n = min(1024, 2 * ff_core - i)
        down_rows.append((i, n))
        blocks = [(i, n, 0)]
        if i + n > 2 * ff_core - ff_last:
            blocks = [(i, n - ff_last, 0), (ff - ff_last, ff_last, n - ff_last)]
        group([(r.w_down, pl.ds(a, b), pl.ds(core * half, half), pl.ds(c, b), all_half) for a, b, c in blocks])
    voc_core = (vocab + 1023) // 1024 * 512
    voc_groups = voc_core // 512
    voc_skip = 2 * voc_core - vocab
    for i in range(voc_groups):
        first = core * (voc_core - (voc_skip if i == voc_groups - 1 else 0)) + 512 * i
        first = pl.multiple_of(first, 8)
        group([(r.w_vocab, pl.ds(first, 512), pl.ds(j * half, half), pl.ds(512 * j, 512), all_half) for j in range(2)])

    def group_copies(g):
        return [pltpu.make_async_copy(ref.at[a, b], r.wbuf[g % w_count].at[c, e], r.w_sem.at[g, i]) for i, (ref, a, b, c, e) in enumerate(groups[g])]

    def load(g):
        if g < len(groups):
            for copy in group_copies(g):
                copy.start()

    taken = [0]

    def with_group(use):
        g = taken[0]
        taken[0] += 1
        for copy in group_copies(g):
            copy.wait()
        use(r.wbuf[g % w_count])
        load(g + w_count)

    barrier = pltpu.get_barrier_semaphore()
    peers = [lax.rem(me + s, beams) for s in range(1, beams)]
    model_peers = [lax.rem(model + s, models) for s in range(1, models)]
    for peer in peers:
        pl.semaphore_signal(barrier, **to(peer))
    for m in model_peers:
        for peer in (me, sibling):
            pl.semaphore_signal(barrier, **across(m, peer))

    @pl.when(is_k)
    def _():
        for c in range(nchunk):
            load_own(k_ref, c).start()

    @pl.when(is_v)
    def _():
        for c in range(nchunk):
            load_own(v_ref, c).start()

    load(0)
    prow = jnp.zeros((1, lanes), jnp.int32)
    for b in range(beams * rows):
        prow = jnp.where(lax.rem(lane_iota, beams * rows) == b, parent_ref[0, b], prow)
    for j in range(rows):
        r.score_rows[j : j + 1, :] = jnp.full((1, lanes), r.score[j])
    angles = pos_ref[0].astype(f32) * r.freq[...]
    cos_part = jnp.cos(angles)
    sin_part = jnp.where(lane_iota < lanes // 2, -1.0, 1.0) * jnp.sin(angles)
    pl.semaphore_wait(barrier, beams - 1 + 2 * (models - 1))

    x_swap = pltpu.make_async_remote_copy(r.x, r.x_got, r.pair_send.at[0], r.pair_recv.at[0], **to(sibling))
    x_swap.start()

    @pl.when(is_k)
    def _():
        for c in range(nchunk):
            swap(v_ref, c).start()

    @pl.when(is_v)
    def _():
        for c in range(nchunk):
            swap(k_ref, c).start()

    for g in range(1, w_count):
        load(g)

    @pl.when(is_k)
    def _():
        for c in range(nchunk):
            load_other(v_ref, c).start()

    @pl.when(is_v)
    def _():
        for c in range(nchunk):
            load_other(k_ref, c).start()

    strip = min(block, 128)

    def build(n, c):
        for d in SIDES:
            code = table[d * TABLE + n]
            row = jnp.minimum(code, pair - 1)

            def body(i):
                at = pl.ds(pl.multiple_of(i * strip, strip), strip)
                x = pool[c][row, at, :]
                for e in range(n):
                    x = jnp.where(code == pair + e, recv[c][2 * e + d, at, :], x)
                send[c][2 * n + d, at, :] = x

            loop(block // strip, body)
        for d in SIDES:
            hop(n, d, c).start()

    waited = set()

    def have_own(c):
        if c not in waited:
            waited.add(c)
            load_own(k_ref, c).wait()

    def first_round(c):
        have_own(c)
        swap(k_ref, c).wait_recv()
        build(0, c)

    def later_round(n, c):
        for d in SIDES:
            hop(n - 1, d, c).wait_recv()
        build(n, c)

    def finish(c):
        for d in SIDES:
            hop(rounds - 1, d, c).wait_recv()
        position = pos_ref[0]

        def put_row(j):
            where = table[2 * TABLE + j]
            row = jnp.minimum(where, pair - 1)
            slot = jnp.clip(where - pair, 0, 2 * rounds - 1)
            new = jnp.concatenate([r.fresh[j]] * (strip // heads))

            def body(i):
                at = pl.ds(pl.multiple_of(i * strip, strip), strip)
                x = jnp.where(where < pair, pool[c][row, at, :], recv[c][slot, at, :])
                here = (lax.broadcasted_iota(jnp.int32, (strip, lanes), 0) + i * strip) // heads + c * span
                stage[c][j, at, :] = jnp.where(here == position, new, x.astype(f32)).astype(bf16)

            loop(block // strip, body)

        loop(pair, put_row)

        @pl.when(is_k)
        def _():
            give(k_out, c).start()
            store_own(k_out, c).start()

        @pl.when(is_v)
        def _():
            give(v_out, c).start()
            store_own(v_out, c).start()

    todo = [functools.partial(first_round, c) for c in range(nchunk)]
    todo += [functools.partial(later_round, n, c) for n in range(1, rounds) for c in range(nchunk)]
    todo += [functools.partial(finish, c) for c in range(nchunk)]

    def serve(n=1):
        for _ in range(n):
            if todo:
                todo.pop(0)()

    res = r.res

    def normed(gain_ref):
        x = res[...]
        inv = lax.rsqrt(jnp.mean(x * x, axis=-1, keepdims=True) + NORM_EPS)
        r.h[...] = (x * inv * gain_ref[...].astype(f32)).astype(bf16)

    def dot(a, b):
        return jnp.dot(a, b, preferred_element_type=f32)

    def dot_halves(w, n):
        def body(j, x):
            a = h[:, pl.ds(pl.multiple_of(j * half, lanes), half)]
            b = w[pl.ds(pl.multiple_of(j * 512, 512), n), :]
            return x + lax.dot_general(a, b, (((1,), (1,)), ((), ())), preferred_element_type=f32)

        return lax.fori_loop(0, 2, body, jnp.zeros((pair, n), f32))

    def dot_rows(a, first, w, n):
        def body(j, x):
            at = pl.multiple_of(j * (n // 2), lanes)
            return x + dot(a[:, pl.ds(first + at, n // 2)], w[pl.ds(at, n // 2), :])

        return lax.fori_loop(0, 2, body, jnp.zeros((pair, half), f32))

    def exchange_model(part_ref, got_ref, phase):
        if models == 1:
            return part_ref[...]
        copies = [
            pltpu.make_async_remote_copy(part_ref, got_ref.at[model], r.model_send.at[phase, s], r.model_recv.at[phase, s], **across(m, me))
            for s, m in enumerate(model_peers)]
        for copy in copies:
            copy.start()
        got_ref[model] = part_ref[...]
        for copy in copies:
            copy.wait()
        total = got_ref[0]
        for m in range(1, models):
            total = total + got_ref[m]
        return total

    serve()
    x_swap.wait()

    @pl.when(is_k)
    def _():
        res[0:rows, :] = r.x[...].astype(f32)
        res[rows:pair, :] = r.x_got[...].astype(f32)

    @pl.when(is_v)
    def _():
        res[0:rows, :] = r.x_got[...].astype(f32)
        res[rows:pair, :] = r.x[...].astype(f32)

    normed(r.gain_attn)
    h = r.h
    head_half = heads // 2
    width = head_half * lanes
    qkv = r.qkv
    for kind in range(3):
        def use(w, kind=kind):
            blocks = d_model // 1024
            each = min(2, blocks)

            def body(i, z):
                for e in range(each):
                    at = i * each + e
                    a = h[:, pl.ds(pl.multiple_of(at * 1024, 1024), 1024)]
                    z = z + dot(a, w[:, pl.ds(pl.multiple_of(at * width, lanes), width)])
                return z

            z = lax.fori_loop(0, blocks // each, body, jnp.zeros((pair, width), f32))
            for n in range(head_half):
                y = z[:, n * lanes : (n + 1) * lanes]
                if kind < 2:
                    y = y * cos_part + pltpu.roll(y, lanes // 2, 1) * sin_part
                qkv[kind, n] = y.astype(bf16)
        with_group(use)
    serve()

    qkv_all = r.qkv_all
    to_parents = Copies(
        [pltpu.make_async_remote_copy(qkv, qkv_all.at[me], r.beam_send.at[0, s], r.beam_recv.at[0, s], **to(p)) for s, p in enumerate(peers)]
        + [pltpu.make_async_remote_copy(r.score_rows, r.scores.at[me], r.beam_send.at[1, s], r.beam_recv.at[1, s], **to(p)) for s, p in enumerate(peers)])
    to_parents.start()
    qkv_all[me] = qkv[...]
    r.scores[me] = r.score_rows[...]
    serve(2)
    to_parents.wait()
    serve()

    cat = r.cat
    for kind in range(3):
        for n in range(heads):
            for x in range(chips):
                at = n * beams * rows + x * pair
                cat[kind, at : at + pair, :] = qkv_all[2 * x + n // head_half, kind, n % head_half].astype(f32)
    for j in range(pair):
        at = pl.ds(chip * pair + j, heads, stride=beams * rows)
        r.fresh[j] = jnp.where(is_k, cat[1, at, :], cat[2, at, :])

    query_t = cat[0].T.astype(bf16)
    new_k = cat[1].astype(bf16)
    total_cols = heads * beams * rows
    tiles = total_cols // lanes
    heads_tile = heads // tiles
    lane_head = lane_iota // (beams * rows)
    spread = r.spread
    logit = r.logit
    position = pos_ref[0]

    def own_rows(c, p, kind):
        a = pool[c][core * rows + p]
        b = other[c][p]
        return jnp.where(core == kind, a, b)

    def score_chunk(c):
        have_own(c)
        load_other(k_ref, c).wait()

        def body(p):
            full = dot(own_rows(c, p, 0), query_t)
            for t in range(tiles):
                spread[t][...] = full[:, t * lanes : (t + 1) * lanes]
            for t in range(tiles):
                here = prow == me * rows + p
                at = pl.ds(c * span, span)
                x = logit[t][at, :]
                for n in range(heads_tile):
                    got = spread[t][pl.ds(t * heads_tile + n, span, stride=heads), :]
                    x = jnp.where(here & (lane_head == n), got, x)
                logit[t][at, :] = x

        loop(rows, body)

    for t in range(tiles):
        logit[t][...] = jnp.zeros_like(logit[t])
    self_full = dot(new_k, query_t)
    scale = lanes ** -0.5
    for c in range(nchunk):
        score_chunk(c)
        serve(c % 4 == 3)
    slot_index = lax.broadcasted_iota(jnp.int32, (slots, lanes), 0)
    self_prob = []
    for t in range(tiles):
        diag = lax.broadcasted_iota(jnp.int32, (total_cols, lanes), 0) == lax.broadcasted_iota(jnp.int32, (total_cols, lanes), 1) + t * lanes
        self_row = jnp.sum(jnp.where(diag, self_full[:, t * lanes : (t + 1) * lanes], 0.0), axis=0, keepdims=True)
        x = jnp.where(slot_index == position, self_row, logit[t][...]) * scale
        x = jnp.where(slot_index <= position, x, -jnp.inf)
        e = jnp.exp(x - jnp.max(x, axis=0, keepdims=True))
        prob = e / jnp.sum(e, axis=0, keepdims=True)
        logit[t][...] = jnp.where(slot_index == position, 0.0, prob)
        self_prob.append(jnp.sum(jnp.where(slot_index == position, prob, 0.0), axis=0, keepdims=True))
    for t in range(tiles):
        spread[t][...] = jnp.zeros_like(spread[t])
    out_t = r.out_t
    out_t[...] = cat[2].T * jnp.concatenate(self_prob, axis=1).astype(bf16).astype(f32)

    def value_chunk(c):
        def body(p):
            for t in range(tiles):
                here = prow == me * rows + p
                x = logit[t][pl.ds(c * span, span), :]
                for n in range(heads_tile):
                    spread[t][pl.ds(t * heads_tile + n, span, stride=heads), :] = jnp.where(here & (lane_head == n), x, 0.0)
            prob = jnp.concatenate([spread[t][...].astype(bf16) for t in range(tiles)], axis=1)
            out_t[...] += lax.dot_general(own_rows(c, p, 1), prob, (((0,), (0,)), ((), ())), preferred_element_type=f32)

        loop(rows, body)

    for c in range(nchunk):
        value_chunk(c)
        serve(c % 3 == 1)
    local = jnp.concatenate([prow] * tiles, axis=1) // rows == me
    o_rows = jnp.where(local, out_t[...], 0.0).T
    o_send, o_got = r.o_send, r.o_got
    for x in range(chips):
        for n in range(heads):
            at = n * beams * rows + x * pair
            o_send[x, n] = o_rows[at : at + pair, :].astype(bf16)
    back = Copies([
        pltpu.make_async_remote_copy(o_send.at[lax.rem(me + s, beams) // 2], o_got.at[me], r.beam_send.at[2, s - 1], r.beam_recv.at[2, s - 1], **to(lax.rem(me + s, beams)))
        for s in range(1, beams)])
    back.start()
    o_got[me] = o_send[chip]
    serve(3)
    back.wait()
    for n in range(heads):
        x = o_got[0, n].astype(f32)
        for s in range(1, beams):
            x = x + o_got[s, n].astype(f32)
        r.o[:, n * lanes : (n + 1) * lanes] = x.astype(bf16)

    part_sum, model_got, res_half, res_got = r.part, r.model_got, r.res_half, r.res_got

    def add_to_residual(phase):
        total = exchange_model(part_sum, model_got.at[phase] if models > 1 else None, phase)
        col = pl.ds(pl.multiple_of(core * half, lanes), half)
        other_col = pl.ds(pl.multiple_of((1 - core) * half, lanes), half)
        fresh = res[:, col] + total
        res_half[phase] = fresh
        trade = pltpu.make_async_remote_copy(res_half.at[phase], res_got.at[phase], r.pair_send.at[1 + phase], r.pair_recv.at[1 + phase], **to(sibling))
        trade.start()
        res[:, col] = fresh
        trade.wait()
        res[:, other_col] = res_got[phase]

    def use_out(w):
        part_sum[0] = dot_rows(r.o, 0, w, heads * lanes)
    with_group(use_out)
    serve(2)
    part_sum_ref = part_sum
    part_sum = part_sum_ref.at[0]
    add_to_residual(0)
    serve(2)
    normed(r.gain_mlp)

    g_own, g_got, g_all = r.g_own, r.g_got, r.g_all
    for i in range(ff_full + 1):
        n = 256 if i < ff_full else ff_last

        def use(w, i=i, n=n):
            z = dot_halves(w, 2 * n)
            gate, up = z[:, :n], z[:, n:]
            y = jax.nn.silu(gate) * up
            if i == ff_full and ff_skip:
                y = jnp.where(is_v & (lax.broadcasted_iota(jnp.int32, (1, n), 1) < ff_skip), 0.0, y)
            g_own[:, 256 * i : 256 * i + n] = y.astype(bf16)
        with_group(use)
        serve(i == 2)
    g_trade = pltpu.make_async_remote_copy(g_own, g_got, r.pair_send.at[3], r.pair_recv.at[3], **to(sibling))
    g_trade.start()
    g_all[:, pl.ds(pl.multiple_of(core * ff_core, lanes), ff_core)] = g_own[...]
    serve()
    g_trade.wait()
    g_all[:, pl.ds(pl.multiple_of((1 - core) * ff_core, lanes), ff_core)] = g_got[...]
    part_sum = part_sum_ref.at[1]
    for at, n in down_rows:
        def use(w, at=at, n=n):
            x = dot_rows(g_all, at, w, n)
            part_sum[...] = x if at == 0 else part_sum[...] + x
        with_group(use)
    serve()
    add_to_residual(1)
    serve(2)
    normed(r.gain_final)

    word = r.word
    for i in range(voc_groups):
        def use(w, i=i):
            word[:, 512 * i : 512 * (i + 1)] = dot_halves(w, 512)
        with_group(use)
        serve(i > 2)
    word_send, word_got = r.word_send, r.word_got
    x = word[...]
    word_send[0] = x[0:rows]
    word_send[1] = x[rows:pair]
    word_trade = pltpu.make_async_remote_copy(word_send.at[1 - core], word_got, r.pair_send.at[4], r.pair_recv.at[4], **to(sibling))
    word_trade.start()
    col = lax.broadcasted_iota(jnp.int32, (1, voc_core), 1)
    twice = is_v & (col >= voc_core - 512) & (col < voc_core - 512 + voc_skip)
    x = jnp.where(twice, -jnp.inf, x)
    top = jnp.max(x, axis=-1, keepdims=True)
    mass = jnp.sum(jnp.exp(x - top), axis=-1, keepdims=True)
    stat, stats = r.stat, r.stats
    stat[0] = jnp.broadcast_to(top, (pair, lanes))
    stat[1] = jnp.broadcast_to(mass, (pair, lanes))
    mates = [(m, p) for m in [model] + model_peers for p in (me, sibling)][1:]
    told = Copies([
        pltpu.make_async_remote_copy(stat, stats.at[2 * model + core], r.stat_send.at[i], r.stat_recv.at[i], **across(m, p))
        for i, (m, p) in enumerate(mates)])
    told.start()
    stats[2 * model + core] = stat[...]
    told.wait()
    top = stats[0, 0]
    for i in range(1, 2 * models):
        top = jnp.maximum(top, stats[i, 0])
    mass = stats[0, 1] * jnp.exp(stats[0, 0] - top)
    for i in range(1, 2 * models):
        mass = mass + stats[i, 1] * jnp.exp(stats[i, 0] - top)
    r.stat[0] = top
    r.stat[1] = jnp.log(mass)
    word_trade.wait()
    own, got = word_send[core], word_got[...]
    low, high = jnp.where(is_k, own, got), jnp.where(is_k, got, own)
    last = voc_core - 512
    for j in range(rows):
        q = parent_ref[0, me * rows + j]
        base = r.scores[q // rows, pl.ds(lax.rem(q, rows), 1), :][:, 0:1]
        at = pl.ds(core * rows + j, 1)
        shift = stat[0, at, 0:1]
        log_mass = stat[1, at, 0:1]
        row = slice(j, j + 1)
        x = base + (high[row] - shift - log_mass)
        r.word_out[row, :voc_core] = base + (low[row] - shift - log_mass)
        r.word_out[row, voc_core : voc_core + last] = x[:, :last]
        r.word_out[row, voc_core + last :] = x[:, last + voc_skip :]

    serve(len(todo))
    for c in range(nchunk):
        swap(k_ref, c).wait_send()
        for n in range(rounds):
            for d in SIDES:
                hop(n, d, c).wait_send()
        store_own(k_out, c).wait()
        give(k_out, c).wait()


def run_step(rounds, beams, models, table, pos, parent, score, freq, x, k_rows, v_rows, gains, weights):
    rows, length, lanes = k_rows.shape
    weights_ = types.SimpleNamespace(**weights)
    d_model = x.shape[1]
    heads = weights_.w_query.shape[1] // lanes
    slots = length // heads
    ff = weights_.w_down.shape[0]
    vocab = weights_.w_vocab.shape[0]
    block = length // CHUNKS
    pair = 2 * rows
    half = d_model // 2
    chips = beams // 2
    cols = heads * beams * rows
    bf16, f32 = jnp.bfloat16, jnp.float32
    vmem, dma = pltpu.VMEM, pltpu.SemaphoreType.DMA
    smem, hbm, ram = (pl.BlockSpec(memory_space=s) for s in (pltpu.SMEM, pl.ANY, pltpu.VMEM))
    voc_core = (vocab + 1023) // 1024 * 512
    ff_core = (ff + 127) // 256 * 128
    n_groups = 4 + ff_core // 256 + 1 + -(-2 * ff_core // 1024) + voc_core // 512
    ins = dict(table=(table, smem), pos=(pos, smem), parent=(parent, smem), score=(score, smem), freq=(freq, ram),
               x=(x, ram), k=(k_rows, hbm), v=(v_rows, hbm))
    ins.update({name: (a, ram) for name, a in gains.items()})
    ins.update({name: (a, hbm) for name, a in weights.items()})
    outs = dict(k_out=(jax.ShapeDtypeStruct(k_rows.shape, bf16), hbm), v_out=(jax.ShapeDtypeStruct(k_rows.shape, bf16), hbm),
                word_out=(jax.ShapeDtypeStruct((rows, vocab), f32), ram))
    scratch = dict(
        pool=[vmem((pair, block, lanes), bf16)] * CHUNKS,
        recv=[vmem((2 * rounds, block, lanes), bf16)] * CHUNKS,
        send=[vmem((2 * rounds, block, lanes), bf16)] * CHUNKS,
        stage=[vmem((pair, block, lanes), bf16)] * CHUNKS,
        other=[vmem((rows, block, lanes), bf16)] * CHUNKS,
        wbuf=[vmem((1024, half), bf16)] * W_BUFFERS,
        spread=[vmem((block, lanes), f32)] * (cols // lanes),
        logit=[vmem((slots, lanes), f32)] * (cols // lanes),
        x_got=vmem(x.shape, bf16),
        res=vmem((pair, d_model), f32),
        h=vmem((pair, d_model), bf16),
        qkv=vmem((3, heads // 2, pair, lanes), bf16),
        qkv_all=vmem((beams, 3, heads // 2, pair, lanes), bf16),
        scores=vmem((beams, rows, lanes), f32),
        score_rows=vmem((rows, lanes), f32),
        cat=vmem((3, cols, lanes), f32),
        fresh=vmem((pair, heads, lanes), f32),
        out_t=vmem((lanes, cols), f32),
        o_send=vmem((chips, heads, pair, lanes), bf16),
        o_got=vmem((beams, heads, pair, lanes), bf16),
        o=vmem((pair, heads * lanes), bf16),
        part=vmem((2, pair, half), f32),
        model_got=vmem((2, models, pair, half), f32),
        res_half=vmem((2, pair, half), f32),
        res_got=vmem((2, pair, half), f32),
        g_own=vmem((pair, ff_core), bf16),
        g_got=vmem((pair, ff_core), bf16),
        g_all=vmem((pair, 2 * ff_core), bf16),
        word=vmem((pair, voc_core), f32),
        word_send=vmem((2, rows, voc_core), f32),
        word_got=vmem((rows, voc_core), f32),
        stat=vmem((2, pair, lanes), f32),
        stats=vmem((2 * models, 2, pair, lanes), f32),
        w_sem=dma((n_groups, 4)),
        pool_sem=dma((CHUNKS,)), other_sem=dma((CHUNKS,)), swap_send=dma((CHUNKS,)), swap_recv=dma((CHUNKS,)),
        hop_send=dma((rounds, 2, CHUNKS)), hop_recv=dma((rounds, 2, CHUNKS)),
        out_sem=dma((CHUNKS,)), give_send=dma((CHUNKS,)), give_recv=dma((CHUNKS,)),
        pair_send=dma((5,)), pair_recv=dma((5,)),
        beam_send=dma((3, beams)), beam_recv=dma((3, beams)),
        model_send=dma((2, models)), model_recv=dma((2, models)),
        stat_send=dma((2 * models,)), stat_recv=dma((2 * models,)),
    )
    flat, places = [], {}
    for name, s in scratch.items():
        many = isinstance(s, list)
        places[name] = (len(flat), len(s) if many else None)
        flat += s if many else [s]
    first = list(ins) + list(outs)

    def kernel(*refs):
        named = list(refs[: len(first)])
        rest = refs[len(first) :]
        for start, count in places.values():
            named.append(rest[start] if count is None else list(rest[start : start + count]))
        step_kernel(rounds, beams, models, rows, heads, slots, d_model, ff, vocab, first + list(places), *named)

    return pl.pallas_call(
        kernel,
        out_shape=tuple(s for s, _ in outs.values()),
        in_specs=[s for _, s in ins.values()],
        out_specs=tuple(s for _, s in outs.values()),
        scratch_shapes=flat,
        compiler_params=pltpu.CompilerParams(collective_id=rounds, has_side_effects=True, vmem_limit_bytes=VMEM_LIMIT),
        name=f"step{rounds}",
    )(*[a for a, _ in ins.values()])


def copy_kernel(pieces, a_ref, b_ref, a_out, b_out, buf, in_sem, out_sem):
    rows, length, _ = a_ref.shape
    per = rows // pieces
    jobs = [(src, dst, i) for i in range(pieces) for src, dst in ((a_ref, a_out), (b_ref, b_out))]

    def get(n):
        src, _, i = jobs[n]
        return pltpu.make_async_copy(src.at[pl.ds(i * per, per)], buf.at[n], in_sem.at[n])

    def put(n):
        _, dst, i = jobs[n]
        return pltpu.make_async_copy(buf.at[n], dst.at[pl.ds(i * per, per)], out_sem.at[n])

    for n in range(len(jobs)):
        get(n).start()
    for n in range(len(jobs)):
        get(n).wait()
        put(n).start()
    for n in range(len(jobs)):
        put(n).wait()


def settle(a, b):
    rows, length, lanes = a.shape
    hbm = pl.BlockSpec(memory_space=pl.ANY)
    out = jax.ShapeDtypeStruct(a.shape, a.dtype)
    return pl.pallas_call(
        functools.partial(copy_kernel, rows),
        out_shape=(out, out),
        in_specs=[hbm, hbm],
        out_specs=(hbm, hbm),
        scratch_shapes=[pltpu.VMEM((2 * rows, 1, length, lanes), a.dtype), pltpu.SemaphoreType.DMA((2 * rows,)), pltpu.SemaphoreType.DMA((2 * rows,))],
        name="settle",
    )(a, b)


def move_any(beams, heads, parent, position, k_rows, v_rows, k_new, v_new):
    rows, length, _ = k_rows.shape
    me = lax.axis_index("beam")
    mine = lax.dynamic_slice(parent.reshape(-1), (me * rows,), (rows,))
    local = lax.rem(mine, rows)
    ring = [(i, (i + 1) % beams) for i in range(beams)]

    def choose(source, here, chosen):
        hit = (mine // rows == source)[:, None, None]
        return jnp.where(hit, jnp.take(here, local, axis=0), chosen)

    def step(s, carry):
        k_here, v_here, k_sel, v_sel = carry
        source = lax.rem(me - s + beams, beams)
        k_sel, v_sel = choose(source, k_here, k_sel), choose(source, v_here, v_sel)
        return lax.ppermute(k_here, "beam", ring), lax.ppermute(v_here, "beam", ring), k_sel, v_sel

    carry = (lax.ppermute(k_rows, "beam", ring), lax.ppermute(v_rows, "beam", ring), choose(me, k_rows, k_new), choose(me, v_rows, v_new))
    carry = lax.fori_loop(1, beams, step, carry)
    written = (jnp.arange(length) // heads == position)[None, :, None]
    return jnp.where(written, k_new, carry[2]), jnp.where(written, v_new, carry[3])


def solution(mesh):
    beams = mesh.shape["beam"]
    models = mesh.shape["model"]
    cache_spec = P(None, ('data', 'beam'), None, 'model', None)
    col_spec = P(None, None, 'model')
    row_spec = P(None, 'model', None)
    in_specs = (P(('data', 'beam'), None), P('data', None), P(), P(('data', 'beam')), cache_spec, cache_spec,
                P(), col_spec, col_spec, col_spec, row_spec, P(), col_spec, col_spec, row_spec, P(), P(None, 'model'))
    out_specs = (cache_spec, cache_spec, P(('data', 'beam'), 'model'))

    def local_step(x_embed, parent, position, score, k_cache, v_cache, gain_attn, w_query, w_key, w_value, w_out, gain_mlp, w_gate, w_up, w_down, gain_final, w_vocab):
        rows = x_embed.shape[0]
        _, _, slots, heads, lanes = k_cache.shape
        table, info = make_plan(parent, beams // 2, 2 * rows)
        k_rows = k_cache.reshape(rows, slots * heads, lanes)
        v_rows = v_cache.reshape(rows, slots * heads, lanes)
        half_dim = lanes // 2
        freq = np.float32(ROPE_BASE) ** (-np.arange(half_dim, dtype=np.float32) / np.float32(half_dim))
        freq = jnp.asarray(np.concatenate([freq, freq])[None])
        pos = position.reshape(1)
        gains = dict(gain_attn=gain_attn, gain_mlp=gain_mlp, gain_final=gain_final.reshape(1, -1))
        weights = dict(w_query=w_query[0], w_key=w_key[0], w_value=w_value[0], w_out=w_out[0],
                       w_gate=w_gate[0].T, w_up=w_up[0].T, w_down=w_down[0], w_vocab=w_vocab.T)
        def step(rounds):
            return run_step(rounds, beams, models, table, pos, parent, score, freq, x_embed, k_rows, v_rows, gains, weights)

        def few(_):
            k_new, v_new, word = step(ROUND_CHOICES[0])
            return *settle(k_new, v_new), word

        def more(_):
            k_new, v_new, word = step(ROUND_CHOICES[1])
            enough = info[0] <= ROUND_CHOICES[1]
            k_new, v_new = lax.cond(enough, settle, lambda a, b: move_any(beams, heads, parent, position, k_rows, v_rows, a, b), k_new, v_new)
            return k_new, v_new, word

        k_new, v_new, candidates = lax.cond(info[0] <= ROUND_CHOICES[0], few, more, 0)
        shape = (1, rows, slots, heads, lanes)
        return k_new.reshape(shape), v_new.reshape(shape), candidates

    return jax.shard_map(local_step, mesh=mesh, in_specs=in_specs, out_specs=out_specs, check_vma=False)
```

```python
import functools
import types

import jax
import jax.numpy as jnp
from jax import lax
from jax.experimental import pallas as pl
from jax.experimental.pallas import tpu as pltpu
import numpy as np
from jax.sharding import PartitionSpec as P

NORM_EPS = 1e-6
ROPE_BASE = 10000.0
MESH = pl.DeviceIdType.MESH
CHUNKS = 8
TABLE = 24
ROUND_CHOICES = (3, 4)
W_BUFFERS = 9
SIDES = (0, 1)
LANES = 128
VMEM_LIMIT = 66 * 10**6


def plan_kernel(chips, chip_rows, parent_ref, table_ref, info_ref, hop_plus, hop_minus, onward, side):
    total = chips * chip_rows
    my_chip = lax.axis_index("beam") // 2
    row_bits, chip_mask, row_mask = chip_rows.bit_length() - 1, chips - 1, chip_rows - 1
    spare = 2 * TABLE + chip_rows

    near, far, back = [jnp.int32(0)] * 3
    parents = [parent_ref[0, b] for b in range(total)]
    for b, q in enumerate(parents):
        dist = ((b >> row_bits) - (q >> row_bits)) & chip_mask
        bit = jnp.left_shift(1, q)
        near |= jnp.where(dist == 1, bit, 0)
        far |= jnp.where(dist == 2, bit, 0)
        back |= jnp.where(dist == 3, bit, 0)

    def bit_of(mask, q):
        return jnp.right_shift(mask, q) & 1

    every = [(q, q >> row_bits, bit_of(near, q), bit_of(far, q), bit_of(back, q)) for q in range(total)]
    right = [(c + 1) & chip_mask for c in range(chips)]
    left = [(c - 1) & chip_mask for c in range(chips)]
    load_plus, load_minus, own_plus, own_minus, two_plus, two_minus = [[jnp.int32(0)] * chips for _ in range(6)]
    plus, minus = [], []
    for q, c, a, b, d in every:
        plus.append(b & a & (1 - d))
        minus.append(b & d & (1 - a))
        own_plus[c] += a
        own_minus[c] += d
        load_plus[right[c]] += plus[q]
        load_minus[left[c]] += minus[q]
    load_plus = [x + y for x, y in zip(load_plus, own_plus)]
    load_minus = [x + y for x, y in zip(load_minus, own_minus)]
    for q, c, a, b, d in every:
        flex = b & (1 - (a ^ d))
        cost_plus = jnp.maximum(load_plus[c] - a, load_plus[right[c]])
        cost_minus = jnp.maximum(load_minus[c] - d, load_minus[left[c]])
        go = jnp.where(cost_plus <= cost_minus, flex, 0)
        stay = flex - go
        for load, own, x, y in ((load_plus, own_plus, go, a), (load_minus, own_minus, stay, d)):
            load[c] += x & (1 - y)
            own[c] += x & (1 - y)
        load_plus[right[c]] += go
        load_minus[left[c]] += stay
        plus[q] += go
        minus[q] += stay
    first_plus, first_minus = [], []
    for q, c, *_ in every:
        first_plus.append(two_plus[c])
        first_minus.append(two_minus[c])
        two_plus[c] += plus[q]
        two_minus[c] += minus[q]
    rounds = jnp.int32(0)

    for at in range(spare):
        table_ref[at] = 0

    def write(cond, place, value):
        table_ref[jnp.where(cond, place, spare)] = value

    for q, c, a, b, d in every:
        a, d = a & (1 - plus[q]), d & (1 - minus[q])
        h_plus = jnp.where(a == 1, two_plus[c], first_plus[q])
        h_minus = jnp.where(d == 1, two_minus[c], first_minus[q])
        two_plus[c] += a
        two_minus[c] += d
        second = jnp.where(plus[q] == 1, jnp.maximum(own_plus[right[c]], 1) + h_plus, jnp.maximum(own_minus[left[c]], 1) + h_minus)
        uses_plus, uses_minus, uses_two = (a + plus[q]) == 1, (d + minus[q]) == 1, (plus[q] + minus[q]) == 1
        for use, h in ((uses_plus, h_plus), (uses_minus, h_minus), (uses_two, second)):
            rounds = jnp.maximum(rounds, jnp.where(use, h + 1, 0))
        hop_plus[q] = h_plus
        hop_minus[q] = h_minus
        onward[q] = second
        side[q] = plus[q]
        here = my_chip == c
        write(here & uses_plus, h_plus, q & row_mask)
        write(here & uses_minus, TABLE + h_minus, q & row_mask)
        write((my_chip == right[c]) & (plus[q] == 1), second, chip_rows + h_plus)
        write((my_chip == left[c]) & (minus[q] == 1), TABLE + second, chip_rows + h_minus)
    info_ref[0] = rounds
    for j in range(chip_rows):
        q = parent_ref[0, my_chip * chip_rows + j]
        dist = (my_chip - (q >> row_bits)) & chip_mask
        at_plus = chip_rows + 2 * jnp.where(dist == 1, hop_plus[q], onward[q])
        at_minus = chip_rows + 2 * jnp.where(dist == 3, hop_minus[q], onward[q]) + 1
        from_plus = (dist == 1) | ((dist == 2) & (side[q] == 1))
        table_ref[2 * TABLE + j] = jnp.where(dist == 0, q & row_mask, jnp.where(from_plus, at_plus, at_minus))


def make_plan(parent, chips, chip_rows):
    total = chips * chip_rows
    smem = pl.BlockSpec(memory_space=pltpu.SMEM)
    return pl.pallas_call(
        functools.partial(plan_kernel, chips, chip_rows),
        out_shape=(jax.ShapeDtypeStruct((2 * TABLE + chip_rows + 1,), jnp.int32), jax.ShapeDtypeStruct((1,), jnp.int32)),
        in_specs=[smem],
        out_specs=(smem, smem),
        scratch_shapes=[pltpu.SMEM((total,), jnp.int32)] * 4,
        name="plan",
    )(parent)


def loop(n, body):
    def step(i, carry):
        body(i)
        return carry

    lax.fori_loop(0, n, step, 0)


class Copies:
    def __init__(self, copies):
        self.copies = copies

    def start(self):
        for copy in self.copies:
            copy.start()

    def wait(self):
        for copy in self.copies:
            copy.wait()


def step_kernel(rounds, beams, models, rows, heads, slots, d_model, ff, vocab, names, *refs):
    r = types.SimpleNamespace(**dict(zip(names, refs)))
    table, pos_ref, parent_ref = r.table, r.pos, r.parent
    k_ref, v_ref, k_out, v_out = r.k, r.v, r.k_out, r.v_out
    f32, bf16 = jnp.float32, jnp.bfloat16
    nchunk = CHUNKS
    block = slots * heads // nchunk
    span = slots // nchunk
    chips = beams // 2
    pair = 2 * rows
    lanes = LANES
    me = lax.axis_index("beam")
    core = lax.rem(me, 2)
    chip = me // 2
    is_k, is_v = core == 0, core == 1
    all_half, all_heads = pl.ds(0, d_model // 2), pl.ds(0, heads * LANES)
    sibling = me + 1 - 2 * core
    right = lax.rem(me + 2, beams)
    left = lax.rem(me + beams - 2, beams)
    model = lax.axis_index("model")
    mine = pl.ds(core * rows, rows)
    theirs = pl.ds((1 - core) * rows, rows)
    lane_iota = lax.broadcasted_iota(jnp.int32, (1, lanes), 1)
    pool, recv, send, stage, other = r.pool, r.recv, r.send, r.stage, r.other
    half = d_model // 2

    def to(peer):
        return dict(device_id={"beam": peer}, device_id_type=MESH)

    def across(m, peer):
        return dict(device_id={"model": m, "beam": peer}, device_id_type=MESH)

    def part(ref, c):
        return ref.at[:, pl.ds(c * block, block), :]

    def load_own(ref, c):
        return pltpu.make_async_copy(part(ref, c), pool[c].at[mine], r.pool_sem.at[c])

    def load_other(ref, c):
        return pltpu.make_async_copy(part(ref, c), other[c], r.other_sem.at[c])

    def swap(ref, c):
        return pltpu.make_async_remote_copy(part(ref, c), pool[c].at[mine], r.swap_send.at[c], r.swap_recv.at[c], **to(sibling))

    def hop(n, d, c):
        return pltpu.make_async_remote_copy(
            send[c].at[2 * n + d], recv[c].at[2 * n + d], r.hop_send.at[n, d, c], r.hop_recv.at[n, d, c], **to(right if d == 0 else left))

    def store_own(ref, c):
        return pltpu.make_async_copy(stage[c].at[mine], part(ref, c), r.out_sem.at[c])

    def give(ref, c):
        return pltpu.make_async_remote_copy(stage[c].at[theirs], part(ref, c), r.give_send.at[c], r.give_recv.at[c], **to(sibling))

    w_count = len(r.wbuf)
    groups = []

    def group(blocks):
        groups.append(blocks)

    for ref in (r.w_query, r.w_key, r.w_value):
        width = heads * lanes // 2
        group([(ref, pl.ds(1024 * i, 1024), pl.ds(core * width, width), pl.ds(0, 1024), pl.ds(i * width, width)) for i in range(d_model // 1024)])
    group([(r.w_out, all_heads, pl.ds(core * half, half), all_heads, all_half)])
    ff_core = (ff + 127) // 256 * 128
    ff_full = ff_core // 256
    ff_last = ff_core - 256 * ff_full
    ff_skip = 2 * ff_core - ff
    for i in range(ff_full + 1):
        n = 256 if i < ff_full else ff_last
        first = core * (ff_core - (ff_skip if i == ff_full else 0)) + 256 * i
        first = pl.multiple_of(first, 8)
        group([(ref, pl.ds(first, n), pl.ds(j * half, half), pl.ds(512 * j + n * u, n), all_half) for u, ref in enumerate((r.w_gate, r.w_up)) for j in range(2)])
    down_rows = []
    for i in range(0, 2 * ff_core, 1024):
        n = min(1024, 2 * ff_core - i)
        down_rows.append((i, n))
        blocks = [(i, n, 0)]
        if i + n > 2 * ff_core - ff_last:
            blocks = [(i, n - ff_last, 0), (ff - ff_last, ff_last, n - ff_last)]
        group([(r.w_down, pl.ds(a, b), pl.ds(core * half, half), pl.ds(c, b), all_half) for a, b, c in blocks])
    voc_core = (vocab + 1023) // 1024 * 512
    voc_groups = voc_core // 512
    voc_skip = 2 * voc_core - vocab
    for i in range(voc_groups):
        first = core * (voc_core - (voc_skip if i == voc_groups - 1 else 0)) + 512 * i
        first = pl.multiple_of(first, 8)
        group([(r.w_vocab, pl.ds(first, 512), pl.ds(j * half, half), pl.ds(512 * j, 512), all_half) for j in range(2)])

    def group_copies(g):
        return [pltpu.make_async_copy(ref.at[a, b], r.wbuf[g % w_count].at[c, e], r.w_sem.at[g, i]) for i, (ref, a, b, c, e) in enumerate(groups[g])]

    def load(g):
        if g < len(groups):
            for copy in group_copies(g):
                copy.start()

    taken = [0]

    def with_group(use):
        g = taken[0]
        taken[0] += 1
        for copy in group_copies(g):
            copy.wait()
        use(r.wbuf[g % w_count])
        load(g + w_count)

    barrier = pltpu.get_barrier_semaphore()
    peers = [lax.rem(me + s, beams) for s in range(1, beams)]
    model_peers = [lax.rem(model + s, models) for s in range(1, models)]
    for peer in peers:
        pl.semaphore_signal(barrier, **to(peer))
    for m in model_peers:
        for peer in (me, sibling):
            pl.semaphore_signal(barrier, **across(m, peer))

    @pl.when(is_k)
    def _():
        for c in range(nchunk):
            load_own(k_ref, c).start()

    @pl.when(is_v)
    def _():
        for c in range(nchunk):
            load_own(v_ref, c).start()

    load(0)
    prow = jnp.zeros((1, lanes), jnp.int32)
    for b in range(beams * rows):
        prow = jnp.where(lax.rem(lane_iota, beams * rows) == b, parent_ref[0, b], prow)
    for j in range(rows):
        r.score_rows[j : j + 1, :] = jnp.full((1, lanes), r.score[j])
    angles = pos_ref[0].astype(f32) * r.freq[...]
    cos_part = jnp.cos(angles)
    sin_part = jnp.where(lane_iota < lanes // 2, -1.0, 1.0) * jnp.sin(angles)
    pl.semaphore_wait(barrier, beams - 1 + 2 * (models - 1))

    x_swap = pltpu.make_async_remote_copy(r.x, r.x_got, r.pair_send.at[0], r.pair_recv.at[0], **to(sibling))
    x_swap.start()
    tell_scores = Copies(
        [pltpu.make_async_remote_copy(r.score_rows, r.scores.at[me], r.beam_send.at[1, s], r.beam_recv.at[1, s], **to(p)) for s, p in enumerate(peers)])
    tell_scores.start()

    @pl.when(is_k)
    def _():
        for c in range(nchunk):
            swap(v_ref, c).start()

    @pl.when(is_v)
    def _():
        for c in range(nchunk):
            swap(k_ref, c).start()

    for g in range(1, w_count):
        load(g)

    @pl.when(is_k)
    def _():
        for c in range(nchunk):
            load_other(v_ref, c).start()

    @pl.when(is_v)
    def _():
        for c in range(nchunk):
            load_other(k_ref, c).start()

    strip = min(block, 128)

    def build(n, c):
        for d in SIDES:
            code = table[d * TABLE + n]
            row = jnp.minimum(code, pair - 1)

            def body(i):
                at = pl.ds(pl.multiple_of(i * strip, strip), strip)
                x = pool[c][row, at, :]
                for e in range(n):
                    x = jnp.where(code == pair + e, recv[c][2 * e + d, at, :], x)
                send[c][2 * n + d, at, :] = x

            loop(block // strip, body)
        for d in SIDES:
            hop(n, d, c).start()

    waited = set()

    def have_own(c):
        if c not in waited:
            waited.add(c)
            load_own(k_ref, c).wait()

    def first_round(c):
        have_own(c)
        swap(k_ref, c).wait_recv()
        build(0, c)

    def later_round(n, c):
        for d in SIDES:
            hop(n - 1, d, c).wait_recv()
        build(n, c)

    def finish(c):
        for d in SIDES:
            hop(rounds - 1, d, c).wait_recv()
        position = pos_ref[0]

        def put_row(j):
            where = table[2 * TABLE + j]
            row = jnp.minimum(where, pair - 1)
            slot = jnp.clip(where - pair, 0, 2 * rounds - 1)
            new = jnp.concatenate([r.fresh[j]] * (strip // heads))

            def body(i):
                at = pl.ds(pl.multiple_of(i * strip, strip), strip)
                x = jnp.where(where < pair, pool[c][row, at, :], recv[c][slot, at, :])
                here = (lax.broadcasted_iota(jnp.int32, (strip, lanes), 0) + i * strip) // heads + c * span
                stage[c][j, at, :] = jnp.where(here == position, new, x.astype(f32)).astype(bf16)

            loop(block // strip, body)

        loop(pair, put_row)

        @pl.when(is_k)
        def _():
            give(k_out, c).start()
            store_own(k_out, c).start()

        @pl.when(is_v)
        def _():
            give(v_out, c).start()
            store_own(v_out, c).start()

    todo = [functools.partial(first_round, c) for c in range(nchunk)]
    todo += [functools.partial(later_round, n, c) for n in range(1, rounds) for c in range(nchunk)]

    def serve(n=1):
        for _ in range(n):
            if todo:
                todo.pop(0)()

    res = r.res

    def normed(gain_ref):
        x = res[...]
        inv = lax.rsqrt(jnp.mean(x * x, axis=-1, keepdims=True) + NORM_EPS)
        r.h[...] = (x * inv * gain_ref[...].astype(f32)).astype(bf16)

    def dot(a, b):
        return jnp.dot(a, b, preferred_element_type=f32)

    def dot_halves(w, n):
        def body(j, x):
            a = h[:, pl.ds(pl.multiple_of(j * half, lanes), half)]
            b = w[pl.ds(pl.multiple_of(j * 512, 512), n), :]
            return x + lax.dot_general(a, b, (((1,), (1,)), ((), ())), preferred_element_type=f32)

        return lax.fori_loop(0, 2, body, jnp.zeros((pair, n), f32))

    def dot_rows(a, first, w, n):
        def body(j, x):
            at = pl.multiple_of(j * (n // 2), lanes)
            return x + dot(a[:, pl.ds(first + at, n // 2)], w[pl.ds(at, n // 2), :])

        return lax.fori_loop(0, 2, body, jnp.zeros((pair, half), f32))

    def exchange_model(part_ref, got_ref, phase):
        if models == 1:
            return part_ref[...]
        copies = [
            pltpu.make_async_remote_copy(part_ref, got_ref.at[model], r.model_send.at[phase, s], r.model_recv.at[phase, s], **across(m, me))
            for s, m in enumerate(model_peers)]
        for copy in copies:
            copy.start()
        got_ref[model] = part_ref[...]
        serve(2)
        for copy in copies:
            copy.wait()
        total = got_ref[0]
        for m in range(1, models):
            total = total + got_ref[m]
        return total

    serve()
    x_swap.wait()

    @pl.when(is_k)
    def _():
        res[0:rows, :] = r.x[...].astype(f32)
        res[rows:pair, :] = r.x_got[...].astype(f32)

    @pl.when(is_v)
    def _():
        res[0:rows, :] = r.x_got[...].astype(f32)
        res[rows:pair, :] = r.x[...].astype(f32)

    normed(r.gain_attn)
    h = r.h
    head_half = heads // 2
    width = head_half * lanes
    qkv = r.qkv
    for kind in range(3):
        def use(w, kind=kind):
            blocks = d_model // 1024
            each = min(2, blocks)

            def body(i, z):
                for e in range(each):
                    at = i * each + e
                    a = h[:, pl.ds(pl.multiple_of(at * 1024, 1024), 1024)]
                    z = z + dot(a, w[:, pl.ds(pl.multiple_of(at * width, lanes), width)])
                return z

            z = lax.fori_loop(0, blocks // each, body, jnp.zeros((pair, width), f32))
            for n in range(head_half):
                y = z[:, n * lanes : (n + 1) * lanes]
                if kind < 2:
                    y = y * cos_part + pltpu.roll(y, lanes // 2, 1) * sin_part
                qkv[kind, n] = y.astype(bf16)
        with_group(use)

    qkv_all = r.qkv_all
    to_parents = Copies(
        [pltpu.make_async_remote_copy(qkv, qkv_all.at[me], r.beam_send.at[0, s], r.beam_recv.at[0, s], **to(p)) for s, p in enumerate(peers)]
        )
    to_parents.start()
    qkv_all[me] = qkv[...]
    serve(2)
    to_parents.wait()

    cat = r.cat
    for kind in range(3):
        for n in range(heads):
            for x in range(chips):
                at = n * beams * rows + x * pair
                cat[kind, at : at + pair, :] = qkv_all[2 * x + n // head_half, kind, n % head_half].astype(f32)
    for j in range(pair):
        at = pl.ds(chip * pair + j, heads, stride=beams * rows)
        r.fresh[j] = jnp.where(is_k, cat[1, at, :], cat[2, at, :])

    query_t = cat[0].T.astype(bf16)
    new_k = cat[1].astype(bf16)
    total_cols = heads * beams * rows
    tiles = total_cols // lanes
    heads_tile = heads // tiles
    lane_head = lane_iota // (beams * rows)
    spread = r.spread
    logit = r.logit
    position = pos_ref[0]

    def own_rows(c, p, kind):
        a = pool[c][core * rows + p]
        b = other[c][p]
        return jnp.where(core == kind, a, b)

    def score_chunk(c):
        have_own(c)
        load_other(k_ref, c).wait()

        def body(p):
            full = dot(own_rows(c, p, 0), query_t)
            for t in range(tiles):
                spread[t][...] = full[:, t * lanes : (t + 1) * lanes]
            for t in range(tiles):
                here = prow == me * rows + p
                at = pl.ds(c * span, span)
                x = logit[t][at, :]
                for n in range(heads_tile):
                    got = spread[t][pl.ds(t * heads_tile + n, span, stride=heads), :]
                    x = jnp.where(here & (lane_head == n), got, x)
                logit[t][at, :] = x

        loop(rows, body)

    for t in range(tiles):
        logit[t][...] = jnp.zeros_like(logit[t])
    self_full = dot(new_k, query_t)
    scale = lanes ** -0.5
    for c in range(nchunk):
        score_chunk(c)
        serve(c == nchunk // 2)
    slot_index = lax.broadcasted_iota(jnp.int32, (slots, lanes), 0)
    self_prob = []
    for t in range(tiles):
        diag = lax.broadcasted_iota(jnp.int32, (total_cols, lanes), 0) == lax.broadcasted_iota(jnp.int32, (total_cols, lanes), 1) + t * lanes
        self_row = jnp.sum(jnp.where(diag, self_full[:, t * lanes : (t + 1) * lanes], 0.0), axis=0, keepdims=True)
        x = jnp.where(slot_index == position, self_row, logit[t][...]) * scale
        x = jnp.where(slot_index <= position, x, -jnp.inf)
        e = jnp.exp(x - jnp.max(x, axis=0, keepdims=True))
        prob = e / jnp.sum(e, axis=0, keepdims=True)
        logit[t][...] = jnp.where(slot_index == position, 0.0, prob)
        self_prob.append(jnp.sum(jnp.where(slot_index == position, prob, 0.0), axis=0, keepdims=True))
    for t in range(tiles):
        spread[t][...] = jnp.zeros_like(spread[t])
    out_t = r.out_t
    out_t[...] = cat[2].T * jnp.concatenate(self_prob, axis=1).astype(bf16).astype(f32)

    def value_chunk(c):
        def body(p):
            for t in range(tiles):
                here = prow == me * rows + p
                x = logit[t][pl.ds(c * span, span), :]
                for n in range(heads_tile):
                    spread[t][pl.ds(t * heads_tile + n, span, stride=heads), :] = jnp.where(here & (lane_head == n), x, 0.0)
            prob = jnp.concatenate([spread[t][...].astype(bf16) for t in range(tiles)], axis=1)
            out_t[...] += lax.dot_general(own_rows(c, p, 1), prob, (((0,), (0,)), ((), ())), preferred_element_type=f32)

        loop(rows, body)

    for c in range(nchunk):
        value_chunk(c)
        serve(c % 4 == 0)
    local = jnp.concatenate([prow] * tiles, axis=1) // rows == me
    o_rows = jnp.where(local, out_t[...], 0.0).T
    o_send, o_got = r.o_send, r.o_got
    for x in range(chips):
        for n in range(heads):
            at = n * beams * rows + x * pair
            o_send[x, n] = o_rows[at : at + pair, :].astype(bf16)
    back = Copies([
        pltpu.make_async_remote_copy(o_send.at[lax.rem(me + s, beams) // 2], o_got.at[me], r.beam_send.at[2, s - 1], r.beam_recv.at[2, s - 1], **to(lax.rem(me + s, beams)))
        for s in range(1, beams)])
    back.start()
    o_got[me] = o_send[chip]
    serve(3)
    back.wait()
    for n in range(heads):
        x = o_got[0, n].astype(f32)
        for s in range(1, beams):
            x = x + o_got[s, n].astype(f32)
        r.o[:, n * lanes : (n + 1) * lanes] = x.astype(bf16)

    part_sum, model_got, res_half, res_got = r.part, r.model_got, r.res_half, r.res_got

    def add_to_residual(phase):
        total = exchange_model(part_sum, model_got.at[phase] if models > 1 else None, phase)
        col = pl.ds(pl.multiple_of(core * half, lanes), half)
        other_col = pl.ds(pl.multiple_of((1 - core) * half, lanes), half)
        fresh = res[:, col] + total
        res_half[phase] = fresh
        trade = pltpu.make_async_remote_copy(res_half.at[phase], res_got.at[phase], r.pair_send.at[1 + phase], r.pair_recv.at[1 + phase], **to(sibling))
        trade.start()
        res[:, col] = fresh
        trade.wait()
        res[:, other_col] = res_got[phase]

    def use_out(w):
        part_sum[0] = dot_rows(r.o, 0, w, heads * lanes)
    with_group(use_out)
    serve(2)
    part_sum_ref = part_sum
    part_sum = part_sum_ref.at[0]
    add_to_residual(0)
    normed(r.gain_mlp)

    g_own, g_got, g_all = r.g_own, r.g_got, r.g_all
    for i in range(ff_full + 1):
        n = 256 if i < ff_full else ff_last

        def use(w, i=i, n=n):
            z = dot_halves(w, 2 * n)
            gate, up = z[:, :n], z[:, n:]
            y = jax.nn.silu(gate) * up
            if i == ff_full and ff_skip:
                y = jnp.where(is_v & (lax.broadcasted_iota(jnp.int32, (1, n), 1) < ff_skip), 0.0, y)
            g_own[:, 256 * i : 256 * i + n] = y.astype(bf16)
        with_group(use)
        serve(i % 2)
    g_trade = pltpu.make_async_remote_copy(g_own, g_got, r.pair_send.at[3], r.pair_recv.at[3], **to(sibling))
    g_trade.start()
    serve()
    g_all[:, pl.ds(pl.multiple_of(core * ff_core, lanes), ff_core)] = g_own[...]
    g_trade.wait()
    g_all[:, pl.ds(pl.multiple_of((1 - core) * ff_core, lanes), ff_core)] = g_got[...]
    part_sum = part_sum_ref.at[1]
    for at, n in down_rows:
        def use(w, at=at, n=n):
            x = dot_rows(g_all, at, w, n)
            part_sum[...] = x if at == 0 else part_sum[...] + x
        with_group(use)
    serve(2)
    add_to_residual(1)
    normed(r.gain_final)

    word = r.word
    for i in range(voc_groups):
        def use(w, i=i):
            word[:, 512 * i : 512 * (i + 1)] = dot_halves(w, 512)
        with_group(use)
        serve(i % 2)
    word_send, word_got = r.word_send, r.word_got
    x = word[...]
    word_send[0] = x[0:rows]
    word_send[1] = x[rows:pair]
    word_trade = pltpu.make_async_remote_copy(word_send.at[1 - core], word_got, r.pair_send.at[4], r.pair_recv.at[4], **to(sibling))
    word_trade.start()
    col = lax.broadcasted_iota(jnp.int32, (1, voc_core), 1)
    twice = is_v & (col >= voc_core - 512) & (col < voc_core - 512 + voc_skip)
    x = jnp.where(twice, -jnp.inf, x)
    top = jnp.max(x, axis=-1, keepdims=True)
    mass = jnp.sum(jnp.exp(x - top), axis=-1, keepdims=True)
    stat, stats = r.stat, r.stats
    stat[0] = jnp.broadcast_to(top, (pair, lanes))
    stat[1] = jnp.broadcast_to(mass, (pair, lanes))
    mates = [(m, p) for m in [model] + model_peers for p in (me, sibling)][1:]
    told = Copies([
        pltpu.make_async_remote_copy(stat, stats.at[2 * model + core], r.stat_send.at[i], r.stat_recv.at[i], **across(m, p))
        for i, (m, p) in enumerate(mates)])
    told.start()
    stats[2 * model + core] = stat[...]
    serve(len(todo))
    for c in range(nchunk // 2):
        finish(c)
    told.wait()
    top = stats[0, 0]
    for i in range(1, 2 * models):
        top = jnp.maximum(top, stats[i, 0])
    mass = stats[0, 1] * jnp.exp(stats[0, 0] - top)
    for i in range(1, 2 * models):
        mass = mass + stats[i, 1] * jnp.exp(stats[i, 0] - top)
    r.stat[0] = top
    r.stat[1] = jnp.log(mass)
    word_trade.wait()
    tell_scores.wait()
    r.scores[me] = r.score_rows[...]
    own, got = word_send[core], word_got[...]
    low, high = jnp.where(is_k, own, got), jnp.where(is_k, got, own)
    last = voc_core - 512
    for j in range(rows):
        q = parent_ref[0, me * rows + j]
        base = r.scores[q // rows, pl.ds(lax.rem(q, rows), 1), :][:, 0:1]
        at = pl.ds(core * rows + j, 1)
        shift = stat[0, at, 0:1]
        log_mass = stat[1, at, 0:1]
        row = slice(j, j + 1)
        x = base + (high[row] - shift - log_mass)
        r.word_out[row, :voc_core] = base + (low[row] - shift - log_mass)
        r.word_out[row, voc_core : voc_core + last] = x[:, :last]
        r.word_out[row, voc_core + last :] = x[:, last + voc_skip :]

    for c in range(nchunk // 2, nchunk):
        finish(c)
    for c in range(nchunk):
        swap(k_ref, c).wait_send()
        for n in range(rounds):
            for d in SIDES:
                hop(n, d, c).wait_send()
        store_own(k_out, c).wait()
        give(k_out, c).wait()


def run_step(rounds, beams, models, table, pos, parent, score, freq, x, k_rows, v_rows, gains, weights):
    rows, length, lanes = k_rows.shape
    weights_ = types.SimpleNamespace(**weights)
    d_model = x.shape[1]
    heads = weights_.w_query.shape[1] // lanes
    slots = length // heads
    ff = weights_.w_down.shape[0]
    vocab = weights_.w_vocab.shape[0]
    block = length // CHUNKS
    pair = 2 * rows
    half = d_model // 2
    chips = beams // 2
    cols = heads * beams * rows
    bf16, f32 = jnp.bfloat16, jnp.float32
    vmem, dma = pltpu.VMEM, pltpu.SemaphoreType.DMA
    smem, hbm, ram = (pl.BlockSpec(memory_space=s) for s in (pltpu.SMEM, pl.ANY, pltpu.VMEM))
    voc_core = (vocab + 1023) // 1024 * 512
    ff_core = (ff + 127) // 256 * 128
    n_groups = 4 + ff_core // 256 + 1 + -(-2 * ff_core // 1024) + voc_core // 512
    ins = dict(table=(table, smem), pos=(pos, smem), parent=(parent, smem), score=(score, smem), freq=(freq, ram),
               x=(x, ram), k=(k_rows, hbm), v=(v_rows, hbm))
    ins.update({name: (a, ram) for name, a in gains.items()})
    ins.update({name: (a, hbm) for name, a in weights.items()})
    outs = dict(k_out=(jax.ShapeDtypeStruct(k_rows.shape, bf16), hbm), v_out=(jax.ShapeDtypeStruct(k_rows.shape, bf16), hbm),
                word_out=(jax.ShapeDtypeStruct((rows, vocab), f32), ram))
    scratch = dict(
        pool=[vmem((pair, block, lanes), bf16)] * CHUNKS,
        recv=[vmem((2 * rounds, block, lanes), bf16)] * CHUNKS,
        send=[vmem((2 * rounds, block, lanes), bf16)] * CHUNKS,
        stage=[vmem((pair, block, lanes), bf16)] * CHUNKS,
        other=[vmem((rows, block, lanes), bf16)] * CHUNKS,
        wbuf=[vmem((1024, half), bf16)] * (W_BUFFERS - rounds),
        spread=[vmem((block, lanes), f32)] * (cols // lanes),
        logit=[vmem((slots, lanes), f32)] * (cols // lanes),
        x_got=vmem(x.shape, bf16),
        res=vmem((pair, d_model), f32),
        h=vmem((pair, d_model), bf16),
        qkv=vmem((3, heads // 2, pair, lanes), bf16),
        qkv_all=vmem((beams, 3, heads // 2, pair, lanes), bf16),
        scores=vmem((beams, rows, lanes), f32),
        score_rows=vmem((rows, lanes), f32),
        cat=vmem((3, cols, lanes), f32),
        fresh=vmem((pair, heads, lanes), f32),
        out_t=vmem((lanes, cols), f32),
        o_send=vmem((chips, heads, pair, lanes), bf16),
        o_got=vmem((beams, heads, pair, lanes), bf16),
        o=vmem((pair, heads * lanes), bf16),
        part=vmem((2, pair, half), f32),
        model_got=vmem((2, models, pair, half), f32),
        res_half=vmem((2, pair, half), f32),
        res_got=vmem((2, pair, half), f32),
        g_own=vmem((pair, ff_core), bf16),
        g_got=vmem((pair, ff_core), bf16),
        g_all=vmem((pair, 2 * ff_core), bf16),
        word=vmem((pair, voc_core), f32),
        word_send=vmem((2, rows, voc_core), f32),
        word_got=vmem((rows, voc_core), f32),
        stat=vmem((2, pair, lanes), f32),
        stats=vmem((2 * models, 2, pair, lanes), f32),
        w_sem=dma((n_groups, 4)),
        pool_sem=dma((CHUNKS,)), other_sem=dma((CHUNKS,)), swap_send=dma((CHUNKS,)), swap_recv=dma((CHUNKS,)),
        hop_send=dma((rounds, 2, CHUNKS)), hop_recv=dma((rounds, 2, CHUNKS)),
        out_sem=dma((CHUNKS,)), give_send=dma((CHUNKS,)), give_recv=dma((CHUNKS,)),
        pair_send=dma((5,)), pair_recv=dma((5,)),
        beam_send=dma((3, beams)), beam_recv=dma((3, beams)),
        model_send=dma((2, models)), model_recv=dma((2, models)),
        stat_send=dma((2 * models,)), stat_recv=dma((2 * models,)),
    )
    flat, places = [], {}
    for name, s in scratch.items():
        many = isinstance(s, list)
        places[name] = (len(flat), len(s) if many else None)
        flat += s if many else [s]
    first = list(ins) + list(outs)

    def kernel(*refs):
        named = list(refs[: len(first)])
        rest = refs[len(first) :]
        for start, count in places.values():
            named.append(rest[start] if count is None else list(rest[start : start + count]))
        step_kernel(rounds, beams, models, rows, heads, slots, d_model, ff, vocab, first + list(places), *named)

    return pl.pallas_call(
        kernel,
        out_shape=tuple(s for s, _ in outs.values()),
        in_specs=[s for _, s in ins.values()],
        out_specs=tuple(s for _, s in outs.values()),
        scratch_shapes=flat,
        compiler_params=pltpu.CompilerParams(collective_id=rounds, has_side_effects=True, vmem_limit_bytes=VMEM_LIMIT),
        name=f"step{rounds}",
    )(*[a for a, _ in ins.values()])


def copy_kernel(pieces, a_ref, b_ref, a_out, b_out, buf, in_sem, out_sem):
    rows, length, _ = a_ref.shape
    per = rows // pieces
    jobs = [(src, dst, i) for i in range(pieces) for src, dst in ((a_ref, a_out), (b_ref, b_out))]

    def get(n):
        src, _, i = jobs[n]
        return pltpu.make_async_copy(src.at[pl.ds(i * per, per)], buf.at[n], in_sem.at[n])

    def put(n):
        _, dst, i = jobs[n]
        return pltpu.make_async_copy(buf.at[n], dst.at[pl.ds(i * per, per)], out_sem.at[n])

    for n in range(len(jobs)):
        get(n).start()
    for n in range(len(jobs)):
        get(n).wait()
        put(n).start()
    for n in range(len(jobs)):
        put(n).wait()


def settle(a, b):
    rows, length, lanes = a.shape
    hbm = pl.BlockSpec(memory_space=pl.ANY)
    out = jax.ShapeDtypeStruct(a.shape, a.dtype)
    return pl.pallas_call(
        functools.partial(copy_kernel, rows),
        out_shape=(out, out),
        in_specs=[hbm, hbm],
        out_specs=(hbm, hbm),
        scratch_shapes=[pltpu.VMEM((2 * rows, 1, length, lanes), a.dtype), pltpu.SemaphoreType.DMA((2 * rows,)), pltpu.SemaphoreType.DMA((2 * rows,))],
        name="settle",
    )(a, b)


def move_any(beams, heads, parent, position, k_rows, v_rows, k_new, v_new):
    rows, length, _ = k_rows.shape
    me = lax.axis_index("beam")
    mine = lax.dynamic_slice(parent.reshape(-1), (me * rows,), (rows,))
    local = lax.rem(mine, rows)
    ring = [(i, (i + 1) % beams) for i in range(beams)]

    def choose(source, here, chosen):
        hit = (mine // rows == source)[:, None, None]
        return jnp.where(hit, jnp.take(here, local, axis=0), chosen)

    def step(s, carry):
        k_here, v_here, k_sel, v_sel = carry
        source = lax.rem(me - s + beams, beams)
        k_sel, v_sel = choose(source, k_here, k_sel), choose(source, v_here, v_sel)
        return lax.ppermute(k_here, "beam", ring), lax.ppermute(v_here, "beam", ring), k_sel, v_sel

    carry = (lax.ppermute(k_rows, "beam", ring), lax.ppermute(v_rows, "beam", ring), choose(me, k_rows, k_new), choose(me, v_rows, v_new))
    carry = lax.fori_loop(1, beams, step, carry)
    written = (jnp.arange(length) // heads == position)[None, :, None]
    return jnp.where(written, k_new, carry[2]), jnp.where(written, v_new, carry[3])


def solution(mesh):
    beams = mesh.shape["beam"]
    models = mesh.shape["model"]
    cache_spec = P(None, ('data', 'beam'), None, 'model', None)
    col_spec = P(None, None, 'model')
    row_spec = P(None, 'model', None)
    in_specs = (P(('data', 'beam'), None), P('data', None), P(), P(('data', 'beam')), cache_spec, cache_spec,
                P(), col_spec, col_spec, col_spec, row_spec, P(), col_spec, col_spec, row_spec, P(), P(None, 'model'))
    out_specs = (cache_spec, cache_spec, P(('data', 'beam'), 'model'))

    def local_step(x_embed, parent, position, score, k_cache, v_cache, gain_attn, w_query, w_key, w_value, w_out, gain_mlp, w_gate, w_up, w_down, gain_final, w_vocab):
        rows = x_embed.shape[0]
        _, _, slots, heads, lanes = k_cache.shape
        table, info = make_plan(parent, beams // 2, 2 * rows)
        k_rows = k_cache.reshape(rows, slots * heads, lanes)
        v_rows = v_cache.reshape(rows, slots * heads, lanes)
        half_dim = lanes // 2
        freq = np.float32(ROPE_BASE) ** (-np.arange(half_dim, dtype=np.float32) / np.float32(half_dim))
        freq = jnp.asarray(np.concatenate([freq, freq])[None])
        pos = position.reshape(1)
        gains = dict(gain_attn=gain_attn, gain_mlp=gain_mlp, gain_final=gain_final.reshape(1, -1))
        weights = dict(w_query=w_query[0], w_key=w_key[0], w_value=w_value[0], w_out=w_out[0],
                       w_gate=w_gate[0].T, w_up=w_up[0].T, w_down=w_down[0], w_vocab=w_vocab.T)
        def step(rounds):
            return run_step(rounds, beams, models, table, pos, parent, score, freq, x_embed, k_rows, v_rows, gains, weights)

        def few(_):
            k_new, v_new, word = step(ROUND_CHOICES[0])
            return *settle(k_new, v_new), word

        def more(_):
            k_new, v_new, word = step(ROUND_CHOICES[1])
            enough = info[0] <= ROUND_CHOICES[1]
            k_new, v_new = lax.cond(enough, settle, lambda a, b: move_any(beams, heads, parent, position, k_rows, v_rows, a, b), k_new, v_new)
            return k_new, v_new, word

        k_new, v_new, candidates = lax.cond(info[0] <= ROUND_CHOICES[0], few, more, 0)
        shape = (1, rows, slots, heads, lanes)
        return k_new.reshape(shape), v_new.reshape(shape), candidates

    return jax.shard_map(local_step, mesh=mesh, in_specs=in_specs, out_specs=out_specs, check_vma=False)
```

```python
import functools
import types

import jax
import jax.numpy as jnp
from jax import lax
from jax.experimental import pallas as pl
from jax.experimental.pallas import tpu as pltpu
import numpy as np
from jax.sharding import PartitionSpec as P

NORM_EPS = 1e-6
ROPE_BASE = 10000.0
MESH = pl.DeviceIdType.MESH
CHUNKS = 8
TABLE = 24
ROUND_CHOICES = (3, 4)
W_BUFFERS = 9
SETTLE_PIECES = 4
SIDES = (0, 1)
LANES = 128
VMEM_LIMIT = 66 * 10**6


def plan_kernel(chips, chip_rows, parent_ref, table_ref, info_ref, hop_plus, hop_minus, onward, side):
    total = chips * chip_rows
    my_chip = lax.axis_index("beam") // 2
    row_bits, chip_mask, row_mask = chip_rows.bit_length() - 1, chips - 1, chip_rows - 1
    spare = 2 * TABLE + chip_rows

    near, far, back = [jnp.int32(0)] * 3
    parents = [parent_ref[0, b] for b in range(total)]
    for b, q in enumerate(parents):
        dist = ((b >> row_bits) - (q >> row_bits)) & chip_mask
        bit = jnp.left_shift(1, q)
        near |= jnp.where(dist == 1, bit, 0)
        far |= jnp.where(dist == 2, bit, 0)
        back |= jnp.where(dist == 3, bit, 0)

    def bit_of(mask, q):
        return jnp.right_shift(mask, q) & 1

    every = [(q, q >> row_bits, bit_of(near, q), bit_of(far, q), bit_of(back, q)) for q in range(total)]
    right = [(c + 1) & chip_mask for c in range(chips)]
    left = [(c - 1) & chip_mask for c in range(chips)]
    load_plus, load_minus, own_plus, own_minus, two_plus, two_minus = [[jnp.int32(0)] * chips for _ in range(6)]
    plus, minus = [], []
    for q, c, a, b, d in every:
        plus.append(b & a & (1 - d))
        minus.append(b & d & (1 - a))
        own_plus[c] += a
        own_minus[c] += d
        load_plus[right[c]] += plus[q]
        load_minus[left[c]] += minus[q]
    load_plus = [x + y for x, y in zip(load_plus, own_plus)]
    load_minus = [x + y for x, y in zip(load_minus, own_minus)]
    for q, c, a, b, d in every:
        flex = b & (1 - (a ^ d))
        cost_plus = jnp.maximum(load_plus[c] - a, load_plus[right[c]])
        cost_minus = jnp.maximum(load_minus[c] - d, load_minus[left[c]])
        go = jnp.where(cost_plus <= cost_minus, flex, 0)
        stay = flex - go
        for load, own, x, y in ((load_plus, own_plus, go, a), (load_minus, own_minus, stay, d)):
            load[c] += x & (1 - y)
            own[c] += x & (1 - y)
        load_plus[right[c]] += go
        load_minus[left[c]] += stay
        plus[q] += go
        minus[q] += stay
    first_plus, first_minus = [], []
    for q, c, *_ in every:
        first_plus.append(two_plus[c])
        first_minus.append(two_minus[c])
        two_plus[c] += plus[q]
        two_minus[c] += minus[q]
    rounds = jnp.int32(0)

    for at in range(spare):
        table_ref[at] = 0

    def write(cond, place, value):
        table_ref[jnp.where(cond, place, spare)] = value

    for q, c, a, b, d in every:
        a, d = a & (1 - plus[q]), d & (1 - minus[q])
        h_plus = jnp.where(a == 1, two_plus[c], first_plus[q])
        h_minus = jnp.where(d == 1, two_minus[c], first_minus[q])
        two_plus[c] += a
        two_minus[c] += d
        second = jnp.where(plus[q] == 1, jnp.maximum(own_plus[right[c]], 1) + h_plus, jnp.maximum(own_minus[left[c]], 1) + h_minus)
        uses_plus, uses_minus, uses_two = (a + plus[q]) == 1, (d + minus[q]) == 1, (plus[q] + minus[q]) == 1
        for use, h in ((uses_plus, h_plus), (uses_minus, h_minus), (uses_two, second)):
            rounds = jnp.maximum(rounds, jnp.where(use, h + 1, 0))
        hop_plus[q] = h_plus
        hop_minus[q] = h_minus
        onward[q] = second
        side[q] = plus[q]
        here = my_chip == c
        write(here & uses_plus, h_plus, q & row_mask)
        write(here & uses_minus, TABLE + h_minus, q & row_mask)
        write((my_chip == right[c]) & (plus[q] == 1), second, chip_rows + h_plus)
        write((my_chip == left[c]) & (minus[q] == 1), TABLE + second, chip_rows + h_minus)
    info_ref[0] = rounds
    for j in range(chip_rows):
        q = parent_ref[0, my_chip * chip_rows + j]
        dist = (my_chip - (q >> row_bits)) & chip_mask
        at_plus = chip_rows + 2 * jnp.where(dist == 1, hop_plus[q], onward[q])
        at_minus = chip_rows + 2 * jnp.where(dist == 3, hop_minus[q], onward[q]) + 1
        from_plus = (dist == 1) | ((dist == 2) & (side[q] == 1))
        table_ref[2 * TABLE + j] = jnp.where(dist == 0, q & row_mask, jnp.where(from_plus, at_plus, at_minus))


def make_plan(parent, chips, chip_rows):
    total = chips * chip_rows
    smem = pl.BlockSpec(memory_space=pltpu.SMEM)
    return pl.pallas_call(
        functools.partial(plan_kernel, chips, chip_rows),
        out_shape=(jax.ShapeDtypeStruct((2 * TABLE + chip_rows + 1,), jnp.int32), jax.ShapeDtypeStruct((1,), jnp.int32)),
        in_specs=[smem],
        out_specs=(smem, smem),
        scratch_shapes=[pltpu.SMEM((total,), jnp.int32)] * 4,
        name="plan",
    )(parent)


def loop(n, body):
    def step(i, carry):
        body(i)
        return carry

    lax.fori_loop(0, n, step, 0)


class Copies:
    def __init__(self, copies):
        self.copies = copies

    def start(self):
        for copy in self.copies:
            copy.start()

    def wait(self):
        for copy in self.copies:
            copy.wait()


def step_kernel(rounds, beams, models, rows, heads, slots, d_model, ff, vocab, names, *refs):
    r = types.SimpleNamespace(**dict(zip(names, refs)))
    table, pos_ref, parent_ref = r.table, r.pos, r.parent
    k_ref, v_ref, k_out, v_out = r.k, r.v, r.k_out, r.v_out
    f32, bf16 = jnp.float32, jnp.bfloat16
    nchunk = CHUNKS
    block = slots * heads // nchunk
    span = slots // nchunk
    chips = beams // 2
    pair = 2 * rows
    lanes = LANES
    me = lax.axis_index("beam")
    core = lax.rem(me, 2)
    chip = me // 2
    is_k, is_v = core == 0, core == 1
    all_half, all_heads = pl.ds(0, d_model // 2), pl.ds(0, heads * LANES)
    sibling = me + 1 - 2 * core
    right = lax.rem(me + 2, beams)
    left = lax.rem(me + beams - 2, beams)
    model = lax.axis_index("model")
    mine = pl.ds(core * rows, rows)
    theirs = pl.ds((1 - core) * rows, rows)
    lane_iota = lax.broadcasted_iota(jnp.int32, (1, lanes), 1)
    pool, recv, send, stage, other = r.pool, r.recv, r.send, r.stage, r.other
    half = d_model // 2

    def to(peer):
        return dict(device_id={"beam": peer}, device_id_type=MESH)

    def across(m, peer):
        return dict(device_id={"model": m, "beam": peer}, device_id_type=MESH)

    def part(ref, c):
        return ref.at[:, pl.ds(c * block, block), :]

    def load_own(ref, c):
        return pltpu.make_async_copy(part(ref, c), pool[c].at[mine], r.pool_sem.at[c])

    def load_other(ref, c):
        return pltpu.make_async_copy(part(ref, c), other[c], r.other_sem.at[c])

    def swap(ref, c):
        return pltpu.make_async_remote_copy(part(ref, c), pool[c].at[mine], r.swap_send.at[c], r.swap_recv.at[c], **to(sibling))

    def hop(n, d, c):
        return pltpu.make_async_remote_copy(
            send[c].at[2 * n + d], recv[c].at[2 * n + d], r.hop_send.at[n, d, c], r.hop_recv.at[n, d, c], **to(right if d == 0 else left))

    def store_own(ref, c):
        return pltpu.make_async_copy(stage[c].at[mine], part(ref, c), r.out_sem.at[c])

    def give(ref, c):
        return pltpu.make_async_remote_copy(stage[c].at[theirs], part(ref, c), r.give_send.at[c], r.give_recv.at[c], **to(sibling))

    w_count = len(r.wbuf)
    groups = []

    def group(blocks):
        groups.append(blocks)

    for ref in (r.w_query, r.w_key, r.w_value):
        width = heads * lanes // 2
        group([(ref, pl.ds(1024 * i, 1024), pl.ds(core * width, width), pl.ds(0, 1024), pl.ds(i * width, width)) for i in range(d_model // 1024)])
    group([(r.w_out, all_heads, pl.ds(core * half, half), all_heads, all_half)])
    ff_core = (ff + 127) // 256 * 128
    ff_full = ff_core // 256
    ff_last = ff_core - 256 * ff_full
    ff_skip = 2 * ff_core - ff
    for i in range(ff_full + 1):
        n = 256 if i < ff_full else ff_last
        first = core * (ff_core - (ff_skip if i == ff_full else 0)) + 256 * i
        first = pl.multiple_of(first, 8)
        group([(ref, pl.ds(first, n), pl.ds(j * half, half), pl.ds(512 * j + n * u, n), all_half) for u, ref in enumerate((r.w_gate, r.w_up)) for j in range(2)])
    down_rows = []
    for i in range(0, 2 * ff_core, 1024):
        n = min(1024, 2 * ff_core - i)
        down_rows.append((i, n))
        blocks = [(i, n, 0)]
        if i + n > 2 * ff_core - ff_last:
            blocks = [(i, n - ff_last, 0), (ff - ff_last, ff_last, n - ff_last)]
        group([(r.w_down, pl.ds(a, b), pl.ds(core * half, half), pl.ds(c, b), all_half) for a, b, c in blocks])
    voc_core = (vocab + 1023) // 1024 * 512
    voc_groups = voc_core // 512
    voc_skip = 2 * voc_core - vocab
    for i in range(voc_groups):
        first = core * (voc_core - (voc_skip if i == voc_groups - 1 else 0)) + 512 * i
        first = pl.multiple_of(first, 8)
        group([(r.w_vocab, pl.ds(first, 512), pl.ds(j * half, half), pl.ds(512 * j, 512), all_half) for j in range(2)])

    def group_copies(g):
        return [pltpu.make_async_copy(ref.at[a, b], r.wbuf[g % w_count].at[c, e], r.w_sem.at[g, i]) for i, (ref, a, b, c, e) in enumerate(groups[g])]

    def load(g):
        if g < len(groups):
            for copy in group_copies(g):
                copy.start()

    taken = [0]

    def with_group(use):
        g = taken[0]
        taken[0] += 1
        for copy in group_copies(g):
            copy.wait()
        use(r.wbuf[g % w_count])
        load(g + w_count)

    barrier = pltpu.get_barrier_semaphore()
    peers = [lax.rem(me + s, beams) for s in range(1, beams)]
    model_peers = [lax.rem(model + s, models) for s in range(1, models)]
    for peer in peers:
        pl.semaphore_signal(barrier, **to(peer))
    for m in model_peers:
        for peer in (me, sibling):
            pl.semaphore_signal(barrier, **across(m, peer))

    @pl.when(is_k)
    def _():
        for c in range(nchunk):
            load_own(k_ref, c).start()

    @pl.when(is_v)
    def _():
        for c in range(nchunk):
            load_own(v_ref, c).start()

    load(0)
    prow = jnp.zeros((1, lanes), jnp.int32)
    for b in range(beams * rows):
        prow = jnp.where(lax.rem(lane_iota, beams * rows) == b, parent_ref[0, b], prow)
    for j in range(rows):
        r.score_rows[j : j + 1, :] = jnp.full((1, lanes), r.score[j])
    angles = pos_ref[0].astype(f32) * r.freq[...]
    cos_part = jnp.cos(angles)
    sin_part = jnp.where(lane_iota < lanes // 2, -1.0, 1.0) * jnp.sin(angles)
    pl.semaphore_wait(barrier, beams - 1 + 2 * (models - 1))

    x_swap = pltpu.make_async_remote_copy(r.x, r.x_got, r.pair_send.at[0], r.pair_recv.at[0], **to(sibling))
    x_swap.start()
    tell_scores = Copies(
        [pltpu.make_async_remote_copy(r.score_rows, r.scores.at[me], r.beam_send.at[1, s], r.beam_recv.at[1, s], **to(p)) for s, p in enumerate(peers)])
    tell_scores.start()

    @pl.when(is_k)
    def _():
        for c in range(nchunk):
            swap(v_ref, c).start()

    @pl.when(is_v)
    def _():
        for c in range(nchunk):
            swap(k_ref, c).start()

    for g in range(1, w_count):
        load(g)

    @pl.when(is_k)
    def _():
        for c in range(nchunk):
            load_other(v_ref, c).start()

    @pl.when(is_v)
    def _():
        for c in range(nchunk):
            load_other(k_ref, c).start()

    strip = min(block, 128)

    def build(n, c):
        for d in SIDES:
            code = table[d * TABLE + n]
            row = jnp.minimum(code, pair - 1)

            def body(i):
                at = pl.ds(pl.multiple_of(i * strip, strip), strip)
                x = pool[c][row, at, :]
                for e in range(n):
                    x = jnp.where(code == pair + e, recv[c][2 * e + d, at, :], x)
                send[c][2 * n + d, at, :] = x

            loop(block // strip, body)
        for d in SIDES:
            hop(n, d, c).start()

    waited = set()

    def have_own(c):
        if c not in waited:
            waited.add(c)
            load_own(k_ref, c).wait()

    def first_round(c):
        have_own(c)
        swap(k_ref, c).wait_recv()
        build(0, c)

    def later_round(n, c):
        for d in SIDES:
            hop(n - 1, d, c).wait_recv()
        build(n, c)

    def finish(c):
        for d in SIDES:
            hop(rounds - 1, d, c).wait_recv()
        position = pos_ref[0]

        def put_row(j):
            where = table[2 * TABLE + j]
            row = jnp.minimum(where, pair - 1)
            slot = jnp.clip(where - pair, 0, 2 * rounds - 1)
            new = jnp.concatenate([r.fresh[j]] * (strip // heads))

            def body(i):
                at = pl.ds(pl.multiple_of(i * strip, strip), strip)
                x = jnp.where(where < pair, pool[c][row, at, :], recv[c][slot, at, :])
                here = (lax.broadcasted_iota(jnp.int32, (strip, lanes), 0) + i * strip) // heads + c * span
                stage[c][j, at, :] = jnp.where(here == position, new, x.astype(f32)).astype(bf16)

            loop(block // strip, body)

        loop(pair, put_row)

        @pl.when(is_k)
        def _():
            give(k_out, c).start()
            store_own(k_out, c).start()

        @pl.when(is_v)
        def _():
            give(v_out, c).start()
            store_own(v_out, c).start()

    todo = [functools.partial(first_round, c) for c in range(nchunk)]
    todo += [functools.partial(later_round, n, c) for n in range(1, rounds) for c in range(nchunk)]

    def serve(n=1):
        for _ in range(n):
            if todo:
                todo.pop(0)()

    res = r.res

    def normed(gain_ref):
        x = res[...]
        inv = lax.rsqrt(jnp.mean(x * x, axis=-1, keepdims=True) + NORM_EPS)
        r.h[...] = (x * inv * gain_ref[...].astype(f32)).astype(bf16)

    def dot(a, b):
        return jnp.dot(a, b, preferred_element_type=f32)

    def dot_halves(w, n):
        def body(j, x):
            a = h[:, pl.ds(pl.multiple_of(j * half, lanes), half)]
            b = w[pl.ds(pl.multiple_of(j * 512, 512), n), :]
            return x + lax.dot_general(a, b, (((1,), (1,)), ((), ())), preferred_element_type=f32)

        return lax.fori_loop(0, 2, body, jnp.zeros((pair, n), f32))

    def dot_rows(a, first, w, n):
        def body(j, x):
            at = pl.multiple_of(j * (n // 2), lanes)
            return x + dot(a[:, pl.ds(first + at, n // 2)], w[pl.ds(at, n // 2), :])

        return lax.fori_loop(0, 2, body, jnp.zeros((pair, half), f32))

    def exchange_model(part_ref, got_ref, phase):
        if models == 1:
            return part_ref[...]
        copies = [
            pltpu.make_async_remote_copy(part_ref, got_ref.at[model], r.model_send.at[phase, s], r.model_recv.at[phase, s], **across(m, me))
            for s, m in enumerate(model_peers)]
        for copy in copies:
            copy.start()
        got_ref[model] = part_ref[...]
        serve(2)
        for copy in copies:
            copy.wait()
        total = got_ref[0]
        for m in range(1, models):
            total = total + got_ref[m]
        return total

    serve()
    x_swap.wait()

    @pl.when(is_k)
    def _():
        res[0:rows, :] = r.x[...].astype(f32)
        res[rows:pair, :] = r.x_got[...].astype(f32)

    @pl.when(is_v)
    def _():
        res[0:rows, :] = r.x_got[...].astype(f32)
        res[rows:pair, :] = r.x[...].astype(f32)

    normed(r.gain_attn)
    h = r.h
    head_half = heads // 2
    width = head_half * lanes
    qkv = r.qkv
    for kind in range(3):
        def use(w, kind=kind):
            blocks = d_model // 1024
            each = min(2, blocks)

            def body(i, z):
                for e in range(each):
                    at = i * each + e
                    a = h[:, pl.ds(pl.multiple_of(at * 1024, 1024), 1024)]
                    z = z + dot(a, w[:, pl.ds(pl.multiple_of(at * width, lanes), width)])
                return z

            z = lax.fori_loop(0, blocks // each, body, jnp.zeros((pair, width), f32))
            for n in range(head_half):
                y = z[:, n * lanes : (n + 1) * lanes]
                if kind < 2:
                    y = y * cos_part + pltpu.roll(y, lanes // 2, 1) * sin_part
                qkv[kind, n] = y.astype(bf16)
        with_group(use)
        serve(kind == 1)

    qkv_all = r.qkv_all
    to_parents = Copies(
        [pltpu.make_async_remote_copy(qkv, qkv_all.at[me], r.beam_send.at[0, s], r.beam_recv.at[0, s], **to(p)) for s, p in enumerate(peers)]
        )
    to_parents.start()
    qkv_all[me] = qkv[...]
    serve(2)
    to_parents.wait()

    cat = r.cat
    for kind in range(3):
        for n in range(heads):
            for x in range(chips):
                at = n * beams * rows + x * pair
                cat[kind, at : at + pair, :] = qkv_all[2 * x + n // head_half, kind, n % head_half].astype(f32)
    for j in range(pair):
        at = pl.ds(chip * pair + j, heads, stride=beams * rows)
        r.fresh[j] = jnp.where(is_k, cat[1, at, :], cat[2, at, :])

    query_t = cat[0].T.astype(bf16)
    new_k = cat[1].astype(bf16)
    total_cols = heads * beams * rows
    tiles = total_cols // lanes
    heads_tile = heads // tiles
    lane_head = lane_iota // (beams * rows)
    spread = r.spread
    logit = r.logit
    position = pos_ref[0]

    def own_rows(c, p, kind):
        a = pool[c][core * rows + p]
        b = other[c][p]
        return jnp.where(core == kind, a, b)

    def score_chunk(c):
        have_own(c)
        load_other(k_ref, c).wait()

        def body(p):
            full = dot(own_rows(c, p, 0), query_t)
            for t in range(tiles):
                spread[t][...] = full[:, t * lanes : (t + 1) * lanes]
            for t in range(tiles):
                here = prow == me * rows + p
                at = pl.ds(c * span, span)
                x = logit[t][at, :]
                for n in range(heads_tile):
                    got = spread[t][pl.ds(t * heads_tile + n, span, stride=heads), :]
                    x = jnp.where(here & (lane_head == n), got, x)
                logit[t][at, :] = x

        loop(rows, body)

    for t in range(tiles):
        logit[t][...] = jnp.zeros_like(logit[t])
    self_full = dot(new_k, query_t)
    scale = lanes ** -0.5
    for c in range(nchunk):
        score_chunk(c)
        serve(c % 4 == 1)
    slot_index = lax.broadcasted_iota(jnp.int32, (slots, lanes), 0)
    self_prob = []
    for t in range(tiles):
        diag = lax.broadcasted_iota(jnp.int32, (total_cols, lanes), 0) == lax.broadcasted_iota(jnp.int32, (total_cols, lanes), 1) + t * lanes
        self_row = jnp.sum(jnp.where(diag, self_full[:, t * lanes : (t + 1) * lanes], 0.0), axis=0, keepdims=True)
        x = jnp.where(slot_index == position, self_row, logit[t][...]) * scale
        x = jnp.where(slot_index <= position, x, -jnp.inf)
        e = jnp.exp(x - jnp.max(x, axis=0, keepdims=True))
        prob = e / jnp.sum(e, axis=0, keepdims=True)
        logit[t][...] = jnp.where(slot_index == position, 0.0, prob)
        self_prob.append(jnp.sum(jnp.where(slot_index == position, prob, 0.0), axis=0, keepdims=True))
    for t in range(tiles):
        spread[t][...] = jnp.zeros_like(spread[t])
    out_t = r.out_t
    out_t[...] = cat[2].T * jnp.concatenate(self_prob, axis=1).astype(bf16).astype(f32)

    def value_chunk(c):
        def body(p):
            for t in range(tiles):
                here = prow == me * rows + p
                x = logit[t][pl.ds(c * span, span), :]
                for n in range(heads_tile):
                    spread[t][pl.ds(t * heads_tile + n, span, stride=heads), :] = jnp.where(here & (lane_head == n), x, 0.0)
            prob = jnp.concatenate([spread[t][...].astype(bf16) for t in range(tiles)], axis=1)
            out_t[...] += lax.dot_general(own_rows(c, p, 1), prob, (((0,), (0,)), ((), ())), preferred_element_type=f32)

        loop(rows, body)

    for c in range(nchunk):
        value_chunk(c)
        serve(c % 4 == 0)
    local = jnp.concatenate([prow] * tiles, axis=1) // rows == me
    o_rows = jnp.where(local, out_t[...], 0.0).T
    o_send, o_got = r.o_send, r.o_got
    for x in range(chips):
        for n in range(heads):
            at = n * beams * rows + x * pair
            o_send[x, n] = o_rows[at : at + pair, :].astype(bf16)
    back = Copies([
        pltpu.make_async_remote_copy(o_send.at[lax.rem(me + s, beams) // 2], o_got.at[me], r.beam_send.at[2, s - 1], r.beam_recv.at[2, s - 1], **to(lax.rem(me + s, beams)))
        for s in range(1, beams)])
    back.start()
    o_got[me] = o_send[chip]
    serve(3)
    back.wait()
    for n in range(heads):
        x = o_got[0, n].astype(f32)
        for s in range(1, beams):
            x = x + o_got[s, n].astype(f32)
        r.o[:, n * lanes : (n + 1) * lanes] = x.astype(bf16)

    part_sum, model_got, res_half, res_got = r.part, r.model_got, r.res_half, r.res_got

    def add_to_residual(phase):
        total = exchange_model(part_sum, model_got.at[phase] if models > 1 else None, phase)
        col = pl.ds(pl.multiple_of(core * half, lanes), half)
        other_col = pl.ds(pl.multiple_of((1 - core) * half, lanes), half)
        fresh = res[:, col] + total
        res_half[phase] = fresh
        trade = pltpu.make_async_remote_copy(res_half.at[phase], res_got.at[phase], r.pair_send.at[1 + phase], r.pair_recv.at[1 + phase], **to(sibling))
        trade.start()
        res[:, col] = fresh
        trade.wait()
        res[:, other_col] = res_got[phase]

    def use_out(w):
        part_sum[0] = dot_rows(r.o, 0, w, heads * lanes)
    with_group(use_out)
    serve(2)
    part_sum_ref = part_sum
    part_sum = part_sum_ref.at[0]
    add_to_residual(0)
    normed(r.gain_mlp)

    g_own, g_got, g_all = r.g_own, r.g_got, r.g_all
    for i in range(ff_full + 1):
        n = 256 if i < ff_full else ff_last

        def use(w, i=i, n=n):
            z = dot_halves(w, 2 * n)
            gate, up = z[:, :n], z[:, n:]
            y = jax.nn.silu(gate) * up
            if i == ff_full and ff_skip:
                y = jnp.where(is_v & (lax.broadcasted_iota(jnp.int32, (1, n), 1) < ff_skip), 0.0, y)
            g_own[:, 256 * i : 256 * i + n] = y.astype(bf16)
        with_group(use)
        serve(i % 2)
    g_trade = pltpu.make_async_remote_copy(g_own, g_got, r.pair_send.at[3], r.pair_recv.at[3], **to(sibling))
    g_trade.start()
    serve()
    g_all[:, pl.ds(pl.multiple_of(core * ff_core, lanes), ff_core)] = g_own[...]
    g_trade.wait()
    g_all[:, pl.ds(pl.multiple_of((1 - core) * ff_core, lanes), ff_core)] = g_got[...]
    part_sum = part_sum_ref.at[1]
    for at, n in down_rows:
        def use(w, at=at, n=n):
            x = dot_rows(g_all, at, w, n)
            part_sum[...] = x if at == 0 else part_sum[...] + x
        with_group(use)
    serve(2)
    add_to_residual(1)
    normed(r.gain_final)

    word = r.word
    for i in range(voc_groups):
        def use(w, i=i):
            word[:, 512 * i : 512 * (i + 1)] = dot_halves(w, 512)
        with_group(use)
        serve(i % 2)
    word_send, word_got = r.word_send, r.word_got
    x = word[...]
    word_send[0] = x[0:rows]
    word_send[1] = x[rows:pair]
    word_trade = pltpu.make_async_remote_copy(word_send.at[1 - core], word_got, r.pair_send.at[4], r.pair_recv.at[4], **to(sibling))
    word_trade.start()
    col = lax.broadcasted_iota(jnp.int32, (1, voc_core), 1)
    twice = is_v & (col >= voc_core - 512) & (col < voc_core - 512 + voc_skip)
    x = jnp.where(twice, -jnp.inf, x)
    top = jnp.max(x, axis=-1, keepdims=True)
    mass = jnp.sum(jnp.exp(x - top), axis=-1, keepdims=True)
    stat, stats = r.stat, r.stats
    stat[0] = jnp.broadcast_to(top, (pair, lanes))
    stat[1] = jnp.broadcast_to(mass, (pair, lanes))
    mates = [(m, p) for m in [model] + model_peers for p in (me, sibling)][1:]
    told = Copies([
        pltpu.make_async_remote_copy(stat, stats.at[2 * model + core], r.stat_send.at[i], r.stat_recv.at[i], **across(m, p))
        for i, (m, p) in enumerate(mates)])
    told.start()
    stats[2 * model + core] = stat[...]
    serve(len(todo))
    for c in range(nchunk // 2):
        finish(c)
    told.wait()
    top = stats[0, 0]
    for i in range(1, 2 * models):
        top = jnp.maximum(top, stats[i, 0])
    mass = stats[0, 1] * jnp.exp(stats[0, 0] - top)
    for i in range(1, 2 * models):
        mass = mass + stats[i, 1] * jnp.exp(stats[i, 0] - top)
    r.stat[0] = top
    r.stat[1] = jnp.log(mass)
    word_trade.wait()
    tell_scores.wait()
    r.scores[me] = r.score_rows[...]
    own, got = word_send[core], word_got[...]
    low, high = jnp.where(is_k, own, got), jnp.where(is_k, got, own)
    last = voc_core - 512
    for j in range(rows):
        q = parent_ref[0, me * rows + j]
        base = r.scores[q // rows, pl.ds(lax.rem(q, rows), 1), :][:, 0:1]
        at = pl.ds(core * rows + j, 1)
        shift = stat[0, at, 0:1]
        log_mass = stat[1, at, 0:1]
        row = slice(j, j + 1)
        x = base + (high[row] - shift - log_mass)
        r.word_out[row, :voc_core] = base + (low[row] - shift - log_mass)
        r.word_out[row, voc_core : voc_core + last] = x[:, :last]
        r.word_out[row, voc_core + last :] = x[:, last + voc_skip :]

    for c in range(nchunk // 2, nchunk):
        finish(c)
    for c in range(nchunk):
        swap(k_ref, c).wait_send()
        for n in range(rounds):
            for d in SIDES:
                hop(n, d, c).wait_send()
        store_own(k_out, c).wait()
        give(k_out, c).wait()


def run_step(rounds, beams, models, table, pos, parent, score, freq, x, k_rows, v_rows, gains, weights):
    rows, length, lanes = k_rows.shape
    weights_ = types.SimpleNamespace(**weights)
    d_model = x.shape[1]
    heads = weights_.w_query.shape[1] // lanes
    slots = length // heads
    ff = weights_.w_down.shape[0]
    vocab = weights_.w_vocab.shape[0]
    block = length // CHUNKS
    pair = 2 * rows
    half = d_model // 2
    chips = beams // 2
    cols = heads * beams * rows
    bf16, f32 = jnp.bfloat16, jnp.float32
    vmem, dma = pltpu.VMEM, pltpu.SemaphoreType.DMA
    smem, hbm, ram = (pl.BlockSpec(memory_space=s) for s in (pltpu.SMEM, pl.ANY, pltpu.VMEM))
    voc_core = (vocab + 1023) // 1024 * 512
    ff_core = (ff + 127) // 256 * 128
    n_groups = 4 + ff_core // 256 + 1 + -(-2 * ff_core // 1024) + voc_core // 512
    ins = dict(table=(table, smem), pos=(pos, smem), parent=(parent, smem), score=(score, smem), freq=(freq, ram),
               x=(x, ram), k=(k_rows, hbm), v=(v_rows, hbm))
    ins.update({name: (a, ram) for name, a in gains.items()})
    ins.update({name: (a, hbm) for name, a in weights.items()})
    outs = dict(k_out=(jax.ShapeDtypeStruct(k_rows.shape, bf16), hbm), v_out=(jax.ShapeDtypeStruct(k_rows.shape, bf16), hbm),
                word_out=(jax.ShapeDtypeStruct((rows, vocab), f32), ram))
    scratch = dict(
        pool=[vmem((pair, block, lanes), bf16)] * CHUNKS,
        recv=[vmem((2 * rounds, block, lanes), bf16)] * CHUNKS,
        send=[vmem((2 * rounds, block, lanes), bf16)] * CHUNKS,
        stage=[vmem((pair, block, lanes), bf16)] * CHUNKS,
        other=[vmem((rows, block, lanes), bf16)] * CHUNKS,
        wbuf=[vmem((1024, half), bf16)] * (W_BUFFERS - rounds),
        spread=[vmem((block, lanes), f32)] * (cols // lanes),
        logit=[vmem((slots, lanes), f32)] * (cols // lanes),
        x_got=vmem(x.shape, bf16),
        res=vmem((pair, d_model), f32),
        h=vmem((pair, d_model), bf16),
        qkv=vmem((3, heads // 2, pair, lanes), bf16),
        qkv_all=vmem((beams, 3, heads // 2, pair, lanes), bf16),
        scores=vmem((beams, rows, lanes), f32),
        score_rows=vmem((rows, lanes), f32),
        cat=vmem((3, cols, lanes), f32),
        fresh=vmem((pair, heads, lanes), f32),
        out_t=vmem((lanes, cols), f32),
        o_send=vmem((chips, heads, pair, lanes), bf16),
        o_got=vmem((beams, heads, pair, lanes), bf16),
        o=vmem((pair, heads * lanes), bf16),
        part=vmem((2, pair, half), f32),
        model_got=vmem((2, models, pair, half), f32),
        res_half=vmem((2, pair, half), f32),
        res_got=vmem((2, pair, half), f32),
        g_own=vmem((pair, ff_core), bf16),
        g_got=vmem((pair, ff_core), bf16),
        g_all=vmem((pair, 2 * ff_core), bf16),
        word=vmem((pair, voc_core), f32),
        word_send=vmem((2, rows, voc_core), f32),
        word_got=vmem((rows, voc_core), f32),
        stat=vmem((2, pair, lanes), f32),
        stats=vmem((2 * models, 2, pair, lanes), f32),
        w_sem=dma((n_groups, 4)),
        pool_sem=dma((CHUNKS,)), other_sem=dma((CHUNKS,)), swap_send=dma((CHUNKS,)), swap_recv=dma((CHUNKS,)),
        hop_send=dma((rounds, 2, CHUNKS)), hop_recv=dma((rounds, 2, CHUNKS)),
        out_sem=dma((CHUNKS,)), give_send=dma((CHUNKS,)), give_recv=dma((CHUNKS,)),
        pair_send=dma((5,)), pair_recv=dma((5,)),
        beam_send=dma((3, beams)), beam_recv=dma((3, beams)),
        model_send=dma((2, models)), model_recv=dma((2, models)),
        stat_send=dma((2 * models,)), stat_recv=dma((2 * models,)),
    )
    flat, places = [], {}
    for name, s in scratch.items():
        many = isinstance(s, list)
        places[name] = (len(flat), len(s) if many else None)
        flat += s if many else [s]
    first = list(ins) + list(outs)

    def kernel(*refs):
        named = list(refs[: len(first)])
        rest = refs[len(first) :]
        for start, count in places.values():
            named.append(rest[start] if count is None else list(rest[start : start + count]))
        step_kernel(rounds, beams, models, rows, heads, slots, d_model, ff, vocab, first + list(places), *named)

    return pl.pallas_call(
        kernel,
        out_shape=tuple(s for s, _ in outs.values()),
        in_specs=[s for _, s in ins.values()],
        out_specs=tuple(s for _, s in outs.values()),
        scratch_shapes=flat,
        compiler_params=pltpu.CompilerParams(collective_id=rounds, has_side_effects=True, vmem_limit_bytes=VMEM_LIMIT),
        name=f"step{rounds}",
    )(*[a for a, _ in ins.values()])


def copy_kernel(pieces, a_ref, b_ref, a_out, b_out, buf, in_sem, out_sem):
    rows, length, _ = a_ref.shape
    per = length // pieces
    jobs = [(src, dst, i, e) for i in range(rows) for e in range(pieces) for src, dst in ((a_ref, a_out), (b_ref, b_out))]

    def get(n):
        src, _, i, e = jobs[n]
        return pltpu.make_async_copy(src.at[i, pl.ds(e * per, per)], buf.at[n], in_sem.at[n])

    def put(n):
        _, dst, i, e = jobs[n]
        return pltpu.make_async_copy(buf.at[n], dst.at[i, pl.ds(e * per, per)], out_sem.at[n])

    for n in range(len(jobs)):
        get(n).start()
    for n in range(len(jobs)):
        get(n).wait()
        put(n).start()
    for n in range(len(jobs)):
        put(n).wait()


def settle(a, b):
    rows, length, lanes = a.shape
    hbm = pl.BlockSpec(memory_space=pl.ANY)
    out = jax.ShapeDtypeStruct(a.shape, a.dtype)
    jobs = 2 * rows * SETTLE_PIECES
    return pl.pallas_call(
        functools.partial(copy_kernel, SETTLE_PIECES),
        out_shape=(out, out),
        in_specs=[hbm, hbm],
        out_specs=(hbm, hbm),
        scratch_shapes=[pltpu.VMEM((jobs, length // SETTLE_PIECES, lanes), a.dtype), pltpu.SemaphoreType.DMA((jobs,)), pltpu.SemaphoreType.DMA((jobs,))],
        name="settle",
    )(a, b)


def move_any(beams, heads, parent, position, k_rows, v_rows, k_new, v_new):
    rows, length, _ = k_rows.shape
    me = lax.axis_index("beam")
    mine = lax.dynamic_slice(parent.reshape(-1), (me * rows,), (rows,))
    local = lax.rem(mine, rows)
    ring = [(i, (i + 1) % beams) for i in range(beams)]

    def choose(source, here, chosen):
        hit = (mine // rows == source)[:, None, None]
        return jnp.where(hit, jnp.take(here, local, axis=0), chosen)

    def step(s, carry):
        k_here, v_here, k_sel, v_sel = carry
        source = lax.rem(me - s + beams, beams)
        k_sel, v_sel = choose(source, k_here, k_sel), choose(source, v_here, v_sel)
        return lax.ppermute(k_here, "beam", ring), lax.ppermute(v_here, "beam", ring), k_sel, v_sel

    carry = (lax.ppermute(k_rows, "beam", ring), lax.ppermute(v_rows, "beam", ring), choose(me, k_rows, k_new), choose(me, v_rows, v_new))
    carry = lax.fori_loop(1, beams, step, carry)
    written = (jnp.arange(length) // heads == position)[None, :, None]
    return jnp.where(written, k_new, carry[2]), jnp.where(written, v_new, carry[3])


def solution(mesh):
    beams = mesh.shape["beam"]
    models = mesh.shape["model"]
    cache_spec = P(None, ('data', 'beam'), None, 'model', None)
    col_spec = P(None, None, 'model')
    row_spec = P(None, 'model', None)
    in_specs = (P(('data', 'beam'), None), P('data', None), P(), P(('data', 'beam')), cache_spec, cache_spec,
                P(), col_spec, col_spec, col_spec, row_spec, P(), col_spec, col_spec, row_spec, P(), P(None, 'model'))
    out_specs = (cache_spec, cache_spec, P(('data', 'beam'), 'model'))

    def local_step(x_embed, parent, position, score, k_cache, v_cache, gain_attn, w_query, w_key, w_value, w_out, gain_mlp, w_gate, w_up, w_down, gain_final, w_vocab):
        rows = x_embed.shape[0]
        _, _, slots, heads, lanes = k_cache.shape
        table, info = make_plan(parent, beams // 2, 2 * rows)
        k_rows = k_cache.reshape(rows, slots * heads, lanes)
        v_rows = v_cache.reshape(rows, slots * heads, lanes)
        half_dim = lanes // 2
        freq = np.float32(ROPE_BASE) ** (-np.arange(half_dim, dtype=np.float32) / np.float32(half_dim))
        freq = jnp.asarray(np.concatenate([freq, freq])[None])
        pos = position.reshape(1)
        gains = dict(gain_attn=gain_attn, gain_mlp=gain_mlp, gain_final=gain_final.reshape(1, -1))
        weights = dict(w_query=w_query[0], w_key=w_key[0], w_value=w_value[0], w_out=w_out[0],
                       w_gate=w_gate[0].T, w_up=w_up[0].T, w_down=w_down[0], w_vocab=w_vocab.T)
        def step(rounds):
            return run_step(rounds, beams, models, table, pos, parent, score, freq, x_embed, k_rows, v_rows, gains, weights)

        def few(_):
            k_new, v_new, word = step(ROUND_CHOICES[0])
            return *settle(k_new, v_new), word

        def more(_):
            k_new, v_new, word = step(ROUND_CHOICES[1])
            enough = info[0] <= ROUND_CHOICES[1]
            k_new, v_new = lax.cond(enough, settle, lambda a, b: move_any(beams, heads, parent, position, k_rows, v_rows, a, b), k_new, v_new)
            return k_new, v_new, word

        k_new, v_new, candidates = lax.cond(info[0] <= ROUND_CHOICES[0], few, more, 0)
        shape = (1, rows, slots, heads, lanes)
        return k_new.reshape(shape), v_new.reshape(shape), candidates

    return jax.shard_map(local_step, mesh=mesh, in_specs=in_specs, out_specs=out_specs, check_vma=False)
```

```python
import functools
import types

import jax
import jax.numpy as jnp
from jax import lax
from jax.experimental import pallas as pl
from jax.experimental.pallas import tpu as pltpu
import numpy as np
from jax.sharding import PartitionSpec as P

NORM_EPS = 1e-6
ROPE_BASE = 10000.0
MESH = pl.DeviceIdType.MESH
CHUNKS = 8
TABLE = 24
ROUND_CHOICES = (3, 4)
W_BUFFERS = 8
SETTLE_PIECES = 1
SIDES = (0, 1)
LANES = 128
VMEM_LIMIT = 66 * 10**6


def plan_kernel(chips, chip_rows, parent_ref, table_ref, info_ref, hop_plus, hop_minus, onward, side):
    total = chips * chip_rows
    my_chip = lax.axis_index("beam") // 2
    row_bits, chip_mask, row_mask = chip_rows.bit_length() - 1, chips - 1, chip_rows - 1
    spare = 2 * TABLE + chip_rows

    near, far, back = [jnp.int32(0)] * 3
    parents = [parent_ref[0, b] for b in range(total)]
    for b, q in enumerate(parents):
        dist = ((b >> row_bits) - (q >> row_bits)) & chip_mask
        bit = jnp.left_shift(1, q)
        near |= jnp.where(dist == 1, bit, 0)
        far |= jnp.where(dist == 2, bit, 0)
        back |= jnp.where(dist == 3, bit, 0)

    def bit_of(mask, q):
        return jnp.right_shift(mask, q) & 1

    every = [(q, q >> row_bits, bit_of(near, q), bit_of(far, q), bit_of(back, q)) for q in range(total)]
    right = [(c + 1) & chip_mask for c in range(chips)]
    left = [(c - 1) & chip_mask for c in range(chips)]
    load_plus, load_minus, own_plus, own_minus, two_plus, two_minus = [[jnp.int32(0)] * chips for _ in range(6)]
    plus, minus = [], []
    for q, c, a, b, d in every:
        plus.append(b & a & (1 - d))
        minus.append(b & d & (1 - a))
        own_plus[c] += a
        own_minus[c] += d
        load_plus[right[c]] += plus[q]
        load_minus[left[c]] += minus[q]
    load_plus = [x + y for x, y in zip(load_plus, own_plus)]
    load_minus = [x + y for x, y in zip(load_minus, own_minus)]
    for q, c, a, b, d in every:
        flex = b & (1 - (a ^ d))
        cost_plus = jnp.maximum(load_plus[c] - a, load_plus[right[c]])
        cost_minus = jnp.maximum(load_minus[c] - d, load_minus[left[c]])
        go = jnp.where(cost_plus <= cost_minus, flex, 0)
        stay = flex - go
        for load, own, x, y in ((load_plus, own_plus, go, a), (load_minus, own_minus, stay, d)):
            load[c] += x & (1 - y)
            own[c] += x & (1 - y)
        load_plus[right[c]] += go
        load_minus[left[c]] += stay
        plus[q] += go
        minus[q] += stay
    first_plus, first_minus = [], []
    for q, c, *_ in every:
        first_plus.append(two_plus[c])
        first_minus.append(two_minus[c])
        two_plus[c] += plus[q]
        two_minus[c] += minus[q]
    rounds = jnp.int32(0)

    for at in range(spare):
        table_ref[at] = 0

    def write(cond, place, value):
        table_ref[jnp.where(cond, place, spare)] = value

    for q, c, a, b, d in every:
        a, d = a & (1 - plus[q]), d & (1 - minus[q])
        h_plus = jnp.where(a == 1, two_plus[c], first_plus[q])
        h_minus = jnp.where(d == 1, two_minus[c], first_minus[q])
        two_plus[c] += a
        two_minus[c] += d
        second = jnp.where(plus[q] == 1, jnp.maximum(own_plus[right[c]], 1) + h_plus, jnp.maximum(own_minus[left[c]], 1) + h_minus)
        uses_plus, uses_minus, uses_two = (a + plus[q]) == 1, (d + minus[q]) == 1, (plus[q] + minus[q]) == 1
        for use, h in ((uses_plus, h_plus), (uses_minus, h_minus), (uses_two, second)):
            rounds = jnp.maximum(rounds, jnp.where(use, h + 1, 0))
        hop_plus[q] = h_plus
        hop_minus[q] = h_minus
        onward[q] = second
        side[q] = plus[q]
        here = my_chip == c
        write(here & uses_plus, h_plus, q & row_mask)
        write(here & uses_minus, TABLE + h_minus, q & row_mask)
        write((my_chip == right[c]) & (plus[q] == 1), second, chip_rows + h_plus)
        write((my_chip == left[c]) & (minus[q] == 1), TABLE + second, chip_rows + h_minus)
    info_ref[0] = rounds
    for j in range(chip_rows):
        q = parent_ref[0, my_chip * chip_rows + j]
        dist = (my_chip - (q >> row_bits)) & chip_mask
        at_plus = chip_rows + 2 * jnp.where(dist == 1, hop_plus[q], onward[q])
        at_minus = chip_rows + 2 * jnp.where(dist == 3, hop_minus[q], onward[q]) + 1
        from_plus = (dist == 1) | ((dist == 2) & (side[q] == 1))
        table_ref[2 * TABLE + j] = jnp.where(dist == 0, q & row_mask, jnp.where(from_plus, at_plus, at_minus))


def make_plan(parent, chips, chip_rows):
    total = chips * chip_rows
    smem = pl.BlockSpec(memory_space=pltpu.SMEM)
    return pl.pallas_call(
        functools.partial(plan_kernel, chips, chip_rows),
        out_shape=(jax.ShapeDtypeStruct((2 * TABLE + chip_rows + 1,), jnp.int32), jax.ShapeDtypeStruct((1,), jnp.int32)),
        in_specs=[smem],
        out_specs=(smem, smem),
        scratch_shapes=[pltpu.SMEM((total,), jnp.int32)] * 4,
        name="plan",
    )(parent)


def loop(n, body):
    def step(i, carry):
        body(i)
        return carry

    lax.fori_loop(0, n, step, 0)


class Copies:
    def __init__(self, copies):
        self.copies = copies

    def start(self):
        for copy in self.copies:
            copy.start()

    def wait(self):
        for copy in self.copies:
            copy.wait()


def step_kernel(rounds, beams, models, rows, heads, slots, d_model, ff, vocab, names, *refs):
    r = types.SimpleNamespace(**dict(zip(names, refs)))
    table, pos_ref, parent_ref = r.table, r.pos, r.parent
    k_ref, v_ref, k_out, v_out = r.k, r.v, r.k_out, r.v_out
    f32, bf16 = jnp.float32, jnp.bfloat16
    nchunk = CHUNKS
    block = slots * heads // nchunk
    span = slots // nchunk
    chips = beams // 2
    pair = 2 * rows
    lanes = LANES
    me = lax.axis_index("beam")
    core = lax.rem(me, 2)
    chip = me // 2
    is_k, is_v = core == 0, core == 1
    all_half, all_heads = pl.ds(0, d_model // 2), pl.ds(0, heads * LANES)
    sibling = me + 1 - 2 * core
    right = lax.rem(me + 2, beams)
    left = lax.rem(me + beams - 2, beams)
    model = lax.axis_index("model")
    mine = pl.ds(core * rows, rows)
    theirs = pl.ds((1 - core) * rows, rows)
    lane_iota = lax.broadcasted_iota(jnp.int32, (1, lanes), 1)
    pool, recv, send, stage, other = r.pool, r.recv, r.send, r.stage, r.other
    half = d_model // 2

    def to(peer):
        return dict(device_id={"beam": peer}, device_id_type=MESH)

    def across(m, peer):
        return dict(device_id={"model": m, "beam": peer}, device_id_type=MESH)

    def part(ref, c):
        return ref.at[:, pl.ds(c * block, block), :]

    def load_own(ref, c):
        return pltpu.make_async_copy(part(ref, c), pool[c].at[mine], r.pool_sem.at[c])

    def load_other(ref, c):
        return pltpu.make_async_copy(part(ref, c), other[c], r.other_sem.at[c])

    def swap(ref, c):
        return pltpu.make_async_remote_copy(part(ref, c), pool[c].at[mine], r.swap_send.at[c], r.swap_recv.at[c], **to(sibling))

    def hop(n, d, c):
        return pltpu.make_async_remote_copy(
            send[c].at[2 * n + d], recv[c].at[2 * n + d], r.hop_send.at[n, d, c], r.hop_recv.at[n, d, c], **to(right if d == 0 else left))

    def store_own(ref, c):
        return pltpu.make_async_copy(stage[c].at[mine], part(ref, c), r.out_sem.at[c])

    def give(ref, c):
        return pltpu.make_async_remote_copy(stage[c].at[theirs], part(ref, c), r.give_send.at[c], r.give_recv.at[c], **to(sibling))

    w_count = len(r.wbuf)
    groups = []

    def group(blocks):
        groups.append(blocks)

    for ref in (r.w_query, r.w_key, r.w_value):
        width = heads * lanes // 2
        group([(ref, pl.ds(1024 * i, 1024), pl.ds(core * width, width), pl.ds(0, 1024), pl.ds(i * width, width)) for i in range(d_model // 1024)])
    group([(r.w_out, all_heads, pl.ds(core * half, half), all_heads, all_half)])
    ff_core = (ff + 127) // 256 * 128
    ff_full = ff_core // 256
    ff_last = ff_core - 256 * ff_full
    ff_skip = 2 * ff_core - ff
    for i in range(ff_full + 1):
        n = 256 if i < ff_full else ff_last
        first = core * (ff_core - (ff_skip if i == ff_full else 0)) + 256 * i
        first = pl.multiple_of(first, 8)
        group([(ref, pl.ds(first, n), pl.ds(j * half, half), pl.ds(512 * j + n * u, n), all_half) for u, ref in enumerate((r.w_gate, r.w_up)) for j in range(2)])
    down_rows = []
    for i in range(0, 2 * ff_core, 1024):
        n = min(1024, 2 * ff_core - i)
        down_rows.append((i, n))
        blocks = [(i, n, 0)]
        if i + n > 2 * ff_core - ff_last:
            blocks = [(i, n - ff_last, 0), (ff - ff_last, ff_last, n - ff_last)]
        group([(r.w_down, pl.ds(a, b), pl.ds(core * half, half), pl.ds(c, b), all_half) for a, b, c in blocks])
    voc_core = (vocab + 1023) // 1024 * 512
    voc_groups = voc_core // 512
    voc_skip = 2 * voc_core - vocab
    for i in range(voc_groups):
        first = core * (voc_core - (voc_skip if i == voc_groups - 1 else 0)) + 512 * i
        first = pl.multiple_of(first, 8)
        group([(r.w_vocab, pl.ds(first, 512), pl.ds(j * half, half), pl.ds(512 * j, 512), all_half) for j in range(2)])

    def group_copies(g):
        return [pltpu.make_async_copy(ref.at[a, b], r.wbuf[g % w_count].at[c, e], r.w_sem.at[g, i]) for i, (ref, a, b, c, e) in enumerate(groups[g])]

    def load(g):
        if g < len(groups):
            for copy in group_copies(g):
                copy.start()

    taken = [0]

    def with_group(use):
        g = taken[0]
        taken[0] += 1
        for copy in group_copies(g):
            copy.wait()
        use(r.wbuf[g % w_count])
        load(g + w_count)

    barrier = pltpu.get_barrier_semaphore()
    peers = [lax.rem(me + s, beams) for s in range(1, beams)]
    model_peers = [lax.rem(model + s, models) for s in range(1, models)]
    for peer in peers:
        pl.semaphore_signal(barrier, **to(peer))
    for m in model_peers:
        for peer in (me, sibling):
            pl.semaphore_signal(barrier, **across(m, peer))

    @pl.when(is_k)
    def _():
        for c in range(nchunk):
            load_own(k_ref, c).start()

    @pl.when(is_v)
    def _():
        for c in range(nchunk):
            load_own(v_ref, c).start()

    load(0)
    for j in range(rows):
        r.score_rows[j : j + 1, :] = jnp.full((1, lanes), r.score[j])
    angles = pos_ref[0].astype(f32) * r.freq[...]
    cos_part = jnp.cos(angles)
    sin_part = jnp.where(lane_iota < lanes // 2, -1.0, 1.0) * jnp.sin(angles)
    pl.semaphore_wait(barrier, beams - 1 + 2 * (models - 1))

    x_swap = pltpu.make_async_remote_copy(r.x, r.x_got, r.pair_send.at[0], r.pair_recv.at[0], **to(sibling))
    x_swap.start()
    tell_scores = Copies(
        [pltpu.make_async_remote_copy(r.score_rows, r.scores.at[me], r.beam_send.at[1, s], r.beam_recv.at[1, s], **to(p)) for s, p in enumerate(peers)])
    tell_scores.start()

    @pl.when(is_k)
    def _():
        for c in range(nchunk):
            swap(v_ref, c).start()

    @pl.when(is_v)
    def _():
        for c in range(nchunk):
            swap(k_ref, c).start()

    for g in range(1, w_count):
        load(g)

    @pl.when(is_k)
    def _():
        for c in range(nchunk):
            load_other(v_ref, c).start()

    @pl.when(is_v)
    def _():
        for c in range(nchunk):
            load_other(k_ref, c).start()

    strip = min(block, 128)

    def build(n, c):
        for d in SIDES:
            code = table[d * TABLE + n]
            row = jnp.minimum(code, pair - 1)

            def body(i):
                at = pl.ds(pl.multiple_of(i * strip, strip), strip)
                x = pool[c][row, at, :]
                for e in range(n):
                    x = jnp.where(code == pair + e, recv[c][2 * e + d, at, :], x)
                send[c][2 * n + d, at, :] = x

            loop(block // strip, body)
        for d in SIDES:
            hop(n, d, c).start()

    waited = set()

    def have_own(c):
        if c not in waited:
            waited.add(c)
            load_own(k_ref, c).wait()

    def first_round(c):
        have_own(c)
        swap(k_ref, c).wait_recv()
        build(0, c)

    def later_round(n, c):
        for d in SIDES:
            hop(n - 1, d, c).wait_recv()
        build(n, c)

    def finish(c):
        for d in SIDES:
            hop(rounds - 1, d, c).wait_recv()
        position = pos_ref[0]

        def put_row(j):
            where = table[2 * TABLE + j]
            row = jnp.minimum(where, pair - 1)
            slot = jnp.clip(where - pair, 0, 2 * rounds - 1)
            new = jnp.concatenate([r.fresh[j]] * (strip // heads))

            def body(i):
                at = pl.ds(pl.multiple_of(i * strip, strip), strip)
                x = jnp.where(where < pair, pool[c][row, at, :], recv[c][slot, at, :])
                here = (lax.broadcasted_iota(jnp.int32, (strip, lanes), 0) + i * strip) // heads + c * span
                stage[c][j, at, :] = jnp.where(here == position, new, x.astype(f32)).astype(bf16)

            loop(block // strip, body)

        loop(pair, put_row)

        @pl.when(is_k)
        def _():
            give(k_out, c).start()
            store_own(k_out, c).start()

        @pl.when(is_v)
        def _():
            give(v_out, c).start()
            store_own(v_out, c).start()

    todo = [functools.partial(first_round, c) for c in range(nchunk)]
    todo += [functools.partial(later_round, n, c) for n in range(1, rounds) for c in range(nchunk)]

    def serve(n=1):
        for _ in range(n):
            if todo:
                todo.pop(0)()

    res = r.res

    def normed(gain_ref):
        x = res[...]
        inv = lax.rsqrt(jnp.mean(x * x, axis=-1, keepdims=True) + NORM_EPS)
        r.h[...] = (x * inv * gain_ref[...].astype(f32)).astype(bf16)

    def dot(a, b):
        return jnp.dot(a, b, preferred_element_type=f32)

    def dot_halves(w, n):
        def body(j, x):
            a = h[:, pl.ds(pl.multiple_of(j * half, lanes), half)]
            b = w[pl.ds(pl.multiple_of(j * 512, 512), n), :]
            return x + lax.dot_general(a, b, (((1,), (1,)), ((), ())), preferred_element_type=f32)

        return lax.fori_loop(0, 2, body, jnp.zeros((pair, n), f32))

    def dot_rows(a, first, w, n):
        def body(j, x):
            at = pl.multiple_of(j * (n // 2), lanes)
            return x + dot(a[:, pl.ds(first + at, n // 2)], w[pl.ds(at, n // 2), :])

        return lax.fori_loop(0, 2, body, jnp.zeros((pair, half), f32))

    def exchange_model(part_ref, got_ref, phase):
        if models == 1:
            return part_ref[...]
        copies = [
            pltpu.make_async_remote_copy(part_ref, got_ref.at[model], r.model_send.at[phase, s], r.model_recv.at[phase, s], **across(m, me))
            for s, m in enumerate(model_peers)]
        for copy in copies:
            copy.start()
        got_ref[model] = part_ref[...]
        serve(2)
        for copy in copies:
            copy.wait()
        total = got_ref[0]
        for m in range(1, models):
            total = total + got_ref[m]
        return total

    serve()
    x_swap.wait()

    @pl.when(is_k)
    def _():
        res[0:rows, :] = r.x[...].astype(f32)
        res[rows:pair, :] = r.x_got[...].astype(f32)

    @pl.when(is_v)
    def _():
        res[0:rows, :] = r.x_got[...].astype(f32)
        res[rows:pair, :] = r.x[...].astype(f32)

    normed(r.gain_attn)
    h = r.h
    head_half = heads // 2
    width = head_half * lanes
    qkv = r.qkv
    for kind in range(3):
        def use(w, kind=kind):
            blocks = d_model // 1024
            each = min(2, blocks)

            def body(i, z):
                for e in range(each):
                    at = i * each + e
                    a = h[:, pl.ds(pl.multiple_of(at * 1024, 1024), 1024)]
                    z = z + dot(a, w[:, pl.ds(pl.multiple_of(at * width, lanes), width)])
                return z

            z = lax.fori_loop(0, blocks // each, body, jnp.zeros((pair, width), f32))
            for n in range(head_half):
                y = z[:, n * lanes : (n + 1) * lanes]
                if kind < 2:
                    y = y * cos_part + pltpu.roll(y, lanes // 2, 1) * sin_part
                qkv[kind, n] = y.astype(bf16)
        with_group(use)
        serve(kind == 1)

    qkv_all = r.qkv_all
    to_parents = Copies(
        [pltpu.make_async_remote_copy(qkv, qkv_all.at[me], r.beam_send.at[0, s], r.beam_recv.at[0, s], **to(p)) for s, p in enumerate(peers)]
        )
    to_parents.start()
    qkv_all[me] = qkv[...]
    serve(2)
    to_parents.wait()

    cat = r.cat
    for kind in range(3):
        for n in range(heads):
            for x in range(chips):
                at = n * beams * rows + x * pair
                cat[kind, at : at + pair, :] = qkv_all[2 * x + n // head_half, kind, n % head_half].astype(f32)
    for j in range(pair):
        at = pl.ds(chip * pair + j, heads, stride=beams * rows)
        r.fresh[j] = jnp.where(is_k, cat[1, at, :], cat[2, at, :])

    query = cat[0].astype(bf16)
    group = beams * rows
    total_rows = heads * group
    pcol = jnp.zeros((group, lanes), jnp.int32)
    for b in range(group):
        pcol = jnp.where(lax.broadcasted_iota(jnp.int32, (group, lanes), 0) == b, parent_ref[0, b], pcol)
    pcol = jnp.concatenate([pcol] * heads)[:, 0:1]
    logit = r.logit
    position = pos_ref[0]

    def own_rows(c, p, kind):
        return jnp.where(core == kind, pool[c][core * rows + p], other[c][p])

    def score_chunk(c):
        have_own(c)
        load_other(k_ref, c).wait()
        at = pl.ds(c * block, block)

        def body(p):
            full = lax.dot_general(query, own_rows(c, p, 0), (((1,), (1,)), ((), ())), preferred_element_type=f32)
            logit[:, at] = jnp.where(pcol == me * rows + p, full, logit[:, at])

        loop(rows, body)

    for c in range(nchunk):
        logit[:, c * block : (c + 1) * block] = jnp.zeros((total_rows, block), f32)
        score_chunk(c)
        serve(c % 4 == 1)
    scale = lanes ** -0.5
    r.self_logit[...] = jnp.broadcast_to(jnp.sum(cat[0] * cat[1], axis=-1, keepdims=True), (total_rows, lanes))
    col = lax.broadcasted_iota(jnp.int32, (1, slots * heads), 1)
    slot_of, head_of = col // heads, lax.rem(col, heads)

    def soften(n):
        at = pl.ds(pl.multiple_of(n * group, group), group)
        x = jnp.where(slot_of == position, r.self_logit[at, 0:1], logit[at, :]) * scale
        x = jnp.where((slot_of <= position) & (head_of == n), x, -jnp.inf)
        e = jnp.exp(x - jnp.max(x, axis=-1, keepdims=True))
        prob = e / jnp.sum(e, axis=-1, keepdims=True)
        logit[at, :] = jnp.where(slot_of == position, 0.0, prob)
        own = jnp.sum(jnp.where(slot_of == position, prob, 0.0), axis=-1, keepdims=True)
        r.out[at, :] = cat[2, at, :] * own.astype(bf16).astype(f32)

    loop(heads, soften)

    def value_chunk(c):
        at = pl.ds(c * block, block)

        def body(p):
            prob = jnp.where(pcol == me * rows + p, logit[:, at], 0.0).astype(bf16)
            r.out[...] += dot(prob, own_rows(c, p, 1))

        loop(rows, body)

    for c in range(nchunk):
        value_chunk(c)
        serve(c % 4 == 0)
    o_rows = jnp.where(pcol // rows == me, r.out[...], 0.0)
    o_send, o_got = r.o_send, r.o_got
    for x in range(chips):
        for n in range(heads):
            at = n * beams * rows + x * pair
            o_send[x, n] = o_rows[at : at + pair, :].astype(bf16)
    back = Copies([
        pltpu.make_async_remote_copy(o_send.at[lax.rem(me + s, beams) // 2], o_got.at[me], r.beam_send.at[2, s - 1], r.beam_recv.at[2, s - 1], **to(lax.rem(me + s, beams)))
        for s in range(1, beams)])
    back.start()
    o_got[me] = o_send[chip]
    serve(3)
    back.wait()
    for n in range(heads):
        x = o_got[0, n].astype(f32)
        for s in range(1, beams):
            x = x + o_got[s, n].astype(f32)
        r.o[:, n * lanes : (n + 1) * lanes] = x.astype(bf16)

    part_sum, model_got, res_half, res_got = r.part, r.model_got, r.res_half, r.res_got

    def add_to_residual(phase):
        total = exchange_model(part_sum, model_got.at[phase] if models > 1 else None, phase)
        col = pl.ds(pl.multiple_of(core * half, lanes), half)
        other_col = pl.ds(pl.multiple_of((1 - core) * half, lanes), half)
        fresh = res[:, col] + total
        res_half[phase] = fresh
        trade = pltpu.make_async_remote_copy(res_half.at[phase], res_got.at[phase], r.pair_send.at[1 + phase], r.pair_recv.at[1 + phase], **to(sibling))
        trade.start()
        res[:, col] = fresh
        trade.wait()
        res[:, other_col] = res_got[phase]

    def use_out(w):
        part_sum[0] = dot_rows(r.o, 0, w, heads * lanes)
    with_group(use_out)
    serve(2)
    part_sum_ref = part_sum
    part_sum = part_sum_ref.at[0]
    add_to_residual(0)
    normed(r.gain_mlp)

    g_own, g_got, g_all = r.g_own, r.g_got, r.g_all
    for i in range(ff_full + 1):
        n = 256 if i < ff_full else ff_last

        def use(w, i=i, n=n):
            z = dot_halves(w, 2 * n)
            gate, up = z[:, :n], z[:, n:]
            y = jax.nn.silu(gate) * up
            if i == ff_full and ff_skip:
                y = jnp.where(is_v & (lax.broadcasted_iota(jnp.int32, (1, n), 1) < ff_skip), 0.0, y)
            g_own[:, 256 * i : 256 * i + n] = y.astype(bf16)
        with_group(use)
        serve(i % 2)
    g_trade = pltpu.make_async_remote_copy(g_own, g_got, r.pair_send.at[3], r.pair_recv.at[3], **to(sibling))
    g_trade.start()
    serve()
    g_all[:, pl.ds(pl.multiple_of(core * ff_core, lanes), ff_core)] = g_own[...]
    g_trade.wait()
    g_all[:, pl.ds(pl.multiple_of((1 - core) * ff_core, lanes), ff_core)] = g_got[...]
    part_sum = part_sum_ref.at[1]
    for at, n in down_rows:
        def use(w, at=at, n=n):
            x = dot_rows(g_all, at, w, n)
            part_sum[...] = x if at == 0 else part_sum[...] + x
        with_group(use)
    serve(2)
    add_to_residual(1)
    normed(r.gain_final)

    word = r.word
    for i in range(voc_groups):
        def use(w, i=i):
            word[:, 512 * i : 512 * (i + 1)] = dot_halves(w, 512)
        with_group(use)
        serve(i % 2)
    word_send, word_got = r.word_send, r.word_got
    x = word[...]
    word_send[0] = x[0:rows]
    word_send[1] = x[rows:pair]
    word_trade = pltpu.make_async_remote_copy(word_send.at[1 - core], word_got, r.pair_send.at[4], r.pair_recv.at[4], **to(sibling))
    word_trade.start()
    col = lax.broadcasted_iota(jnp.int32, (1, voc_core), 1)
    twice = is_v & (col >= voc_core - 512) & (col < voc_core - 512 + voc_skip)
    x = jnp.where(twice, -jnp.inf, x)
    top = jnp.max(x, axis=-1, keepdims=True)
    mass = jnp.sum(jnp.exp(x - top), axis=-1, keepdims=True)
    stat, stats = r.stat, r.stats
    stat[0] = jnp.broadcast_to(top, (pair, lanes))
    stat[1] = jnp.broadcast_to(mass, (pair, lanes))
    mates = [(m, p) for m in [model] + model_peers for p in (me, sibling)][1:]
    told = Copies([
        pltpu.make_async_remote_copy(stat, stats.at[2 * model + core], r.stat_send.at[i], r.stat_recv.at[i], **across(m, p))
        for i, (m, p) in enumerate(mates)])
    told.start()
    stats[2 * model + core] = stat[...]
    serve(len(todo))
    for c in range(nchunk // 2):
        finish(c)
    told.wait()
    top = stats[0, 0]
    for i in range(1, 2 * models):
        top = jnp.maximum(top, stats[i, 0])
    mass = stats[0, 1] * jnp.exp(stats[0, 0] - top)
    for i in range(1, 2 * models):
        mass = mass + stats[i, 1] * jnp.exp(stats[i, 0] - top)
    r.stat[0] = top
    r.stat[1] = jnp.log(mass)
    word_trade.wait()
    tell_scores.wait()
    r.scores[me] = r.score_rows[...]
    own, got = word_send[core], word_got[...]
    low, high = jnp.where(is_k, own, got), jnp.where(is_k, got, own)
    last = voc_core - 512
    for j in range(rows):
        q = parent_ref[0, me * rows + j]
        base = r.scores[q // rows, pl.ds(lax.rem(q, rows), 1), :][:, 0:1]
        at = pl.ds(core * rows + j, 1)
        shift = stat[0, at, 0:1]
        log_mass = stat[1, at, 0:1]
        row = slice(j, j + 1)
        x = base + (high[row] - shift - log_mass)
        r.word_out[row, :voc_core] = base + (low[row] - shift - log_mass)
        r.word_out[row, voc_core : voc_core + last] = x[:, :last]
        r.word_out[row, voc_core + last :] = x[:, last + voc_skip :]

    for c in range(nchunk // 2, nchunk):
        finish(c)
    for c in range(nchunk):
        swap(k_ref, c).wait_send()
        for n in range(rounds):
            for d in SIDES:
                hop(n, d, c).wait_send()
        store_own(k_out, c).wait()
        give(k_out, c).wait()


def run_step(rounds, beams, models, table, pos, parent, score, freq, x, k_rows, v_rows, gains, weights):
    rows, length, lanes = k_rows.shape
    weights_ = types.SimpleNamespace(**weights)
    d_model = x.shape[1]
    heads = weights_.w_query.shape[1] // lanes
    slots = length // heads
    ff = weights_.w_down.shape[0]
    vocab = weights_.w_vocab.shape[0]
    block = length // CHUNKS
    pair = 2 * rows
    half = d_model // 2
    chips = beams // 2
    cols = heads * beams * rows
    bf16, f32 = jnp.bfloat16, jnp.float32
    vmem, dma = pltpu.VMEM, pltpu.SemaphoreType.DMA
    smem, hbm, ram = (pl.BlockSpec(memory_space=s) for s in (pltpu.SMEM, pl.ANY, pltpu.VMEM))
    voc_core = (vocab + 1023) // 1024 * 512
    ff_core = (ff + 127) // 256 * 128
    n_groups = 4 + ff_core // 256 + 1 + -(-2 * ff_core // 1024) + voc_core // 512
    ins = dict(table=(table, smem), pos=(pos, smem), parent=(parent, smem), score=(score, smem), freq=(freq, ram),
               x=(x, ram), k=(k_rows, hbm), v=(v_rows, hbm))
    ins.update({name: (a, ram) for name, a in gains.items()})
    ins.update({name: (a, hbm) for name, a in weights.items()})
    outs = dict(k_out=(jax.ShapeDtypeStruct(k_rows.shape, bf16), hbm), v_out=(jax.ShapeDtypeStruct(k_rows.shape, bf16), hbm),
                word_out=(jax.ShapeDtypeStruct((rows, vocab), f32), ram))
    scratch = dict(
        pool=[vmem((pair, block, lanes), bf16)] * CHUNKS,
        recv=[vmem((2 * rounds, block, lanes), bf16)] * CHUNKS,
        send=[vmem((2 * rounds, block, lanes), bf16)] * CHUNKS,
        stage=[vmem((pair, block, lanes), bf16)] * CHUNKS,
        other=[vmem((rows, block, lanes), bf16)] * CHUNKS,
        wbuf=[vmem((1024, half), bf16)] * (W_BUFFERS - rounds),
        logit=vmem((cols, length), f32),
        self_logit=vmem((cols, lanes), f32),
        x_got=vmem(x.shape, bf16),
        res=vmem((pair, d_model), f32),
        h=vmem((pair, d_model), bf16),
        qkv=vmem((3, heads // 2, pair, lanes), bf16),
        qkv_all=vmem((beams, 3, heads // 2, pair, lanes), bf16),
        scores=vmem((beams, rows, lanes), f32),
        score_rows=vmem((rows, lanes), f32),
        cat=vmem((3, cols, lanes), f32),
        fresh=vmem((pair, heads, lanes), f32),
        out=vmem((cols, lanes), f32),
        o_send=vmem((chips, heads, pair, lanes), bf16),
        o_got=vmem((beams, heads, pair, lanes), bf16),
        o=vmem((pair, heads * lanes), bf16),
        part=vmem((2, pair, half), f32),
        model_got=vmem((2, models, pair, half), f32),
        res_half=vmem((2, pair, half), f32),
        res_got=vmem((2, pair, half), f32),
        g_own=vmem((pair, ff_core), bf16),
        g_got=vmem((pair, ff_core), bf16),
        g_all=vmem((pair, 2 * ff_core), bf16),
        word=vmem((pair, voc_core), f32),
        word_send=vmem((2, rows, voc_core), f32),
        word_got=vmem((rows, voc_core), f32),
        stat=vmem((2, pair, lanes), f32),
        stats=vmem((2 * models, 2, pair, lanes), f32),
        w_sem=dma((n_groups, 4)),
        pool_sem=dma((CHUNKS,)), other_sem=dma((CHUNKS,)), swap_send=dma((CHUNKS,)), swap_recv=dma((CHUNKS,)),
        hop_send=dma((rounds, 2, CHUNKS)), hop_recv=dma((rounds, 2, CHUNKS)),
        out_sem=dma((CHUNKS,)), give_send=dma((CHUNKS,)), give_recv=dma((CHUNKS,)),
        pair_send=dma((5,)), pair_recv=dma((5,)),
        beam_send=dma((3, beams)), beam_recv=dma((3, beams)),
        model_send=dma((2, models)), model_recv=dma((2, models)),
        stat_send=dma((2 * models,)), stat_recv=dma((2 * models,)),
    )
    flat, places = [], {}
    for name, s in scratch.items():
        many = isinstance(s, list)
        places[name] = (len(flat), len(s) if many else None)
        flat += s if many else [s]
    first = list(ins) + list(outs)

    def kernel(*refs):
        named = list(refs[: len(first)])
        rest = refs[len(first) :]
        for start, count in places.values():
            named.append(rest[start] if count is None else list(rest[start : start + count]))
        step_kernel(rounds, beams, models, rows, heads, slots, d_model, ff, vocab, first + list(places), *named)

    return pl.pallas_call(
        kernel,
        out_shape=tuple(s for s, _ in outs.values()),
        in_specs=[s for _, s in ins.values()],
        out_specs=tuple(s for _, s in outs.values()),
        scratch_shapes=flat,
        compiler_params=pltpu.CompilerParams(collective_id=rounds, has_side_effects=True, vmem_limit_bytes=VMEM_LIMIT),
        name=f"step{rounds}",
    )(*[a for a, _ in ins.values()])


def copy_kernel(pieces, a_ref, b_ref, a_out, b_out, buf, in_sem, out_sem):
    rows, length, _ = a_ref.shape
    per = length // pieces
    jobs = [(src, dst, i, e) for i in range(rows) for e in range(pieces) for src, dst in ((a_ref, a_out), (b_ref, b_out))]

    def get(n):
        src, _, i, e = jobs[n]
        return pltpu.make_async_copy(src.at[i, pl.ds(e * per, per)], buf.at[n], in_sem.at[n])

    def put(n):
        _, dst, i, e = jobs[n]
        return pltpu.make_async_copy(buf.at[n], dst.at[i, pl.ds(e * per, per)], out_sem.at[n])

    for n in range(len(jobs)):
        get(n).start()
    for n in range(len(jobs)):
        get(n).wait()
        put(n).start()
    for n in range(len(jobs)):
        put(n).wait()


def settle(a, b):
    rows, length, lanes = a.shape
    hbm = pl.BlockSpec(memory_space=pl.ANY)
    out = jax.ShapeDtypeStruct(a.shape, a.dtype)
    jobs = 2 * rows * SETTLE_PIECES
    return pl.pallas_call(
        functools.partial(copy_kernel, SETTLE_PIECES),
        out_shape=(out, out),
        in_specs=[hbm, hbm],
        out_specs=(hbm, hbm),
        scratch_shapes=[pltpu.VMEM((jobs, length // SETTLE_PIECES, lanes), a.dtype), pltpu.SemaphoreType.DMA((jobs,)), pltpu.SemaphoreType.DMA((jobs,))],
        name="settle",
    )(a, b)


def move_any(beams, heads, parent, position, k_rows, v_rows, k_new, v_new):
    rows, length, _ = k_rows.shape
    me = lax.axis_index("beam")
    mine = lax.dynamic_slice(parent.reshape(-1), (me * rows,), (rows,))
    local = lax.rem(mine, rows)
    ring = [(i, (i + 1) % beams) for i in range(beams)]

    def choose(source, here, chosen):
        hit = (mine // rows == source)[:, None, None]
        return jnp.where(hit, jnp.take(here, local, axis=0), chosen)

    def step(s, carry):
        k_here, v_here, k_sel, v_sel = carry
        source = lax.rem(me - s + beams, beams)
        k_sel, v_sel = choose(source, k_here, k_sel), choose(source, v_here, v_sel)
        return lax.ppermute(k_here, "beam", ring), lax.ppermute(v_here, "beam", ring), k_sel, v_sel

    carry = (lax.ppermute(k_rows, "beam", ring), lax.ppermute(v_rows, "beam", ring), choose(me, k_rows, k_new), choose(me, v_rows, v_new))
    carry = lax.fori_loop(1, beams, step, carry)
    written = (jnp.arange(length) // heads == position)[None, :, None]
    return jnp.where(written, k_new, carry[2]), jnp.where(written, v_new, carry[3])


def solution(mesh):
    beams = mesh.shape["beam"]
    models = mesh.shape["model"]
    cache_spec = P(None, ('data', 'beam'), None, 'model', None)
    col_spec = P(None, None, 'model')
    row_spec = P(None, 'model', None)
    in_specs = (P(('data', 'beam'), None), P('data', None), P(), P(('data', 'beam')), cache_spec, cache_spec,
                P(), col_spec, col_spec, col_spec, row_spec, P(), col_spec, col_spec, row_spec, P(), P(None, 'model'))
    out_specs = (cache_spec, cache_spec, P(('data', 'beam'), 'model'))

    def local_step(x_embed, parent, position, score, k_cache, v_cache, gain_attn, w_query, w_key, w_value, w_out, gain_mlp, w_gate, w_up, w_down, gain_final, w_vocab):
        rows = x_embed.shape[0]
        _, _, slots, heads, lanes = k_cache.shape
        table, info = make_plan(parent, beams // 2, 2 * rows)
        k_rows = k_cache.reshape(rows, slots * heads, lanes)
        v_rows = v_cache.reshape(rows, slots * heads, lanes)
        half_dim = lanes // 2
        freq = np.float32(ROPE_BASE) ** (-np.arange(half_dim, dtype=np.float32) / np.float32(half_dim))
        freq = jnp.asarray(np.concatenate([freq, freq])[None])
        pos = position.reshape(1)
        gains = dict(gain_attn=gain_attn, gain_mlp=gain_mlp, gain_final=gain_final.reshape(1, -1))
        weights = dict(w_query=w_query[0], w_key=w_key[0], w_value=w_value[0], w_out=w_out[0],
                       w_gate=w_gate[0].T, w_up=w_up[0].T, w_down=w_down[0], w_vocab=w_vocab.T)
        def step(rounds):
            return run_step(rounds, beams, models, table, pos, parent, score, freq, x_embed, k_rows, v_rows, gains, weights)

        def few(_):
            k_new, v_new, word = step(ROUND_CHOICES[0])
            return *settle(k_new, v_new), word

        def more(_):
            k_new, v_new, word = step(ROUND_CHOICES[1])
            enough = info[0] <= ROUND_CHOICES[1]
            k_new, v_new = lax.cond(enough, settle, lambda a, b: move_any(beams, heads, parent, position, k_rows, v_rows, a, b), k_new, v_new)
            return k_new, v_new, word

        k_new, v_new, candidates = lax.cond(info[0] <= ROUND_CHOICES[0], few, more, 0)
        shape = (1, rows, slots, heads, lanes)
        return k_new.reshape(shape), v_new.reshape(shape), candidates

    return jax.shard_map(local_step, mesh=mesh, in_specs=in_specs, out_specs=out_specs, check_vma=False)
```

```python
import functools
import types

import jax
import jax.numpy as jnp
from jax import lax
from jax.experimental import pallas as pl
from jax.experimental.pallas import tpu as pltpu
import numpy as np
from jax.sharding import PartitionSpec as P

NORM_EPS = 1e-6
ROPE_BASE = 10000.0
MESH = pl.DeviceIdType.MESH
CHUNKS = 8
TABLE = 24
ROUND_CHOICES = (3, 4)
W_BUFFERS = 9
SETTLE_PIECES = 1
SIDES = (0, 1)
LANES = 128
VMEM_LIMIT = 66 * 10**6


def plan_kernel(chips, chip_rows, parent_ref, table_ref, info_ref, hop_plus, hop_minus, onward, side):
    total = chips * chip_rows
    my_chip = lax.axis_index("beam") // 2
    row_bits, chip_mask, row_mask = chip_rows.bit_length() - 1, chips - 1, chip_rows - 1
    spare = 2 * TABLE + chip_rows

    near, far, back = [jnp.int32(0)] * 3
    parents = [parent_ref[0, b] for b in range(total)]
    for b, q in enumerate(parents):
        dist = ((b >> row_bits) - (q >> row_bits)) & chip_mask
        bit = jnp.left_shift(1, q)
        near |= jnp.where(dist == 1, bit, 0)
        far |= jnp.where(dist == 2, bit, 0)
        back |= jnp.where(dist == 3, bit, 0)

    def bit_of(mask, q):
        return jnp.right_shift(mask, q) & 1

    every = [(q, q >> row_bits, bit_of(near, q), bit_of(far, q), bit_of(back, q)) for q in range(total)]
    right = [(c + 1) & chip_mask for c in range(chips)]
    left = [(c - 1) & chip_mask for c in range(chips)]
    load_plus, load_minus, own_plus, own_minus, two_plus, two_minus = [[jnp.int32(0)] * chips for _ in range(6)]
    plus, minus = [], []
    for q, c, a, b, d in every:
        plus.append(b & a & (1 - d))
        minus.append(b & d & (1 - a))
        own_plus[c] += a
        own_minus[c] += d
        load_plus[right[c]] += plus[q]
        load_minus[left[c]] += minus[q]
    load_plus = [x + y for x, y in zip(load_plus, own_plus)]
    load_minus = [x + y for x, y in zip(load_minus, own_minus)]
    for q, c, a, b, d in every:
        flex = b & (1 - (a ^ d))
        cost_plus = jnp.maximum(load_plus[c] - a, load_plus[right[c]])
        cost_minus = jnp.maximum(load_minus[c] - d, load_minus[left[c]])
        go = jnp.where(cost_plus <= cost_minus, flex, 0)
        stay = flex - go
        for load, own, x, y in ((load_plus, own_plus, go, a), (load_minus, own_minus, stay, d)):
            load[c] += x & (1 - y)
            own[c] += x & (1 - y)
        load_plus[right[c]] += go
        load_minus[left[c]] += stay
        plus[q] += go
        minus[q] += stay
    first_plus, first_minus = [], []
    for q, c, *_ in every:
        first_plus.append(two_plus[c])
        first_minus.append(two_minus[c])
        two_plus[c] += plus[q]
        two_minus[c] += minus[q]
    rounds = jnp.int32(0)

    for at in range(spare):
        table_ref[at] = 0

    def write(cond, place, value):
        table_ref[jnp.where(cond, place, spare)] = value

    for q, c, a, b, d in every:
        a, d = a & (1 - plus[q]), d & (1 - minus[q])
        h_plus = jnp.where(a == 1, two_plus[c], first_plus[q])
        h_minus = jnp.where(d == 1, two_minus[c], first_minus[q])
        two_plus[c] += a
        two_minus[c] += d
        second = jnp.where(plus[q] == 1, jnp.maximum(own_plus[right[c]], 1) + h_plus, jnp.maximum(own_minus[left[c]], 1) + h_minus)
        uses_plus, uses_minus, uses_two = (a + plus[q]) == 1, (d + minus[q]) == 1, (plus[q] + minus[q]) == 1
        for use, h in ((uses_plus, h_plus), (uses_minus, h_minus), (uses_two, second)):
            rounds = jnp.maximum(rounds, jnp.where(use, h + 1, 0))
        hop_plus[q] = h_plus
        hop_minus[q] = h_minus
        onward[q] = second
        side[q] = plus[q]
        here = my_chip == c
        write(here & uses_plus, h_plus, q & row_mask)
        write(here & uses_minus, TABLE + h_minus, q & row_mask)
        write((my_chip == right[c]) & (plus[q] == 1), second, chip_rows + h_plus)
        write((my_chip == left[c]) & (minus[q] == 1), TABLE + second, chip_rows + h_minus)
    info_ref[0] = rounds
    for j in range(chip_rows):
        q = parent_ref[0, my_chip * chip_rows + j]
        dist = (my_chip - (q >> row_bits)) & chip_mask
        at_plus = chip_rows + 2 * jnp.where(dist == 1, hop_plus[q], onward[q])
        at_minus = chip_rows + 2 * jnp.where(dist == 3, hop_minus[q], onward[q]) + 1
        from_plus = (dist == 1) | ((dist == 2) & (side[q] == 1))
        table_ref[2 * TABLE + j] = jnp.where(dist == 0, q & row_mask, jnp.where(from_plus, at_plus, at_minus))


def make_plan(parent, chips, chip_rows):
    total = chips * chip_rows
    smem = pl.BlockSpec(memory_space=pltpu.SMEM)
    return pl.pallas_call(
        functools.partial(plan_kernel, chips, chip_rows),
        out_shape=(jax.ShapeDtypeStruct((2 * TABLE + chip_rows + 1,), jnp.int32), jax.ShapeDtypeStruct((1,), jnp.int32)),
        in_specs=[smem],
        out_specs=(smem, smem),
        scratch_shapes=[pltpu.SMEM((total,), jnp.int32)] * 4,
        name="plan",
    )(parent)


def loop(n, body):
    def step(i, carry):
        body(i)
        return carry

    lax.fori_loop(0, n, step, 0)


class Copies:
    def __init__(self, copies):
        self.copies = copies

    def start(self):
        for copy in self.copies:
            copy.start()

    def wait(self):
        for copy in self.copies:
            copy.wait()


def step_kernel(rounds, beams, models, rows, heads, slots, d_model, ff, vocab, names, *refs):
    r = types.SimpleNamespace(**dict(zip(names, refs)))
    table, pos_ref, parent_ref = r.table, r.pos, r.parent
    k_ref, v_ref, k_out, v_out = r.k, r.v, r.k_out, r.v_out
    f32, bf16 = jnp.float32, jnp.bfloat16
    nchunk = CHUNKS
    block = slots * heads // nchunk
    span = slots // nchunk
    chips = beams // 2
    pair = 2 * rows
    lanes = LANES
    me = lax.axis_index("beam")
    core = lax.rem(me, 2)
    chip = me // 2
    is_k, is_v = core == 0, core == 1
    all_half, all_heads = pl.ds(0, d_model // 2), pl.ds(0, heads * LANES)
    sibling = me + 1 - 2 * core
    right = lax.rem(me + 2, beams)
    left = lax.rem(me + beams - 2, beams)
    model = lax.axis_index("model")
    mine = pl.ds(core * rows, rows)
    theirs = pl.ds((1 - core) * rows, rows)
    lane_iota = lax.broadcasted_iota(jnp.int32, (1, lanes), 1)
    pool, recv, send, stage, other = r.pool, r.recv, r.send, r.stage, r.other
    half = d_model // 2

    def to(peer):
        return dict(device_id={"beam": peer}, device_id_type=MESH)

    def across(m, peer):
        return dict(device_id={"model": m, "beam": peer}, device_id_type=MESH)

    def part(ref, c):
        return ref.at[:, pl.ds(c * block, block), :]

    def load_own(ref, c):
        return pltpu.make_async_copy(part(ref, c), pool[c].at[mine], r.pool_sem.at[c])

    def load_other(ref, c):
        return pltpu.make_async_copy(part(ref, c), other[c], r.other_sem.at[c])

    def swap(ref, c):
        return pltpu.make_async_remote_copy(part(ref, c), pool[c].at[mine], r.swap_send.at[c], r.swap_recv.at[c], **to(sibling))

    def hop(n, d, c):
        return pltpu.make_async_remote_copy(
            send[c].at[2 * n + d], recv[c].at[2 * n + d], r.hop_send.at[n, d, c], r.hop_recv.at[n, d, c], **to(right if d == 0 else left))

    def store_own(ref, c):
        return pltpu.make_async_copy(stage[c].at[mine], part(ref, c), r.out_sem.at[c])

    def give(ref, c):
        return pltpu.make_async_remote_copy(stage[c].at[theirs], part(ref, c), r.give_send.at[c], r.give_recv.at[c], **to(sibling))

    w_count = len(r.wbuf)
    groups = []

    def group(blocks):
        groups.append(blocks)

    for ref in (r.w_query, r.w_key, r.w_value):
        width = heads * lanes // 2
        group([(ref, pl.ds(1024 * i, 1024), pl.ds(core * width, width), pl.ds(0, 1024), pl.ds(i * width, width)) for i in range(d_model // 1024)])
    group([(r.w_out, all_heads, pl.ds(core * half, half), all_heads, all_half)])
    ff_core = (ff + 127) // 256 * 128
    ff_full = ff_core // 256
    ff_last = ff_core - 256 * ff_full
    ff_skip = 2 * ff_core - ff
    for i in range(ff_full + 1):
        n = 256 if i < ff_full else ff_last
        first = core * (ff_core - (ff_skip if i == ff_full else 0)) + 256 * i
        first = pl.multiple_of(first, 8)
        group([(ref, pl.ds(first, n), pl.ds(j * half, half), pl.ds(512 * j + n * u, n), all_half) for u, ref in enumerate((r.w_gate, r.w_up)) for j in range(2)])
    down_rows = []
    for i in range(0, 2 * ff_core, 1024):
        n = min(1024, 2 * ff_core - i)
        down_rows.append((i, n))
        blocks = [(i, n, 0)]
        if i + n > 2 * ff_core - ff_last:
            blocks = [(i, n - ff_last, 0), (ff - ff_last, ff_last, n - ff_last)]
        group([(r.w_down, pl.ds(a, b), pl.ds(core * half, half), pl.ds(c, b), all_half) for a, b, c in blocks])
    voc_core = (vocab + 1023) // 1024 * 512
    voc_groups = voc_core // 512
    voc_skip = 2 * voc_core - vocab
    for i in range(voc_groups):
        first = core * (voc_core - (voc_skip if i == voc_groups - 1 else 0)) + 512 * i
        first = pl.multiple_of(first, 8)
        group([(r.w_vocab, pl.ds(first, 512), pl.ds(j * half, half), pl.ds(512 * j, 512), all_half) for j in range(2)])

    def group_copies(g):
        return [pltpu.make_async_copy(ref.at[a, b], r.wbuf[g % w_count].at[c, e], r.w_sem.at[g, i]) for i, (ref, a, b, c, e) in enumerate(groups[g])]

    def load(g):
        if g < len(groups):
            for copy in group_copies(g):
                copy.start()

    taken = [0]

    def with_group(use):
        g = taken[0]
        taken[0] += 1
        for copy in group_copies(g):
            copy.wait()
        use(r.wbuf[g % w_count])
        load(g + w_count)

    barrier = pltpu.get_barrier_semaphore()
    peers = [lax.rem(me + s, beams) for s in range(1, beams)]
    model_peers = [lax.rem(model + s, models) for s in range(1, models)]
    for peer in peers:
        pl.semaphore_signal(barrier, **to(peer))
    for m in model_peers:
        for peer in (me, sibling):
            pl.semaphore_signal(barrier, **across(m, peer))

    @pl.when(is_k)
    def _():
        for c in range(nchunk):
            load_own(k_ref, c).start()

    @pl.when(is_v)
    def _():
        for c in range(nchunk):
            load_own(v_ref, c).start()

    load(0)
    prow = jnp.zeros((1, lanes), jnp.int32)
    for b in range(beams * rows):
        prow = jnp.where(lax.rem(lane_iota, beams * rows) == b, parent_ref[0, b], prow)
    for j in range(rows):
        r.score_rows[j : j + 1, :] = jnp.full((1, lanes), r.score[j])
    angles = pos_ref[0].astype(f32) * r.freq[...]
    cos_part = jnp.cos(angles)
    sin_part = jnp.where(lane_iota < lanes // 2, -1.0, 1.0) * jnp.sin(angles)
    pl.semaphore_wait(barrier, beams - 1 + 2 * (models - 1))

    x_swap = pltpu.make_async_remote_copy(r.x, r.x_got, r.pair_send.at[0], r.pair_recv.at[0], **to(sibling))
    x_swap.start()
    tell_scores = Copies(
        [pltpu.make_async_remote_copy(r.score_rows, r.scores.at[me], r.beam_send.at[1, s], r.beam_recv.at[1, s], **to(p)) for s, p in enumerate(peers)])
    tell_scores.start()

    @pl.when(is_k)
    def _():
        for c in range(nchunk):
            swap(v_ref, c).start()

    @pl.when(is_v)
    def _():
        for c in range(nchunk):
            swap(k_ref, c).start()

    for g in range(1, w_count):
        load(g)

    @pl.when(is_k)
    def _():
        for c in range(nchunk):
            load_other(v_ref, c).start()

    @pl.when(is_v)
    def _():
        for c in range(nchunk):
            load_other(k_ref, c).start()

    strip = min(block, 128)

    def build(n, c):
        for d in SIDES:
            code = table[d * TABLE + n]
            row = jnp.minimum(code, pair - 1)

            def body(i):
                at = pl.ds(pl.multiple_of(i * strip, strip), strip)
                x = pool[c][row, at, :]
                for e in range(n):
                    x = jnp.where(code == pair + e, recv[c][2 * e + d, at, :], x)
                send[c][2 * n + d, at, :] = x

            loop(block // strip, body)
        for d in SIDES:
            hop(n, d, c).start()

    waited = set()

    def have_own(c):
        if c not in waited:
            waited.add(c)
            load_own(k_ref, c).wait()

    def first_round(c):
        have_own(c)
        swap(k_ref, c).wait_recv()
        build(0, c)

    def later_round(n, c):
        for d in SIDES:
            hop(n - 1, d, c).wait_recv()
        build(n, c)

    def finish(c):
        for d in SIDES:
            hop(rounds - 1, d, c).wait_recv()
        position = pos_ref[0]

        def put_row(j):
            where = table[2 * TABLE + j]
            row = jnp.minimum(where, pair - 1)
            slot = jnp.clip(where - pair, 0, 2 * rounds - 1)
            new = jnp.concatenate([r.fresh[j]] * (strip // heads))

            def body(i):
                at = pl.ds(pl.multiple_of(i * strip, strip), strip)
                x = jnp.where(where < pair, pool[c][row, at, :], recv[c][slot, at, :])
                here = (lax.broadcasted_iota(jnp.int32, (strip, lanes), 0) + i * strip) // heads + c * span
                stage[c][j, at, :] = jnp.where(here == position, new, x.astype(f32)).astype(bf16)

            loop(block // strip, body)

        loop(pair, put_row)

        @pl.when(is_k)
        def _():
            give(k_out, c).start()
            store_own(k_out, c).start()

        @pl.when(is_v)
        def _():
            give(v_out, c).start()
            store_own(v_out, c).start()

    todo = [functools.partial(first_round, c) for c in range(nchunk)]
    todo += [functools.partial(later_round, n, c) for n in range(1, rounds) for c in range(nchunk)]

    early = int(rounds > ROUND_CHOICES[0])

    def serve(n=1):
        for _ in range(n):
            if todo:
                todo.pop(0)()

    res = r.res

    def normed(gain_ref):
        x = res[...]
        inv = lax.rsqrt(jnp.mean(x * x, axis=-1, keepdims=True) + NORM_EPS)
        r.h[...] = (x * inv * gain_ref[...].astype(f32)).astype(bf16)

    def dot(a, b):
        return jnp.dot(a, b, preferred_element_type=f32)

    def dot_halves(w, n):
        def body(j, x):
            a = h[:, pl.ds(pl.multiple_of(j * half, lanes), half)]
            b = w[pl.ds(pl.multiple_of(j * 512, 512), n), :]
            return x + lax.dot_general(a, b, (((1,), (1,)), ((), ())), preferred_element_type=f32)

        return lax.fori_loop(0, 2, body, jnp.zeros((pair, n), f32))

    def dot_rows(a, first, w, n):
        def body(j, x):
            at = pl.multiple_of(j * (n // 2), lanes)
            return x + dot(a[:, pl.ds(first + at, n // 2)], w[pl.ds(at, n // 2), :])

        return lax.fori_loop(0, 2, body, jnp.zeros((pair, half), f32))

    def exchange_model(part_ref, got_ref, phase):
        if models == 1:
            return part_ref[...]
        copies = [
            pltpu.make_async_remote_copy(part_ref, got_ref.at[model], r.model_send.at[phase, s], r.model_recv.at[phase, s], **across(m, me))
            for s, m in enumerate(model_peers)]
        for copy in copies:
            copy.start()
        got_ref[model] = part_ref[...]
        serve(2)
        for copy in copies:
            copy.wait()
        total = got_ref[0]
        for m in range(1, models):
            total = total + got_ref[m]
        return total

    serve()
    x_swap.wait()

    @pl.when(is_k)
    def _():
        res[0:rows, :] = r.x[...].astype(f32)
        res[rows:pair, :] = r.x_got[...].astype(f32)

    @pl.when(is_v)
    def _():
        res[0:rows, :] = r.x_got[...].astype(f32)
        res[rows:pair, :] = r.x[...].astype(f32)

    normed(r.gain_attn)
    h = r.h
    head_half = heads // 2
    width = head_half * lanes
    qkv = r.qkv
    for kind in range(3):
        def use(w, kind=kind):
            blocks = d_model // 1024
            each = min(2, blocks)

            def body(i, z):
                for e in range(each):
                    at = i * each + e
                    a = h[:, pl.ds(pl.multiple_of(at * 1024, 1024), 1024)]
                    z = z + dot(a, w[:, pl.ds(pl.multiple_of(at * width, lanes), width)])
                return z

            z = lax.fori_loop(0, blocks // each, body, jnp.zeros((pair, width), f32))
            for n in range(head_half):
                y = z[:, n * lanes : (n + 1) * lanes]
                if kind < 2:
                    y = y * cos_part + pltpu.roll(y, lanes // 2, 1) * sin_part
                qkv[kind, n] = y.astype(bf16)
        with_group(use)
        serve(early * (kind == 1))

    qkv_all = r.qkv_all
    to_parents = Copies(
        [pltpu.make_async_remote_copy(qkv, qkv_all.at[me], r.beam_send.at[0, s], r.beam_recv.at[0, s], **to(p)) for s, p in enumerate(peers)]
        )
    to_parents.start()
    qkv_all[me] = qkv[...]
    serve(2)
    to_parents.wait()
    serve(early)

    cat = r.cat
    for kind in range(3):
        for n in range(heads):
            for x in range(chips):
                at = n * beams * rows + x * pair
                cat[kind, at : at + pair, :] = qkv_all[2 * x + n // head_half, kind, n % head_half].astype(f32)
    for j in range(pair):
        at = pl.ds(chip * pair + j, heads, stride=beams * rows)
        r.fresh[j] = jnp.where(is_k, cat[1, at, :], cat[2, at, :])

    query_t = cat[0].T.astype(bf16)
    new_k = cat[1].astype(bf16)
    total_cols = heads * beams * rows
    tiles = total_cols // lanes
    heads_tile = heads // tiles
    lane_head = lane_iota // (beams * rows)
    spread = r.spread
    logit = r.logit
    position = pos_ref[0]

    def own_rows(c, p, kind):
        a = pool[c][core * rows + p]
        b = other[c][p]
        return jnp.where(core == kind, a, b)

    def score_chunk(c):
        have_own(c)
        load_other(k_ref, c).wait()

        def body(p):
            full = dot(own_rows(c, p, 0), query_t)
            for t in range(tiles):
                spread[t][...] = full[:, t * lanes : (t + 1) * lanes]
            for t in range(tiles):
                here = prow == me * rows + p
                at = pl.ds(c * span, span)
                x = logit[t][at, :]
                for n in range(heads_tile):
                    got = spread[t][pl.ds(t * heads_tile + n, span, stride=heads), :]
                    x = jnp.where(here & (lane_head == n), got, x)
                logit[t][at, :] = x

        loop(rows, body)

    for t in range(tiles):
        logit[t][...] = jnp.zeros_like(logit[t])
    self_full = dot(new_k, query_t)
    scale = lanes ** -0.5
    for c in range(nchunk):
        score_chunk(c)
        serve(c % 4 == 1 if early else c == nchunk // 2)
    slot_index = lax.broadcasted_iota(jnp.int32, (slots, lanes), 0)
    self_prob = []
    for t in range(tiles):
        diag = lax.broadcasted_iota(jnp.int32, (total_cols, lanes), 0) == lax.broadcasted_iota(jnp.int32, (total_cols, lanes), 1) + t * lanes
        self_row = jnp.sum(jnp.where(diag, self_full[:, t * lanes : (t + 1) * lanes], 0.0), axis=0, keepdims=True)
        x = jnp.where(slot_index == position, self_row, logit[t][...]) * scale
        x = jnp.where(slot_index <= position, x, -jnp.inf)
        e = jnp.exp(x - jnp.max(x, axis=0, keepdims=True))
        prob = e / jnp.sum(e, axis=0, keepdims=True)
        logit[t][...] = jnp.where(slot_index == position, 0.0, prob)
        self_prob.append(jnp.sum(jnp.where(slot_index == position, prob, 0.0), axis=0, keepdims=True))
    for t in range(tiles):
        spread[t][...] = jnp.zeros_like(spread[t])
    out_t = r.out_t
    out_t[...] = cat[2].T * jnp.concatenate(self_prob, axis=1).astype(bf16).astype(f32)

    def value_chunk(c):
        def body(p):
            for t in range(tiles):
                here = prow == me * rows + p
                x = logit[t][pl.ds(c * span, span), :]
                for n in range(heads_tile):
                    spread[t][pl.ds(t * heads_tile + n, span, stride=heads), :] = jnp.where(here & (lane_head == n), x, 0.0)
            prob = jnp.concatenate([spread[t][...].astype(bf16) for t in range(tiles)], axis=1)
            out_t[...] += lax.dot_general(own_rows(c, p, 1), prob, (((0,), (0,)), ((), ())), preferred_element_type=f32)

        loop(rows, body)

    for c in range(nchunk):
        value_chunk(c)
        serve(c % 3 == 1 if early else c % 4 == 0)
    local = jnp.concatenate([prow] * tiles, axis=1) // rows == me
    o_rows = jnp.where(local, out_t[...], 0.0).T
    o_send, o_got = r.o_send, r.o_got
    for x in range(chips):
        for n in range(heads):
            at = n * beams * rows + x * pair
            o_send[x, n] = o_rows[at : at + pair, :].astype(bf16)
    back = Copies([
        pltpu.make_async_remote_copy(o_send.at[lax.rem(me + s, beams) // 2], o_got.at[me], r.beam_send.at[2, s - 1], r.beam_recv.at[2, s - 1], **to(lax.rem(me + s, beams)))
        for s in range(1, beams)])
    back.start()
    o_got[me] = o_send[chip]
    serve(3)
    back.wait()
    for n in range(heads):
        x = o_got[0, n].astype(f32)
        for s in range(1, beams):
            x = x + o_got[s, n].astype(f32)
        r.o[:, n * lanes : (n + 1) * lanes] = x.astype(bf16)

    part_sum, model_got, res_half, res_got = r.part, r.model_got, r.res_half, r.res_got

    def add_to_residual(phase):
        total = exchange_model(part_sum, model_got.at[phase] if models > 1 else None, phase)
        col = pl.ds(pl.multiple_of(core * half, lanes), half)
        other_col = pl.ds(pl.multiple_of((1 - core) * half, lanes), half)
        fresh = res[:, col] + total
        res_half[phase] = fresh
        trade = pltpu.make_async_remote_copy(res_half.at[phase], res_got.at[phase], r.pair_send.at[1 + phase], r.pair_recv.at[1 + phase], **to(sibling))
        trade.start()
        res[:, col] = fresh
        trade.wait()
        res[:, other_col] = res_got[phase]

    def use_out(w):
        part_sum[0] = dot_rows(r.o, 0, w, heads * lanes)
    with_group(use_out)
    serve(2)
    part_sum_ref = part_sum
    part_sum = part_sum_ref.at[0]
    add_to_residual(0)
    normed(r.gain_mlp)

    g_own, g_got, g_all = r.g_own, r.g_got, r.g_all
    for i in range(ff_full + 1):
        n = 256 if i < ff_full else ff_last

        def use(w, i=i, n=n):
            z = dot_halves(w, 2 * n)
            gate, up = z[:, :n], z[:, n:]
            y = jax.nn.silu(gate) * up
            if i == ff_full and ff_skip:
                y = jnp.where(is_v & (lax.broadcasted_iota(jnp.int32, (1, n), 1) < ff_skip), 0.0, y)
            g_own[:, 256 * i : 256 * i + n] = y.astype(bf16)
        with_group(use)
        serve(i % 2)
    g_trade = pltpu.make_async_remote_copy(g_own, g_got, r.pair_send.at[3], r.pair_recv.at[3], **to(sibling))
    g_trade.start()
    serve()
    g_all[:, pl.ds(pl.multiple_of(core * ff_core, lanes), ff_core)] = g_own[...]
    g_trade.wait()
    g_all[:, pl.ds(pl.multiple_of((1 - core) * ff_core, lanes), ff_core)] = g_got[...]
    part_sum = part_sum_ref.at[1]
    for at, n in down_rows:
        def use(w, at=at, n=n):
            x = dot_rows(g_all, at, w, n)
            part_sum[...] = x if at == 0 else part_sum[...] + x
        with_group(use)
    serve(2)
    add_to_residual(1)
    normed(r.gain_final)

    word = r.word
    for i in range(voc_groups):
        def use(w, i=i):
            word[:, 512 * i : 512 * (i + 1)] = dot_halves(w, 512)
        with_group(use)
        serve(i % 2)
    word_send, word_got = r.word_send, r.word_got
    x = word[...]
    word_send[0] = x[0:rows]
    word_send[1] = x[rows:pair]
    word_trade = pltpu.make_async_remote_copy(word_send.at[1 - core], word_got, r.pair_send.at[4], r.pair_recv.at[4], **to(sibling))
    word_trade.start()
    col = lax.broadcasted_iota(jnp.int32, (1, voc_core), 1)
    twice = is_v & (col >= voc_core - 512) & (col < voc_core - 512 + voc_skip)
    x = jnp.where(twice, -jnp.inf, x)
    top = jnp.max(x, axis=-1, keepdims=True)
    mass = jnp.sum(jnp.exp(x - top), axis=-1, keepdims=True)
    stat, stats = r.stat, r.stats
    stat[0] = jnp.broadcast_to(top, (pair, lanes))
    stat[1] = jnp.broadcast_to(mass, (pair, lanes))
    mates = [(m, p) for m in [model] + model_peers for p in (me, sibling)][1:]
    told = Copies([
        pltpu.make_async_remote_copy(stat, stats.at[2 * model + core], r.stat_send.at[i], r.stat_recv.at[i], **across(m, p))
        for i, (m, p) in enumerate(mates)])
    told.start()
    stats[2 * model + core] = stat[...]
    serve(len(todo))
    for c in range(nchunk // 2):
        finish(c)
    told.wait()
    top = stats[0, 0]
    for i in range(1, 2 * models):
        top = jnp.maximum(top, stats[i, 0])
    mass = stats[0, 1] * jnp.exp(stats[0, 0] - top)
    for i in range(1, 2 * models):
        mass = mass + stats[i, 1] * jnp.exp(stats[i, 0] - top)
    r.stat[0] = top
    r.stat[1] = jnp.log(mass)
    word_trade.wait()
    tell_scores.wait()
    r.scores[me] = r.score_rows[...]
    own, got = word_send[core], word_got[...]
    low, high = jnp.where(is_k, own, got), jnp.where(is_k, got, own)
    last = voc_core - 512
    for j in range(rows):
        q = parent_ref[0, me * rows + j]
        base = r.scores[q // rows, pl.ds(lax.rem(q, rows), 1), :][:, 0:1]
        at = pl.ds(core * rows + j, 1)
        shift = stat[0, at, 0:1]
        log_mass = stat[1, at, 0:1]
        row = slice(j, j + 1)
        x = base + (high[row] - shift - log_mass)
        r.word_out[row, :voc_core] = base + (low[row] - shift - log_mass)
        r.word_out[row, voc_core : voc_core + last] = x[:, :last]
        r.word_out[row, voc_core + last :] = x[:, last + voc_skip :]

    for c in range(nchunk // 2, nchunk):
        finish(c)
    for c in range(nchunk):
        swap(k_ref, c).wait_send()
        for n in range(rounds):
            for d in SIDES:
                hop(n, d, c).wait_send()
        store_own(k_out, c).wait()
        give(k_out, c).wait()


def run_step(rounds, beams, models, table, pos, parent, score, freq, x, k_rows, v_rows, gains, weights):
    rows, length, lanes = k_rows.shape
    weights_ = types.SimpleNamespace(**weights)
    d_model = x.shape[1]
    heads = weights_.w_query.shape[1] // lanes
    slots = length // heads
    ff = weights_.w_down.shape[0]
    vocab = weights_.w_vocab.shape[0]
    block = length // CHUNKS
    pair = 2 * rows
    half = d_model // 2
    chips = beams // 2
    cols = heads * beams * rows
    bf16, f32 = jnp.bfloat16, jnp.float32
    vmem, dma = pltpu.VMEM, pltpu.SemaphoreType.DMA
    smem, hbm, ram = (pl.BlockSpec(memory_space=s) for s in (pltpu.SMEM, pl.ANY, pltpu.VMEM))
    voc_core = (vocab + 1023) // 1024 * 512
    ff_core = (ff + 127) // 256 * 128
    n_groups = 4 + ff_core // 256 + 1 + -(-2 * ff_core // 1024) + voc_core // 512
    ins = dict(table=(table, smem), pos=(pos, smem), parent=(parent, smem), score=(score, smem), freq=(freq, ram),
               x=(x, ram), k=(k_rows, hbm), v=(v_rows, hbm))
    ins.update({name: (a, ram) for name, a in gains.items()})
    ins.update({name: (a, hbm) for name, a in weights.items()})
    outs = dict(k_out=(jax.ShapeDtypeStruct(k_rows.shape, bf16), hbm), v_out=(jax.ShapeDtypeStruct(k_rows.shape, bf16), hbm),
                word_out=(jax.ShapeDtypeStruct((rows, vocab), f32), ram))
    scratch = dict(
        pool=[vmem((pair, block, lanes), bf16)] * CHUNKS,
        recv=[vmem((2 * rounds, block, lanes), bf16)] * CHUNKS,
        send=[vmem((2 * rounds, block, lanes), bf16)] * CHUNKS,
        stage=[vmem((pair, block, lanes), bf16)] * CHUNKS,
        other=[vmem((rows, block, lanes), bf16)] * CHUNKS,
        wbuf=[vmem((1024, half), bf16)] * (W_BUFFERS - rounds),
        spread=[vmem((block, lanes), f32)] * (cols // lanes),
        logit=[vmem((slots, lanes), f32)] * (cols // lanes),
        x_got=vmem(x.shape, bf16),
        res=vmem((pair, d_model), f32),
        h=vmem((pair, d_model), bf16),
        qkv=vmem((3, heads // 2, pair, lanes), bf16),
        qkv_all=vmem((beams, 3, heads // 2, pair, lanes), bf16),
        scores=vmem((beams, rows, lanes), f32),
        score_rows=vmem((rows, lanes), f32),
        cat=vmem((3, cols, lanes), f32),
        fresh=vmem((pair, heads, lanes), f32),
        out_t=vmem((lanes, cols), f32),
        o_send=vmem((chips, heads, pair, lanes), bf16),
        o_got=vmem((beams, heads, pair, lanes), bf16),
        o=vmem((pair, heads * lanes), bf16),
        part=vmem((2, pair, half), f32),
        model_got=vmem((2, models, pair, half), f32),
        res_half=vmem((2, pair, half), f32),
        res_got=vmem((2, pair, half), f32),
        g_own=vmem((pair, ff_core), bf16),
        g_got=vmem((pair, ff_core), bf16),
        g_all=vmem((pair, 2 * ff_core), bf16),
        word=vmem((pair, voc_core), f32),
        word_send=vmem((2, rows, voc_core), f32),
        word_got=vmem((rows, voc_core), f32),
        stat=vmem((2, pair, lanes), f32),
        stats=vmem((2 * models, 2, pair, lanes), f32),
        w_sem=dma((n_groups, 4)),
        pool_sem=dma((CHUNKS,)), other_sem=dma((CHUNKS,)), swap_send=dma((CHUNKS,)), swap_recv=dma((CHUNKS,)),
        hop_send=dma((rounds, 2, CHUNKS)), hop_recv=dma((rounds, 2, CHUNKS)),
        out_sem=dma((CHUNKS,)), give_send=dma((CHUNKS,)), give_recv=dma((CHUNKS,)),
        pair_send=dma((5,)), pair_recv=dma((5,)),
        beam_send=dma((3, beams)), beam_recv=dma((3, beams)),
        model_send=dma((2, models)), model_recv=dma((2, models)),
        stat_send=dma((2 * models,)), stat_recv=dma((2 * models,)),
    )
    flat, places = [], {}
    for name, s in scratch.items():
        many = isinstance(s, list)
        places[name] = (len(flat), len(s) if many else None)
        flat += s if many else [s]
    first = list(ins) + list(outs)

    def kernel(*refs):
        named = list(refs[: len(first)])
        rest = refs[len(first) :]
        for start, count in places.values():
            named.append(rest[start] if count is None else list(rest[start : start + count]))
        step_kernel(rounds, beams, models, rows, heads, slots, d_model, ff, vocab, first + list(places), *named)

    return pl.pallas_call(
        kernel,
        out_shape=tuple(s for s, _ in outs.values()),
        in_specs=[s for _, s in ins.values()],
        out_specs=tuple(s for _, s in outs.values()),
        scratch_shapes=flat,
        compiler_params=pltpu.CompilerParams(collective_id=rounds, has_side_effects=True, vmem_limit_bytes=VMEM_LIMIT),
        name=f"step{rounds}",
    )(*[a for a, _ in ins.values()])


def copy_kernel(pieces, a_ref, b_ref, a_out, b_out, buf, in_sem, out_sem):
    rows, length, _ = a_ref.shape
    per = length // pieces
    jobs = [(src, dst, i, e) for i in range(rows) for e in range(pieces) for src, dst in ((a_ref, a_out), (b_ref, b_out))]

    def get(n):
        src, _, i, e = jobs[n]
        return pltpu.make_async_copy(src.at[i, pl.ds(e * per, per)], buf.at[n], in_sem.at[n])

    def put(n):
        _, dst, i, e = jobs[n]
        return pltpu.make_async_copy(buf.at[n], dst.at[i, pl.ds(e * per, per)], out_sem.at[n])

    for n in range(len(jobs)):
        get(n).start()
    for n in range(len(jobs)):
        get(n).wait()
        put(n).start()
    for n in range(len(jobs)):
        put(n).wait()


def settle(a, b):
    rows, length, lanes = a.shape
    hbm = pl.BlockSpec(memory_space=pl.ANY)
    out = jax.ShapeDtypeStruct(a.shape, a.dtype)
    jobs = 2 * rows * SETTLE_PIECES
    return pl.pallas_call(
        functools.partial(copy_kernel, SETTLE_PIECES),
        out_shape=(out, out),
        in_specs=[hbm, hbm],
        out_specs=(hbm, hbm),
        scratch_shapes=[pltpu.VMEM((jobs, length // SETTLE_PIECES, lanes), a.dtype), pltpu.SemaphoreType.DMA((jobs,)), pltpu.SemaphoreType.DMA((jobs,))],
        name="settle",
    )(a, b)


def move_any(beams, heads, parent, position, k_rows, v_rows, k_new, v_new):
    rows, length, _ = k_rows.shape
    me = lax.axis_index("beam")
    mine = lax.dynamic_slice(parent.reshape(-1), (me * rows,), (rows,))
    local = lax.rem(mine, rows)
    ring = [(i, (i + 1) % beams) for i in range(beams)]

    def choose(source, here, chosen):
        hit = (mine // rows == source)[:, None, None]
        return jnp.where(hit, jnp.take(here, local, axis=0), chosen)

    def step(s, carry):
        k_here, v_here, k_sel, v_sel = carry
        source = lax.rem(me - s + beams, beams)
        k_sel, v_sel = choose(source, k_here, k_sel), choose(source, v_here, v_sel)
        return lax.ppermute(k_here, "beam", ring), lax.ppermute(v_here, "beam", ring), k_sel, v_sel

    carry = (lax.ppermute(k_rows, "beam", ring), lax.ppermute(v_rows, "beam", ring), choose(me, k_rows, k_new), choose(me, v_rows, v_new))
    carry = lax.fori_loop(1, beams, step, carry)
    written = (jnp.arange(length) // heads == position)[None, :, None]
    return jnp.where(written, k_new, carry[2]), jnp.where(written, v_new, carry[3])


def solution(mesh):
    beams = mesh.shape["beam"]
    models = mesh.shape["model"]
    cache_spec = P(None, ('data', 'beam'), None, 'model', None)
    col_spec = P(None, None, 'model')
    row_spec = P(None, 'model', None)
    in_specs = (P(('data', 'beam'), None), P('data', None), P(), P(('data', 'beam')), cache_spec, cache_spec,
                P(), col_spec, col_spec, col_spec, row_spec, P(), col_spec, col_spec, row_spec, P(), P(None, 'model'))
    out_specs = (cache_spec, cache_spec, P(('data', 'beam'), 'model'))

    def local_step(x_embed, parent, position, score, k_cache, v_cache, gain_attn, w_query, w_key, w_value, w_out, gain_mlp, w_gate, w_up, w_down, gain_final, w_vocab):
        rows = x_embed.shape[0]
        _, _, slots, heads, lanes = k_cache.shape
        table, info = make_plan(parent, beams // 2, 2 * rows)
        k_rows = k_cache.reshape(rows, slots * heads, lanes)
        v_rows = v_cache.reshape(rows, slots * heads, lanes)
        half_dim = lanes // 2
        freq = np.float32(ROPE_BASE) ** (-np.arange(half_dim, dtype=np.float32) / np.float32(half_dim))
        freq = jnp.asarray(np.concatenate([freq, freq])[None])
        pos = position.reshape(1)
        gains = dict(gain_attn=gain_attn, gain_mlp=gain_mlp, gain_final=gain_final.reshape(1, -1))
        weights = dict(w_query=w_query[0], w_key=w_key[0], w_value=w_value[0], w_out=w_out[0],
                       w_gate=w_gate[0].T, w_up=w_up[0].T, w_down=w_down[0], w_vocab=w_vocab.T)
        def step(rounds):
            return run_step(rounds, beams, models, table, pos, parent, score, freq, x_embed, k_rows, v_rows, gains, weights)

        def few(_):
            k_new, v_new, word = step(ROUND_CHOICES[0])
            return *settle(k_new, v_new), word

        def more(_):
            k_new, v_new, word = step(ROUND_CHOICES[1])
            enough = info[0] <= ROUND_CHOICES[1]
            k_new, v_new = lax.cond(enough, settle, lambda a, b: move_any(beams, heads, parent, position, k_rows, v_rows, a, b), k_new, v_new)
            return k_new, v_new, word

        k_new, v_new, candidates = lax.cond(info[0] <= ROUND_CHOICES[0], few, more, 0)
        shape = (1, rows, slots, heads, lanes)
        return k_new.reshape(shape), v_new.reshape(shape), candidates

    return jax.shard_map(local_step, mesh=mesh, in_specs=in_specs, out_specs=out_specs, check_vma=False)
```
